32 devices in a mesh: dp: 2 (over x), sp: 16 (over z, y, core).
Axes of the slice: x: 2, y: 2, z: 4, core: 2. Of those that a mesh axis runs over, the one named last changes fastest.
Arguments:
- atom_act: bfloat16 [64, 1024, 128], P('dp', 'sp'), parts along dimension 0
- cond: bfloat16 [1024, 128], P('sp')
- pair: bfloat16 [32, 32, 128, 16], P('sp')
- atom_mask: int32 [1024], P('sp')
- w_cond: bfloat16 [3, 128, 768], replicated
- b_cond: float32 [3, 512], replicated
- w_qkvg: bfloat16 [3, 128, 512], replicated
- b_query: float32 [3, 128], replicated
- w_pair: bfloat16 [16, 12], replicated
- w_out: bfloat16 [3, 128, 128], replicated
- w_up: bfloat16 [3, 128, 512], replicated
- w_down: bfloat16 [3, 256, 128], replicated
Outputs:
- output: bfloat16 [64, 1024, 128], P('dp', 'sp'), parts along dimension 0
There are 2 independent parts. The reference program is written for one: setup_inputs(seed, part) draws one part's arguments, and reference() takes and returns one part's arrays. A program takes and returns all parts, laid end to end along the dimension named above; an argument that names none is the same for every part.
All inputs are finite; a program needn't handle non-finite values.
Results may differ from the reference program's by a relative error of at most 0.0131585.
Values are sent between devices in bfloat16 or wider.
A program may use at most 1 GiB of HBM per device.

```python
import jax
import jax.numpy as jnp
from jax import lax

SAMPLES = 32
NUM_ATOMS = 1024
C_ATOM = 128
C_PAIR = 16
NUM_HEADS = 4
LAYERS = 3
QBLOCK = 32
KEY_WINDOW = 128

EDGE = (KEY_WINDOW - QBLOCK) // 2
WIN_BLOCKS = KEY_WINDOW // QBLOCK
LN_EPS = 1e-5


def setup_inputs(seed: int = 0, part: int = 0) -> dict:
    key_list = jax.random.split(jax.random.key(seed), 16)
    part_key = jax.random.fold_in(key_list[0], part)
    n_blocks = NUM_ATOMS // QBLOCK
    width = C_ATOM

    def normal(key, shape, scale):
        return jax.random.normal(key, shape, jnp.float32) * scale

    pad_count = jax.random.randint(key_list[3], (n_blocks,), 0, QBLOCK)
    full_block = jax.random.randint(key_list[4], (), 0, n_blocks)
    pad_count = pad_count.at[full_block].set(QBLOCK - 1)
    slot_idx = jnp.arange(QBLOCK)
    atom_mask = (slot_idx[None, :] < (QBLOCK - pad_count)[:, None]).astype(jnp.int32).reshape(NUM_ATOMS)
    return {
        'atom_act': normal(part_key, (SAMPLES, NUM_ATOMS, width), 1.0).astype(jnp.bfloat16),
        'cond': normal(key_list[1], (NUM_ATOMS, width), 1.0).astype(jnp.bfloat16),
        'pair': normal(key_list[2], (n_blocks, QBLOCK, KEY_WINDOW, C_PAIR), 1.0).astype(jnp.bfloat16),
        'atom_mask': atom_mask,
        'w_cond': normal(key_list[5], (LAYERS, width, 6 * width), width ** -0.5).astype(jnp.bfloat16),
        'b_cond': normal(key_list[6], (LAYERS, 4 * width), 1.0),
        'w_qkvg': normal(key_list[7], (LAYERS, width, 4 * width), width ** -0.5).astype(jnp.bfloat16),
        'b_query': normal(key_list[8], (LAYERS, width), 1.0),
        'w_pair': normal(key_list[9], (C_PAIR, LAYERS * NUM_HEADS), 2.0 * C_PAIR ** -0.5).astype(jnp.bfloat16),
        'w_out': normal(key_list[10], (LAYERS, width, width), 2.0 * width ** -0.5).astype(jnp.bfloat16),
        'w_up': normal(key_list[11], (LAYERS, width, 4 * width), width ** -0.5).astype(jnp.bfloat16),
        'w_down': normal(key_list[12], (LAYERS, 2 * width, width), (2 * width) ** -0.5).astype(jnp.bfloat16),
    }


def layer_norm(vals):
    vals = vals.astype(jnp.float32)
    mean_val = jnp.mean(vals, axis=-1, keepdims=True)
    centered = vals - mean_val
    var_val = jnp.mean(centered * centered, axis=-1, keepdims=True)
    return centered * lax.rsqrt(var_val + LN_EPS)


def windows(ext, n_blocks):
    lead_shape = ext.shape[:-2]
    blocks = ext.reshape(lead_shape + (n_blocks + WIN_BLOCKS - 1, QBLOCK, ext.shape[-1]))
    return jnp.concatenate([blocks[..., blk_off:blk_off + n_blocks, :, :] for blk_off in range(WIN_BLOCKS)], axis=-2)


def reference(atom_act, cond, pair, atom_mask, w_cond, b_cond, w_qkvg, b_query, w_pair, w_out, w_up, w_down):
    width = C_ATOM
    n_blocks = NUM_ATOMS // QBLOCK
    head_dim = C_ATOM // NUM_HEADS
    cond_norm = layer_norm(cond).astype(jnp.bfloat16)
    pair_norm = layer_norm(pair).astype(jnp.bfloat16)
    pair_heads = w_pair.reshape(C_PAIR, LAYERS, NUM_HEADS).transpose(1, 0, 2)
    mask_ext = jnp.pad(atom_mask, (EDGE, EDGE))
    key_valid = windows(mask_ext[:, None], n_blocks)[..., 0]
    mask_bias = (key_valid.astype(jnp.float32) - 1.0) * 1e9

    def layer_step(residual, layer_w):
        cond_w, cond_b, proj_w, query_b, head_w, out_w, up_w, down_w = layer_w
        cond_proj = jnp.dot(cond_norm, cond_w, preferred_element_type=jnp.float32)
        gate_a = jax.nn.sigmoid(cond_proj[:, 0:width] + cond_b[0:width])
        shift_a = cond_proj[:, width:2 * width]
        zero_a = jax.nn.sigmoid(cond_proj[:, 2 * width:3 * width] + cond_b[width:2 * width])
        gate_b = jax.nn.sigmoid(cond_proj[:, 3 * width:4 * width] + cond_b[2 * width:3 * width])
        shift_b = cond_proj[:, 4 * width:5 * width]
        zero_b = jax.nn.sigmoid(cond_proj[:, 5 * width:] + cond_b[3 * width:])
        bias = jnp.einsum('nqkc,ch->nqhk', pair_norm.astype(jnp.float32), head_w.astype(jnp.float32)).astype(jnp.bfloat16)
        logit_add = bias.astype(jnp.float32) + mask_bias[:, None, None, :]

        def one_sample(res_one):
            h_attn = (layer_norm(res_one) * gate_a + shift_a).astype(jnp.bfloat16)
            projected = jnp.dot(h_attn, proj_w, preferred_element_type=jnp.float32)
            q_val = (projected[:, :width] + query_b).astype(jnp.bfloat16)
            kv_loc = projected[:, width:3 * width].astype(jnp.bfloat16)
            gate_o = jax.nn.sigmoid(projected[:, 3 * width:])
            kv_win = windows(jnp.pad(kv_loc, ((EDGE, EDGE), (0, 0))), n_blocks)
            k_win = kv_win[..., :width].reshape(n_blocks, KEY_WINDOW, NUM_HEADS, head_dim)
            v_win = kv_win[..., width:].reshape(n_blocks, KEY_WINDOW, NUM_HEADS, head_dim)
            q_blk = q_val.reshape(n_blocks, QBLOCK, NUM_HEADS, head_dim)
            logits = jnp.einsum('nqhd,nkhd->nqhk', q_blk.astype(jnp.float32), k_win.astype(jnp.float32)) * head_dim ** -0.5 + logit_add
            attn_prob = jax.nn.softmax(logits, axis=-1).astype(jnp.bfloat16)
            attended = jnp.einsum('nqhk,nkhd->nqhd', attn_prob.astype(jnp.float32), v_win.astype(jnp.float32))
            attended = (attended.reshape(NUM_ATOMS, width) * gate_o).astype(jnp.bfloat16)
            res_one = res_one + zero_a * jnp.dot(attended, out_w, preferred_element_type=jnp.float32)
            h_mlp = (layer_norm(res_one) * gate_b + shift_b).astype(jnp.bfloat16)
            up_proj = jnp.dot(h_mlp, up_w, preferred_element_type=jnp.float32)
            hidden = (jax.nn.silu(up_proj[:, :2 * width]) * up_proj[:, 2 * width:]).astype(jnp.bfloat16)
            return res_one + zero_b * jnp.dot(hidden, down_w, preferred_element_type=jnp.float32)

        return lax.map(one_sample, residual), None

    start_res = atom_act.astype(jnp.float32)
    layer_ws = (w_cond, b_cond, w_qkvg, b_query, pair_heads, w_out, w_up, w_down)
    final_res, unused = lax.scan(layer_step, start_res, layer_ws)
    return final_res.astype(jnp.bfloat16)
```

```python
import functools
import math

import jax
import jax.numpy as jnp
from jax import lax
from jax.experimental import pallas as pl
from jax.experimental.pallas import tpu as pltpu
from jax.sharding import PartitionSpec as P

QBLOCK = 32
KEY_WINDOW = 128
EDGE = 48
LN_EPS = 1e-5
GROUP = 4
LOG2E = math.log2(math.e)
NT = (((1,), (1,)), ((), ()))
MESH = pl.DeviceIdType.MESH


def mm(lhs, rhs):
    return jnp.dot(lhs, rhs, preferred_element_type=jnp.float32)


def mm_nt(lhs, rhs):
    return lax.dot_general(lhs, rhs, NT, preferred_element_type=jnp.float32)


def sigmoid(vals):
    return 0.5 * jnp.tanh(0.5 * vals) + 0.5


def norm(vals, axis):
    mean = jnp.mean(vals, axis=axis, keepdims=True)
    cent = vals - mean
    var = jnp.mean(cent * cent, axis=axis, keepdims=True)
    return cent * lax.rsqrt(var + LN_EPS)


def body(n_dev, act_hbm, cond_ref, pair_hbm, mask_ref, wcond_hbm, bcond_ref, wqkvg_hbm, bquery_ref, wpair_ref,
         wout_hbm, wup_hbm, wdown_hbm, out_ref,
         act, pair, wcond, wqkvg, wout, wup, wdown,
         pairf, res, h_cm, h_ext, tab, bias, wv_t, wg_t, wo_t, wu_t, wd_t,
         k_scr, q_scr, v_scr, o_scr, mask_buf,
         in_sem, send_sem, recv_sem, msend_sem, mrecv_sem):
    n_layers, width = bquery_ref.shape
    n_heads = width // QBLOCK
    head_dim = width // n_heads
    n_groups = act.shape[0] // GROUP
    seq = act.shape[1]
    ext = seq + 2 * EDGE
    f32, bf16 = jnp.float32, jnp.bfloat16

    me = lax.axis_index('sp')
    nxt = lax.rem(me + 1, n_dev)
    prv = lax.rem(me + n_dev - 1, n_dev)

    loads = [pltpu.make_async_copy(src, dst, in_sem.at[pos]) for pos, (src, dst) in enumerate(
        [(wcond_hbm, wcond), (act_hbm, act), (pair_hbm, pair), (wqkvg_hbm, wqkvg),
         (wout_hbm, wout), (wup_hbm, wup), (wdown_hbm, wdown)])]
    for load in loads:
        load.start()

    barrier = pltpu.get_barrier_semaphore()
    for peer in (prv, nxt):
        pl.semaphore_signal(barrier, inc=1, device_id={'sp': peer}, device_id_type=MESH)

    mask_buf[1] = jnp.zeros_like(mask_buf[1])
    mask_buf[1, 0:1, 0:seq] = mask_ref[...]

    cond_norm = norm(cond_ref[...].astype(f32), -1).astype(bf16)
    loads[0].wait()

    def tables(layer):
        proj = mm(cond_norm, wcond[layer])
        gates = bcond_ref[layer]
        pieces = []
        for idx, bias_idx in enumerate((0, None, 1, 2, None, 3)):
            piece = proj[:, idx * width:(idx + 1) * width]
            if bias_idx is not None:
                piece = sigmoid(piece + gates[:, bias_idx * width:(bias_idx + 1) * width])
            pieces.append(piece)
        for idx, piece in enumerate(pieces):
            for blk in range(2):
                rows = piece[blk * QBLOCK:(blk + 1) * QBLOCK]
                tab[layer, idx, :, blk * 128:(blk + 1) * 128] = jnp.concatenate([rows] * GROUP, axis=0).T

    tables(0)
    pl.semaphore_wait(barrier, 2)

    def mask_copy(direction):
        return pltpu.make_async_remote_copy(
            src_ref=mask_buf.at[1], dst_ref=mask_buf.at[2 - 2 * direction],
            send_sem=msend_sem.at[direction], recv_sem=mrecv_sem.at[direction],
            device_id={'sp': nxt if direction else prv}, device_id_type=MESH)

    def halo_copy(layer, grp, direction):
        samples = pl.ds(grp * GROUP, GROUP)
        src = pl.ds(seq if direction else EDGE, EDGE)
        dst = pl.ds(0 if direction else seq + EDGE, EDGE)
        return pltpu.make_async_remote_copy(
            src_ref=h_ext.at[layer, samples, src, :], dst_ref=h_ext.at[layer, samples, dst, :],
            send_sem=send_sem.at[layer, grp, direction], recv_sem=recv_sem.at[layer, grp, direction],
            device_id={'sp': nxt if direction else prv}, device_id_type=MESH)

    for direction in range(2):
        mask_copy(direction).start()

    def emit_h(layer, grp, resid):
        h_t = (norm(resid, 0) * tab[layer, 0] + tab[layer, 1]).astype(bf16)
        h_cm[grp] = h_t
        for blk in range(2):
            h_nat = h_t[:, blk * 128:(blk + 1) * 128].T
            for smp in range(GROUP):
                h_ext[layer, grp * GROUP + smp, EDGE + blk * QBLOCK:EDGE + (blk + 1) * QBLOCK, :] = (
                    h_nat[smp * QBLOCK:(smp + 1) * QBLOCK])
        for direction in range(2):
            halo_copy(layer, grp, direction).start()

    loads[1].wait()

    @pl.loop(0, n_groups)
    def _(grp):
        rows = act[pl.ds(grp * GROUP, GROUP)].astype(f32)
        cols = [rows[:, blk * QBLOCK:(blk + 1) * QBLOCK].reshape(128, width).T for blk in range(2)]
        resid = jnp.concatenate(cols, axis=1)
        res[grp] = resid
        emit_h(0, grp, resid)

    @pl.loop(1, n_layers)
    def _(layer):
        tables(layer)

    loads[3].wait()
    loads[4].wait()
    loads[5].wait()
    loads[6].wait()

    @pl.loop(0, n_layers)
    def _(layer):
        wv_t[layer] = wqkvg[layer, :, 2 * width:3 * width].T
        wg_t[layer] = wqkvg[layer, :, 3 * width:].T
        wo_t[layer] = wout[layer].T
        for idx in range(4):
            wu_t[layer, idx * width:(idx + 1) * width, :] = wup[layer, :, idx * width:(idx + 1) * width].T
        for idx in range(2):
            wd_t[layer, :, idx * width:(idx + 1) * width] = wdown[layer, idx * width:(idx + 1) * width, :].T

    loads[2].wait()
    pairf[...] = pair[...].astype(f32)
    for direction in range(2):
        mask_copy(direction).wait_recv()
    mask_prev = jnp.where(me > 0, mask_buf[0, 0:1, :], 0)
    mask_next = jnp.where(me < n_dev - 1, mask_buf[2, 0:1, :], 0)
    mask_own = mask_buf[1, 0:1, :]
    ext_mask = jnp.concatenate(
        [mask_prev[:, seq - EDGE:seq], mask_own[:, :seq], mask_next[:, :EDGE], jnp.zeros((1, 256 - ext), jnp.int32)], axis=1)
    ext_bias = (ext_mask.astype(f32) - 1.0) * 1e9
    wpair = wpair_ref[...].astype(f32)
    c_pair = wpair.shape[0]
    for blk in range(2):
        planes = [pairf[pl.ds(blk * QBLOCK * c_pair + chan, QBLOCK, stride=c_pair), :] for chan in range(c_pair)]
        mean = functools.reduce(jnp.add, planes) * (1.0 / c_pair)
        planes = [plane - mean for plane in planes]
        var = functools.reduce(jnp.add, [plane * plane for plane in planes]) * (1.0 / c_pair)
        rstd = lax.rsqrt(var + LN_EPS)
        planes = [(plane * rstd).astype(bf16).astype(f32) for plane in planes]
        mask_row = ext_bias[:, blk * QBLOCK:blk * QBLOCK + KEY_WINDOW]
        for layer in range(n_layers):
            heads = []
            for head in range(n_heads):
                col = layer * n_heads + head
                val = functools.reduce(jnp.add, [
                    planes[chan] * wpair[chan:chan + 1, col:col + 1] for chan in range(c_pair)])
                heads.append(val.astype(bf16).astype(f32))
            table = (jnp.concatenate(heads, axis=0) + mask_row) * LOG2E
            table = table.T
            for smp in range(GROUP):
                bias[layer, smp, blk] = table if smp == 0 else pltpu.roll(table, smp * QBLOCK, 1)

    lane = lax.broadcasted_iota(jnp.int32, (1, width), 1)
    head_of_lane = lane // head_dim
    scale = head_dim ** -0.5 * LOG2E

    def step(layer, grp, last):
        for direction in range(2):
            halo_copy(layer, grp, direction).wait_recv()
        w_qk = wqkvg[layer, :, :2 * width]
        b_q = bquery_ref[pl.ds(layer, 1), :]
        w_v = wv_t[layer]
        for smp in range(GROUP):
            h_nat = h_ext[layer, grp * GROUP + smp]
            q_k = mm(h_nat, w_qk)
            k_scr[smp] = q_k[:, width:].astype(bf16)
            q_val = (q_k[EDGE:EDGE + seq, :width] + b_q).astype(bf16)
            for blk in range(2):
                rows = q_val[blk * QBLOCK:(blk + 1) * QBLOCK]
                for slot in range(n_heads):
                    head = (slot - smp) % n_heads
                    q_scr[smp, blk * 128 + slot * QBLOCK:blk * 128 + (slot + 1) * QBLOCK, :] = jnp.where(
                        head_of_lane == head, rows, jnp.zeros_like(rows))
            v_scr[smp] = mm_nt(w_v, h_nat).astype(bf16)
        for smp in range(GROUP):
            logits = mm_nt(k_scr[smp], q_scr[smp])
            probs = []
            for blk in range(2):
                x = logits[blk * QBLOCK:blk * QBLOCK + KEY_WINDOW, blk * 128:(blk + 1) * 128] * scale + bias[layer, smp, blk]
                e = jnp.exp2(x - jnp.max(x, axis=0, keepdims=True))
                p = (e * (1.0 / jnp.sum(e, axis=0, keepdims=True))).astype(bf16)
                zero = jnp.zeros((QBLOCK, 128), bf16)
                probs.append(jnp.concatenate([zero, p] if blk else [p, zero], axis=0))
            o_t = mm(v_scr[smp], jnp.concatenate(probs, axis=1))
            for head in range(n_heads):
                slot = (head + smp) % n_heads
                rows = slice(head * head_dim, (head + 1) * head_dim)
                for blk in range(2):
                    cols = slice(blk * 128, (blk + 1) * 128)
                    part = o_t[rows, cols]
                    if smp == 0:
                        o_scr[rows, cols] = part
                    else:
                        o_scr[rows, cols] = jnp.where(lane // QBLOCK == slot, part, o_scr[rows, cols])
        gate = sigmoid(mm(wg_t[layer], h_cm[grp]))
        heads = []
        for head in range(n_heads):
            rows = slice(head * head_dim, (head + 1) * head_dim)
            parts = []
            for blk in range(2):
                part = o_scr[rows, blk * 128:(blk + 1) * 128]
                parts.append(pltpu.roll(part, (128 - head * QBLOCK) % 128, 1) if head else part)
            heads.append(jnp.concatenate(parts, axis=1))
        o_val = (gate * jnp.concatenate(heads, axis=0)).astype(bf16)
        resid = res[grp] + tab[layer, 2] * mm(wo_t[layer], o_val)
        h_t = (norm(resid, 0) * tab[layer, 3] + tab[layer, 4]).astype(bf16)
        up = mm(wu_t[layer], h_t)
        left, right = up[:2 * width], up[2 * width:]
        half = 0.5 * left
        hidden = ((half * jnp.tanh(half) + half) * right).astype(bf16)
        resid = resid + tab[layer, 5] * mm(wd_t[layer], hidden)
        if last:
            for blk in range(2):
                nat = resid[:, blk * 128:(blk + 1) * 128].T.astype(bf16)
                for smp in range(GROUP):
                    out_ref[grp * GROUP + smp, blk * QBLOCK:(blk + 1) * QBLOCK, :] = nat[smp * QBLOCK:(smp + 1) * QBLOCK]
        else:
            res[grp] = resid
            emit_h(layer + 1, grp, resid)

    @pl.loop(0, n_layers - 1)
    def _(layer):
        @pl.loop(0, n_groups)
        def _(grp):
            step(layer, grp, False)

    @pl.loop(0, n_groups)
    def _(grp):
        step(n_layers - 1, grp, True)

    for direction in range(2):
        mask_copy(direction).wait_send()

    @pl.loop(0, n_layers)
    def _(layer):
        @pl.loop(0, n_groups)
        def _(grp):
            for direction in range(2):
                halo_copy(layer, grp, direction).wait_send()


def solution(mesh):
    n_dev = mesh.shape['sp']

    def device_fn(atom_act, cond, pair, atom_mask, w_cond, b_cond, w_qkvg, b_query, w_pair, w_out, w_up, w_down):
        samples, seq, width = atom_act.shape
        n_layers = w_qkvg.shape[0]
        n_groups = samples // GROUP
        ext = seq + 2 * EDGE
        blocks, _, window, c_pair = pair.shape
        f32, bf16 = jnp.float32, jnp.bfloat16
        pair_t = pair.transpose(0, 1, 3, 2).reshape(blocks * QBLOCK * c_pair, window)
        vmem = pl.BlockSpec(memory_space=pltpu.VMEM)
        hbm = pl.BlockSpec(memory_space=pl.ANY)
        cols = GROUP * seq
        return pl.pallas_call(
            functools.partial(body, n_dev),
            out_shape=jax.ShapeDtypeStruct(atom_act.shape, bf16),
            in_specs=[hbm, vmem, hbm, vmem, hbm, vmem, hbm, vmem, vmem, hbm, hbm, hbm],
            out_specs=vmem,
            scratch_shapes=[
                pltpu.VMEM(atom_act.shape, bf16),
                pltpu.VMEM(pair_t.shape, bf16),
                pltpu.VMEM(w_cond.shape, bf16),
                pltpu.VMEM(w_qkvg.shape, bf16),
                pltpu.VMEM(w_out.shape, bf16),
                pltpu.VMEM(w_up.shape, bf16),
                pltpu.VMEM(w_down.shape, bf16),
                pltpu.VMEM(pair_t.shape, f32),
                pltpu.VMEM((n_groups, width, cols), f32),
                pltpu.VMEM((n_groups, width, cols), bf16),
                pltpu.VMEM((n_layers, samples, ext, width), bf16),
                pltpu.VMEM((n_layers, 6, width, cols), f32),
                pltpu.VMEM((n_layers, GROUP, blocks, KEY_WINDOW, 128), f32),
                pltpu.VMEM((n_layers, width, width), bf16),
                pltpu.VMEM((n_layers, width, width), bf16),
                pltpu.VMEM((n_layers, width, width), bf16),
                pltpu.VMEM((n_layers, 4 * width, width), bf16),
                pltpu.VMEM((n_layers, width, 2 * width), bf16),
                pltpu.VMEM((GROUP, ext, width), bf16),
                pltpu.VMEM((GROUP, cols, width), bf16),
                pltpu.VMEM((GROUP, width, ext), bf16),
                pltpu.VMEM((width, cols), f32),
                pltpu.VMEM((3, 8, 128), jnp.int32),
                pltpu.SemaphoreType.DMA((7,)),
                pltpu.SemaphoreType.DMA((n_layers, n_groups, 2)),
                pltpu.SemaphoreType.DMA((n_layers, n_groups, 2)),
                pltpu.SemaphoreType.DMA((2,)),
                pltpu.SemaphoreType.DMA((2,)),
            ],
            compiler_params=pltpu.CompilerParams(
                collective_id=0, has_side_effects=True, vmem_limit_bytes=60 * 1024 * 1024),
        )(atom_act, cond, pair_t, atom_mask.reshape(1, seq), w_cond, b_cond.reshape(n_layers, 1, 4 * width), w_qkvg, b_query,
          w_pair, w_out, w_up, w_down)

    act_spec = P('dp', 'sp', None)
    in_specs = (act_spec, P('sp', None), P('sp', None, None, None), P('sp'), P(), P(), P(), P(), P(), P(), P(), P())
    return jax.shard_map(device_fn, mesh=mesh, in_specs=in_specs, out_specs=act_spec, check_vma=False)
```

```python
import functools
import math

import jax
import jax.numpy as jnp
from jax import lax
from jax.experimental import pallas as pl
from jax.experimental.pallas import tpu as pltpu
from jax.sharding import PartitionSpec as P

QBLOCK = 32
KEY_WINDOW = 128
EDGE = 48
LN_EPS = 1e-5
GROUP = 4
LOG2E = math.log2(math.e)
NT = (((1,), (1,)), ((), ()))
MESH = pl.DeviceIdType.MESH


def mm(lhs, rhs):
    return jnp.dot(lhs, rhs, preferred_element_type=jnp.float32)


def mm_nt(lhs, rhs):
    return lax.dot_general(lhs, rhs, NT, preferred_element_type=jnp.float32)


def sigmoid(vals):
    return 0.5 * jnp.tanh(0.5 * vals) + 0.5


def norm(vals, axis):
    mean = jnp.mean(vals, axis=axis, keepdims=True)
    cent = vals - mean
    var = jnp.mean(cent * cent, axis=axis, keepdims=True)
    return cent * lax.rsqrt(var + LN_EPS)


def body(n_dev, act_hbm, cond_ref, pair_hbm, mask_ref, wcond_hbm, bcond_ref, wqkvg_hbm, bquery_ref, wpair_ref,
         wout_hbm, wup_hbm, wdown_hbm, out_ref,
         act, pair, wcond, wqkvg, wout, wup, wdown,
         pairf, res, h_cm, h_ext, tab, bias, wq_t, wg_t, wo_t, wu_t, wd_t, bq_t,
         k_scr, q_scr, v_scr, o_scr, r_scr, m_scr, mask_buf,
         in_sem, send_sem, recv_sem, msend_sem, mrecv_sem):
    n_layers, width = bquery_ref.shape
    n_heads = width // QBLOCK
    head_dim = width // n_heads
    n_groups = act.shape[0] // GROUP
    seq = act.shape[1]
    ext = seq + 2 * EDGE
    f32, bf16 = jnp.float32, jnp.bfloat16

    me = lax.axis_index('sp')
    nxt = lax.rem(me + 1, n_dev)
    prv = lax.rem(me + n_dev - 1, n_dev)

    loads = [pltpu.make_async_copy(src, dst, in_sem.at[pos]) for pos, (src, dst) in enumerate(
        [(wcond_hbm, wcond), (act_hbm, act), (pair_hbm, pair), (wqkvg_hbm, wqkvg),
         (wout_hbm, wout), (wup_hbm, wup), (wdown_hbm, wdown)])]
    for load in loads:
        load.start()

    barrier = pltpu.get_barrier_semaphore()
    for peer in (prv, nxt):
        pl.semaphore_signal(barrier, inc=1, device_id={'sp': peer}, device_id_type=MESH)

    mask_buf[1] = jnp.zeros_like(mask_buf[1])
    mask_buf[1, 0:1, 0:seq] = mask_ref[...]

    cond_norm = norm(cond_ref[...].astype(f32), -1).astype(bf16)
    loads[0].wait()

    def tables(layer):
        proj = mm(cond_norm, wcond[layer])
        gates = bcond_ref[pl.ds(layer, 1), :]
        pieces = []
        for idx, bias_idx in enumerate((0, None, 1, 2, None, 3)):
            piece = proj[:, idx * width:(idx + 1) * width]
            if bias_idx is not None:
                piece = sigmoid(piece + gates[:, bias_idx * width:(bias_idx + 1) * width])
            pieces.append(piece)
        for idx, piece in enumerate(pieces):
            for blk in range(2):
                rows = piece[blk * QBLOCK:(blk + 1) * QBLOCK]
                tab[layer, idx, :, blk * 128:(blk + 1) * 128] = jnp.concatenate([rows] * GROUP, axis=0).T

    tables(0)
    pl.semaphore_wait(barrier, 2)

    def mask_copy(direction):
        return pltpu.make_async_remote_copy(
            src_ref=mask_buf.at[1], dst_ref=mask_buf.at[2 - 2 * direction],
            send_sem=msend_sem.at[direction], recv_sem=mrecv_sem.at[direction],
            device_id={'sp': nxt if direction else prv}, device_id_type=MESH)

    def halo_copy(layer, grp, direction):
        samples = pl.ds(grp * GROUP, GROUP)
        src = pl.ds(seq if direction else EDGE, EDGE)
        dst = pl.ds(0 if direction else seq + EDGE, EDGE)
        return pltpu.make_async_remote_copy(
            src_ref=h_ext.at[layer, samples, src, :], dst_ref=h_ext.at[layer, samples, dst, :],
            send_sem=send_sem.at[layer, grp, direction], recv_sem=recv_sem.at[layer, grp, direction],
            device_id={'sp': nxt if direction else prv}, device_id_type=MESH)

    for direction in range(2):
        mask_copy(direction).start()

    def emit_h(layer, grp, resid):
        h_t = (norm(resid, 0) * tab[layer, 0] + tab[layer, 1]).astype(bf16)
        h_cm[grp] = h_t
        for blk in range(2):
            h_nat = h_t[:, blk * 128:(blk + 1) * 128].T
            for smp in range(GROUP):
                h_ext[layer, grp * GROUP + smp, EDGE + blk * QBLOCK:EDGE + (blk + 1) * QBLOCK, :] = (
                    h_nat[smp * QBLOCK:(smp + 1) * QBLOCK])
        for direction in range(2):
            halo_copy(layer, grp, direction).start()

    loads[1].wait()

    @pl.loop(0, n_groups)
    def _(grp):
        rows = act[pl.ds(grp * GROUP, GROUP)].astype(f32)
        cols = [rows[:, blk * QBLOCK:(blk + 1) * QBLOCK].reshape(128, width).T for blk in range(2)]
        resid = jnp.concatenate(cols, axis=1)
        res[grp] = resid
        emit_h(0, grp, resid)

    @pl.loop(1, n_layers)
    def _(layer):
        tables(layer)

    loads[3].wait()
    loads[4].wait()
    loads[5].wait()
    loads[6].wait()

    @pl.loop(0, n_layers)
    def _(layer):
        wq_t[layer] = wqkvg[layer, :, :width].T
        row = jnp.broadcast_to(bquery_ref[pl.ds(layer, 1), :], (width, width)).T
        bq_t[layer] = jnp.concatenate([row, row], axis=1)
        wg_t[layer] = wqkvg[layer, :, 3 * width:].T
        wo_t[layer] = wout[layer].T
        for idx in range(4):
            wu_t[layer, idx * width:(idx + 1) * width, :] = wup[layer, :, idx * width:(idx + 1) * width].T
        for idx in range(2):
            wd_t[layer, :, idx * width:(idx + 1) * width] = wdown[layer, idx * width:(idx + 1) * width, :].T

    loads[2].wait()
    pairf[...] = pair[...].astype(f32)
    for direction in range(2):
        mask_copy(direction).wait_recv()
    mask_prev = jnp.where(me > 0, mask_buf[0, 0:1, :], 0)
    mask_next = jnp.where(me < n_dev - 1, mask_buf[2, 0:1, :], 0)
    mask_own = mask_buf[1, 0:1, :]
    ext_mask = jnp.concatenate(
        [mask_prev[:, seq - EDGE:seq], mask_own[:, :seq], mask_next[:, :EDGE], jnp.zeros((1, 256 - ext), jnp.int32)], axis=1)
    ext_bias = (ext_mask.astype(f32) - 1.0) * 1e9
    wpair = wpair_ref[...].astype(f32)
    c_pair = wpair.shape[0]
    for blk in range(2):
        planes = [pairf[pl.ds(blk * QBLOCK * c_pair + chan, QBLOCK, stride=c_pair), :] for chan in range(c_pair)]
        mean = functools.reduce(jnp.add, planes) * (1.0 / c_pair)
        planes = [plane - mean for plane in planes]
        var = functools.reduce(jnp.add, [plane * plane for plane in planes]) * (1.0 / c_pair)
        rstd = lax.rsqrt(var + LN_EPS)
        planes = [(plane * rstd).astype(bf16).astype(f32) for plane in planes]
        mask_row = ext_bias[:, blk * QBLOCK:blk * QBLOCK + KEY_WINDOW]
        for layer in range(n_layers):
            heads = []
            for head in range(n_heads):
                col = layer * n_heads + head
                val = functools.reduce(jnp.add, [
                    planes[chan] * wpair[chan:chan + 1, col:col + 1] for chan in range(c_pair)])
                heads.append(val.astype(bf16).astype(f32))
            table = (jnp.concatenate(heads, axis=0) + mask_row) * LOG2E
            table = table.T
            for smp in range(GROUP):
                bias[layer, smp, blk] = table if smp == 0 else pltpu.roll(table, smp * QBLOCK, 1)

    lane = lax.broadcasted_iota(jnp.int32, (1, width), 1)
    scale = head_dim ** -0.5 * LOG2E

    def split(idx):
        return idx // n_groups, idx % n_groups

    def project(idx):
        layer, grp = split(idx)
        for direction in range(2):
            halo_copy(layer, grp, direction).wait_recv()
        q_t = mm(wq_t[layer], h_cm[grp])
        w_kv = wqkvg[layer, :, width:3 * width]
        yield
        for smp in range(GROUP):
            k_v = mm(h_ext[layer, grp * GROUP + smp], w_kv)
            yield
            k_scr[smp] = k_v[:, :width].astype(bf16)
            v_scr[smp] = k_v[:, width:].astype(bf16).T
            yield
            if smp == 0:
                q_t = q_t + bq_t[layer]
            heads = []
            for head in range(n_heads):
                rows = slice(head * head_dim, (head + 1) * head_dim)
                keep = lane // QBLOCK == (head + smp) % n_heads
                for blk in range(2):
                    part = q_t[rows, blk * 128:(blk + 1) * 128]
                    part = pltpu.roll(part, head * QBLOCK, 1) if head else part
                    q_scr[smp, rows, blk * 128:(blk + 1) * 128] = jnp.where(keep, part, 0.0).astype(bf16)
            yield

    def attend(idx):
        layer, grp = split(idx)
        logits = {}
        out = {}

        def score(smp):
            logits[smp] = mm(k_scr[smp], q_scr[smp])

        def soft(smp):
            probs = []
            for blk in range(2):
                x = logits[smp][blk * QBLOCK:blk * QBLOCK + KEY_WINDOW, blk * 128:(blk + 1) * 128] * scale + bias[layer, smp, blk]
                e = jnp.exp2(x - jnp.max(x, axis=0, keepdims=True))
                p = (e * (1.0 / jnp.sum(e, axis=0, keepdims=True))).astype(bf16)
                zero = jnp.zeros((QBLOCK, 128), bf16)
                probs.append(jnp.concatenate([zero, p] if blk else [p, zero], axis=0))
            out[smp] = mm(v_scr[smp], jnp.concatenate(probs, axis=1))

        def place(smp):
            for head in range(n_heads):
                slot = (head + smp) % n_heads
                rows = slice(head * head_dim, (head + 1) * head_dim)
                for blk in range(2):
                    cols = slice(blk * 128, (blk + 1) * 128)
                    part = out[smp][rows, cols]
                    if smp:
                        part = jnp.where(lane // QBLOCK == slot, part, o_scr[rows, cols])
                    o_scr[rows, cols] = part

        score(0)
        yield
        score(1)
        yield
        for smp in range(GROUP):
            soft(smp)
            yield
            if smp + 2 < GROUP:
                score(smp + 2)
            yield
            place(smp)
            yield

    def mix(idx):
        layer, grp = split(idx)
        gate = mm(wg_t[layer], h_cm[grp])
        heads = []
        for head in range(n_heads):
            rows = slice(head * head_dim, (head + 1) * head_dim)
            parts = []
            for blk in range(2):
                part = o_scr[rows, blk * 128:(blk + 1) * 128]
                parts.append(pltpu.roll(part, (128 - head * QBLOCK) % 128, 1) if head else part)
            heads.append(jnp.concatenate(parts, axis=1))
        o_val = (sigmoid(gate) * jnp.concatenate(heads, axis=0)).astype(bf16)
        proj = mm(wo_t[layer], o_val)
        yield
        resid = res[grp] + tab[layer, 2] * proj
        r_scr[...] = resid
        yield
        h_t = (norm(resid, 0) * tab[layer, 3] + tab[layer, 4]).astype(bf16)
        yield
        n_chunk = 4
        rows = 2 * width // n_chunk
        ups = {}
        for pos in range(n_chunk + 1):
            if pos < n_chunk:
                ups[pos] = [mm(wu_t[layer, pl.ds(base + pos * rows, rows), :], h_t) for base in (0, 2 * width)]
                yield
            if pos:
                left, right = ups[pos - 1]
                half = 0.5 * left
                m_scr[(pos - 1) * rows:pos * rows, :] = ((half * jnp.tanh(half) + half) * right).astype(bf16)
                yield

    def finish(idx, last):
        layer, grp = split(idx)
        resid = r_scr[...]
        down = mm(wd_t[layer], m_scr[...])
        yield
        resid = resid + tab[layer, 5] * down
        yield
        if last:
            for blk in range(2):
                nat = resid[:, blk * 128:(blk + 1) * 128].T.astype(bf16)
                for smp in range(GROUP):
                    out_ref[grp * GROUP + smp, blk * QBLOCK:(blk + 1) * QBLOCK, :] = nat[smp * QBLOCK:(smp + 1) * QBLOCK]
                yield
        else:
            res[grp] = resid
            yield
            emit_h(layer + 1, grp, resid)
            yield

    def interleave(*stages):
        stages = list(stages)
        while stages:
            for stage in list(stages):
                if next(stage, stages) is stages:
                    stages.remove(stage)

    n_steps = n_layers * n_groups
    split_at = n_steps - n_groups
    interleave(project(0))
    interleave(attend(0), project(1))
    interleave(mix(0), attend(1), project(2))

    @pl.loop(2, split_at + 2)
    def _(idx):
        interleave(finish(idx - 2, False), mix(idx - 1), attend(idx), project(idx + 1))

    @pl.loop(split_at + 2, n_steps - 1)
    def _(idx):
        interleave(finish(idx - 2, True), mix(idx - 1), attend(idx), project(idx + 1))

    interleave(finish(n_steps - 3, True), mix(n_steps - 2), attend(n_steps - 1))
    interleave(finish(n_steps - 2, True), mix(n_steps - 1))
    interleave(finish(n_steps - 1, True))

    for direction in range(2):
        mask_copy(direction).wait_send()

    @pl.loop(0, n_layers)
    def _(layer):
        @pl.loop(0, n_groups)
        def _(grp):
            for direction in range(2):
                halo_copy(layer, grp, direction).wait_send()


def solution(mesh):
    n_dev = mesh.shape['sp']

    def device_fn(atom_act, cond, pair, atom_mask, w_cond, b_cond, w_qkvg, b_query, w_pair, w_out, w_up, w_down):
        samples, seq, width = atom_act.shape
        n_layers = w_qkvg.shape[0]
        n_groups = samples // GROUP
        ext = seq + 2 * EDGE
        blocks, _, window, c_pair = pair.shape
        f32, bf16 = jnp.float32, jnp.bfloat16
        pair_t = pair.transpose(0, 1, 3, 2).reshape(blocks * QBLOCK * c_pair, window)
        vmem = pl.BlockSpec(memory_space=pltpu.VMEM)
        hbm = pl.BlockSpec(memory_space=pl.ANY)
        cols = GROUP * seq
        return pl.pallas_call(
            functools.partial(body, n_dev),
            out_shape=jax.ShapeDtypeStruct(atom_act.shape, bf16),
            in_specs=[hbm, vmem, hbm, vmem, hbm, vmem, hbm, vmem, vmem, hbm, hbm, hbm],
            out_specs=vmem,
            scratch_shapes=[
                pltpu.VMEM(atom_act.shape, bf16),
                pltpu.VMEM(pair_t.shape, bf16),
                pltpu.VMEM(w_cond.shape, bf16),
                pltpu.VMEM(w_qkvg.shape, bf16),
                pltpu.VMEM(w_out.shape, bf16),
                pltpu.VMEM(w_up.shape, bf16),
                pltpu.VMEM(w_down.shape, bf16),
                pltpu.VMEM(pair_t.shape, f32),
                pltpu.VMEM((n_groups, width, cols), f32),
                pltpu.VMEM((n_groups, width, cols), bf16),
                pltpu.VMEM((n_layers, samples, ext, width), bf16),
                pltpu.VMEM((n_layers, 6, width, cols), f32),
                pltpu.VMEM((n_layers, GROUP, blocks, KEY_WINDOW, 128), f32),
                pltpu.VMEM((n_layers, width, width), bf16),
                pltpu.VMEM((n_layers, width, width), bf16),
                pltpu.VMEM((n_layers, width, width), bf16),
                pltpu.VMEM((n_layers, 4 * width, width), bf16),
                pltpu.VMEM((n_layers, width, 2 * width), bf16),
                pltpu.VMEM((n_layers, width, cols), f32),
                pltpu.VMEM((GROUP, ext, width), bf16),
                pltpu.VMEM((GROUP, width, cols), bf16),
                pltpu.VMEM((GROUP, width, ext), bf16),
                pltpu.VMEM((width, cols), f32),
                pltpu.VMEM((width, cols), f32),
                pltpu.VMEM((2 * width, cols), bf16),
                pltpu.VMEM((3, 8, 128), jnp.int32),
                pltpu.SemaphoreType.DMA((7,)),
                pltpu.SemaphoreType.DMA((n_layers, n_groups, 2)),
                pltpu.SemaphoreType.DMA((n_layers, n_groups, 2)),
                pltpu.SemaphoreType.DMA((2,)),
                pltpu.SemaphoreType.DMA((2,)),
            ],
            compiler_params=pltpu.CompilerParams(
                collective_id=0, has_side_effects=True, vmem_limit_bytes=60 * 1024 * 1024),
        )(atom_act, cond, pair_t, atom_mask.reshape(1, seq), w_cond, b_cond, w_qkvg, b_query,
          w_pair, w_out, w_up, w_down)

    act_spec = P('dp', 'sp', None)
    in_specs = (act_spec, P('sp', None), P('sp', None, None, None), P('sp'), P(), P(), P(), P(), P(), P(), P(), P())
    return jax.shard_map(device_fn, mesh=mesh, in_specs=in_specs, out_specs=act_spec, check_vma=False)
```

```python
import functools
import math

import jax
import jax.numpy as jnp
from jax import lax
from jax.experimental import pallas as pl
from jax.experimental.pallas import tpu as pltpu
from jax.sharding import PartitionSpec as P

QBLOCK = 32
KEY_WINDOW = 128
EDGE = 48
LN_EPS = 1e-5
GROUP = 2
LOG2E = math.log2(math.e)
MESH = pl.DeviceIdType.MESH


def mm(lhs, rhs):
    return jnp.dot(lhs, rhs, preferred_element_type=jnp.float32)


def sigmoid(vals):
    return 0.5 * jnp.tanh(0.5 * vals) + 0.5


def norm(vals, axis):
    mean = jnp.mean(vals, axis=axis, keepdims=True)
    cent = vals - mean
    var = jnp.mean(cent * cent, axis=axis, keepdims=True)
    return cent * lax.rsqrt(var + LN_EPS)


def body(n_dev, act_hbm, cond_hbm, pair_hbm, mask_ref, wcond_hbm, bcond_ref, wqkvg_hbm, bquery_ref, wpair_ref,
         wout_hbm, wup_hbm, wdown_hbm, out_hbm,
         pair, wcond, wqkvg, wout, wup, wdown,
         act_in, cond_in, mask_own, mask_in, bias_own, bias_in, out_stage,
         res, h_cm, h_ext, tab, bias, wq_t, wg_t, wo_t, wu_t, wd_t, bq_t,
         k_scr, q_scr, v_nat, v_scr, o_scr, r_scr, m_scr,
         in_sem, send_sem, recv_sem, csend_sem, crecv_sem, msend_sem, mrecv_sem, asend_sem, arecv_sem,
         bsend_sem, brecv_sem, osend_sem, orecv_sem):
    n_layers, width = bquery_ref.shape
    n_heads = width // QBLOCK
    head_dim = width // n_heads
    samples, seq, _ = act_hbm.shape
    half_smp = samples // 2
    n_groups = half_smp // GROUP
    own = 2 * seq
    ext = own + 2 * EDGE
    n_blocks = own // QBLOCK
    f32, bf16 = jnp.float32, jnp.bfloat16

    me = lax.axis_index('sp')
    plane, row, core = me // 4, (me // 2) % 2, me % 2
    n_planes = n_dev // 4
    chunk = 2 * plane + core
    has_prev, has_next = chunk > 0, chunk < 2 * n_planes - 1

    def owner(chunk_idx, row_idx):
        return (chunk_idx // 2) * 4 + 2 * row_idx + chunk_idx % 2

    def remote(src, dst, ssem, rsem, peer):
        return pltpu.make_async_remote_copy(
            src_ref=src, dst_ref=dst, send_sem=ssem, recv_sem=rsem, device_id={'sp': peer}, device_id_type=MESH)

    def push(src, dst, ssem, rsem, peer):
        @pl.when(peer != me)
        def _():
            remote(src, dst, ssem, rsem, peer).start()

        @pl.when(peer == me)
        def _():
            pltpu.make_async_copy(src, dst, rsem).start()

    def push_done(src, dst, ssem, rsem, peer):
        @pl.when(peer != me)
        def _():
            remote(src, dst, ssem, rsem, peer).wait_send()

    def arrived(dst, rsem):
        pltpu.make_async_copy(dst, dst, rsem).wait()

    loads = [pltpu.make_async_copy(src, dst, in_sem.at[pos]) for pos, (src, dst) in enumerate(
        [(pair_hbm, pair), (wcond_hbm, wcond), (wqkvg_hbm, wqkvg), (wout_hbm, wout), (wup_hbm, wup), (wdown_hbm, wdown)])]
    for load in loads:
        load.start()

    zero_rows = jnp.zeros((GROUP, EDGE, width), bf16)

    @pl.loop(0, n_layers)
    def _(layer):
        @pl.loop(0, n_groups)
        def _(grp):
            h_ext[layer, pl.ds(grp * GROUP, GROUP), 0:EDGE, :] = zero_rows
            h_ext[layer, pl.ds(grp * GROUP, GROUP), EDGE + own:ext, :] = zero_rows

    mask_own[...] = jnp.zeros_like(mask_own)
    mask_own[0:1, 0:seq] = mask_ref[...]
    mask_in[0] = jnp.zeros_like(mask_own)
    mask_in[3] = jnp.zeros_like(mask_own)

    barrier = pltpu.get_barrier_semaphore()

    def greet(plane_idx, skip):
        for other in range(4):
            peer = 4 * plane_idx + other
            if skip:
                @pl.when(peer != me)
                def _():
                    pl.semaphore_signal(barrier, inc=1, device_id={'sp': peer}, device_id_type=MESH)
            else:
                pl.semaphore_signal(barrier, inc=1, device_id={'sp': peer}, device_id_type=MESH)

    greet(plane, True)

    @pl.when(plane > 0)
    def _():
        greet(plane - 1, False)

    @pl.when(plane < n_planes - 1)
    def _():
        greet(plane + 1, False)

    pl.semaphore_wait(barrier, 3 + 4 * jnp.where(plane > 0, 1, 0) + 4 * jnp.where(plane < n_planes - 1, 1, 0))

    home = 2 * plane + row

    def cond_push(half):
        return (cond_hbm, cond_in.at[pl.ds(core * seq, seq)], csend_sem.at[half], crecv_sem.at[core], owner(home, half))

    def mask_push(half):
        return (mask_own, mask_in.at[1 + core], msend_sem.at[half], mrecv_sem.at[1 + core], owner(home, half))

    side = home + 2 * core - 1
    side_slot = 3 - 3 * core
    side_ok = jnp.logical_and(side >= 0, side < 2 * n_planes)

    def mask_side(half):
        return (mask_own, mask_in.at[side_slot], msend_sem.at[2 + half], mrecv_sem.at[side_slot], owner(side, half))

    def act_push(half, grp):
        return (act_hbm.at[pl.ds(half * half_smp + grp * GROUP, GROUP)],
                act_in.at[pl.ds(grp * GROUP, GROUP), pl.ds(core * seq, seq)],
                asend_sem.at[half, grp], arecv_sem.at[core, grp], owner(home, half))

    def bias_push(half, layer):
        return (bias_own.at[layer], bias_in.at[layer, core], bsend_sem.at[half, layer], brecv_sem.at[core, layer],
                owner(home, half))

    for half in range(2):
        push(*cond_push(half))
        push(*mask_push(half))

        @pl.when(side_ok)
        def _():
            push(*mask_side(half))

    early = 3
    for grp in range(early):
        for half in range(2):
            push(*act_push(half, grp))

    c_pair = wpair_ref.shape[0]
    n_col = wpair_ref.shape[1]
    tall, deep = n_col * 16, 16 * c_pair
    pick_col = (lax.broadcasted_iota(jnp.int32, (tall, n_col), 0) // 16
                == lax.broadcasted_iota(jnp.int32, (tall, n_col), 1)).astype(bf16)
    pick_chan = (lax.broadcasted_iota(jnp.int32, (c_pair, deep), 1) % c_pair
                 == lax.broadcasted_iota(jnp.int32, (c_pair, deep), 0)).astype(bf16)
    spread = lax.dot_general(
        wpair_ref[...], pick_chan, (((0,), (0,)), ((), ())), preferred_element_type=f32).astype(bf16)
    spread = mm(pick_col, spread)
    same = (lax.broadcasted_iota(jnp.int32, (tall, deep), 0) % 16 == lax.broadcasted_iota(jnp.int32, (tall, deep), 1) // c_pair)
    w_block = jnp.where(same, spread, 0.0).astype(bf16)
    loads[0].wait()
    for part in range(seq // 16):
        vals = pair[part * deep:(part + 1) * deep].astype(f32).reshape(16, c_pair, KEY_WINDOW)
        vals = norm(vals, 1).astype(bf16).reshape(deep, KEY_WINDOW)
        res_bias = mm(w_block, vals).astype(bf16)
        blk, sub = part // 2, part % 2
        for layer in range(n_layers):
            for head in range(n_heads):
                col = layer * n_heads + head
                bias_own[layer, blk, head * QBLOCK + sub * 16:head * QBLOCK + (sub + 1) * 16, :] = res_bias[col * 16:(col + 1) * 16]
    for half in range(2):
        push(*bias_push(half, 0))
    for grp in range(early, n_groups):
        for half in range(2):
            push(*act_push(half, grp))
    for layer in range(1, n_layers):
        for half in range(2):
            push(*bias_push(half, layer))

    for slot in range(2):
        arrived(cond_in.at[pl.ds(slot * seq, seq)], crecv_sem.at[slot])
    cond_norm = norm(cond_in[...].astype(f32), -1).astype(bf16)
    loads[1].wait()

    def tables(layer):
        proj = mm(cond_norm, wcond[layer])
        gates = bcond_ref[pl.ds(layer, 1), :]
        for idx, bias_idx in enumerate((0, None, 1, 2, None, 3)):
            piece = proj[:, idx * width:(idx + 1) * width]
            if bias_idx is not None:
                piece = sigmoid(piece + gates[:, bias_idx * width:(bias_idx + 1) * width])
            tab[layer, idx] = piece.T

    tables(0)

    def both(vals):
        return jnp.concatenate([vals] * GROUP, axis=1)

    def halo_copy(layer, grp, direction):
        smp = pl.ds(grp * GROUP, GROUP)
        src = pl.ds(own if direction else EDGE, EDGE)
        dst = pl.ds(0 if direction else own + EDGE, EDGE)
        return remote(h_ext.at[layer, smp, src, :], h_ext.at[layer, smp, dst, :],
                      send_sem.at[layer, grp, direction], recv_sem.at[layer, grp, direction],
                      owner(chunk + 1 if direction else chunk - 1, row))

    def halo_start(layer, grp):
        @pl.when(has_prev)
        def _():
            halo_copy(layer, grp, 0).start()

        @pl.when(has_next)
        def _():
            halo_copy(layer, grp, 1).start()

    def halo_wait(layer, grp):
        @pl.when(has_next)
        def _():
            halo_copy(layer, grp, 0).wait_recv()

        @pl.when(has_prev)
        def _():
            halo_copy(layer, grp, 1).wait_recv()

    def emit_h(layer, grp, resid):
        h_t = (norm(resid, 0) * both(tab[layer, 0]) + both(tab[layer, 1])).astype(bf16)
        h_cm[grp] = h_t
        for smp in range(GROUP):
            h_ext[layer, grp * GROUP + smp, EDGE:EDGE + own, :] = h_t[:, smp * own:(smp + 1) * own].T

    def enter(grp):
        for slot in range(2):
            arrived(act_in.at[pl.ds(grp * GROUP, GROUP), pl.ds(slot * seq, seq)], arecv_sem.at[slot, grp])
        cols = [act_in[grp * GROUP + smp].T.astype(f32) for smp in range(GROUP)]
        resid = jnp.concatenate(cols, axis=1)
        res[grp] = resid
        emit_h(0, grp, resid)
        halo_start(0, grp)

    def weights(layer):
        wq_t[layer] = wqkvg[layer, :, :width].T
        bq_t[layer] = jnp.broadcast_to(bquery_ref[pl.ds(layer, 1), :], (width, width)).T
        wg_t[layer] = wqkvg[layer, :, 3 * width:].T
        wo_t[layer] = wout[layer].T
        for idx in range(4):
            wu_t[layer, idx * width:(idx + 1) * width, :] = wup[layer, :, idx * width:(idx + 1) * width].T
        for idx in range(2):
            wd_t[layer, :, idx * width:(idx + 1) * width] = wdown[layer, idx * width:(idx + 1) * width, :].T

    def bias_table(layer, mask_bias):
        for slot in range(2):
            arrived(bias_in.at[layer, slot], brecv_sem.at[slot, layer])
        for blk in range(n_blocks):
            nat = bias_in[layer, blk // 2, blk % 2].astype(f32)
            order = [(slot - blk) % n_heads for slot in range(n_heads)]
            nat = jnp.concatenate([nat[head * QBLOCK:(head + 1) * QBLOCK] for head in order], axis=0)
            bias[layer, blk] = ((nat + mask_bias[:, blk * QBLOCK:blk * QBLOCK + KEY_WINDOW]) * LOG2E).T

    enter(0)
    for load in loads[2:]:
        load.wait()
    weights(0)

    @pl.loop(1, 4)
    def _(grp):
        enter(grp)

    @pl.loop(1, n_layers)
    def _(layer):
        weights(layer)
        tables(layer)

    for slot in range(1, 3):
        arrived(mask_in.at[slot], mrecv_sem.at[slot])

    @pl.when(has_prev)
    def _():
        arrived(mask_in.at[0], mrecv_sem.at[0])

    @pl.when(has_next)
    def _():
        arrived(mask_in.at[3], mrecv_sem.at[3])

    mask_row = jnp.concatenate([mask_in[0, 0:1, seq - EDGE:seq], mask_in[1, 0:1, :seq], mask_in[2, 0:1, :seq],
                                mask_in[3, 0:1, :EDGE], jnp.zeros((1, 256 - ext), jnp.int32)], axis=1)
    mask_bias = (mask_row.astype(f32) - 1.0) * 1e9
    bias_table(0, mask_bias)

    @pl.loop(4, n_groups)
    def _(grp):
        enter(grp)

    for layer in range(1, n_layers):
        bias_table(layer, mask_bias)

    lane = lax.broadcasted_iota(jnp.int32, (1, width), 1)
    scale = head_dim ** -0.5 * LOG2E

    def split(idx):
        return idx // n_groups, idx % n_groups

    def project(idx):
        layer, grp = split(idx)
        q_t = mm(wq_t[layer], h_cm[grp])
        w_kv = wqkvg[layer, :, width:3 * width]
        yield
        for smp in range(GROUP):
            k_v = mm(h_ext[layer, grp * GROUP + smp], w_kv)
            yield
            k_scr[smp] = k_v[:, :width].astype(bf16)
            v_nat[smp] = k_v[:, width:].astype(bf16)
            yield
            if smp == 0:
                q_t = q_t + both(bq_t[layer])
            for head in range(n_heads):
                rows = slice(head * head_dim, (head + 1) * head_dim)
                part = q_t[rows, smp * own:(smp + 1) * own]
                part = pltpu.roll(part, head * QBLOCK, 1) if head else part
                for blk in range(n_blocks):
                    keep = lane // QBLOCK == (head + blk) % n_heads
                    q_scr[smp, rows, blk * 128:(blk + 1) * 128] = jnp.where(keep, part, 0.0).astype(bf16)
                if head % 2:
                    yield
            yield
            v_scr[smp] = v_nat[smp].T
            yield

    def attend(idx):
        layer, grp = split(idx)
        logits = {}
        out = {}

        def score(unit):
            smp, duo = unit // 2, unit % 2
            logits[unit] = mm(k_scr[smp, duo * 64:duo * 64 + 160], q_scr[smp, :, duo * 256:(duo + 1) * 256])

        def soft(unit):
            smp, duo = unit // 2, unit % 2
            probs = []
            for sub in range(2):
                blk = 2 * duo + sub
                x = logits[unit][sub * QBLOCK:sub * QBLOCK + KEY_WINDOW, sub * 128:(sub + 1) * 128] * scale + bias[layer, blk]
                e = jnp.exp2(x - jnp.max(x, axis=0, keepdims=True))
                p = (e * (1.0 / jnp.sum(e, axis=0, keepdims=True))).astype(bf16)
                parts = [p]
                if blk:
                    parts = [jnp.zeros((blk * QBLOCK, 128), bf16)] + parts
                if blk < n_blocks - 1:
                    parts = parts + [jnp.zeros(((n_blocks - 1 - blk) * QBLOCK, 128), bf16)]
                probs.append(jnp.concatenate(parts, axis=0))
            out[unit] = mm(v_scr[smp], jnp.concatenate(probs, axis=1))

        def place(unit):
            smp, duo = unit // 2, unit % 2
            cols = slice(smp * own, (smp + 1) * own)
            for head in range(n_heads):
                rows = slice(head * head_dim, (head + 1) * head_dim)
                for sub in range(2):
                    blk = 2 * duo + sub
                    part = out[unit][rows, sub * 128:(sub + 1) * 128]
                    if blk:
                        part = jnp.where(lane // QBLOCK == (head + blk) % n_heads, part, o_scr[rows, cols])
                    o_scr[rows, cols] = part

        score(0)
        yield
        score(1)
        yield
        for unit in range(2 * GROUP):
            soft(unit)
            yield
            if unit + 2 < 2 * GROUP:
                score(unit + 2)
            yield
            place(unit)
            yield

    def mix(idx):
        layer, grp = split(idx)
        gate = mm(wg_t[layer], h_cm[grp])
        heads = []
        for head in range(n_heads):
            rows = slice(head * head_dim, (head + 1) * head_dim)
            parts = []
            for smp in range(GROUP):
                part = o_scr[rows, smp * own:(smp + 1) * own]
                parts.append(pltpu.roll(part, (128 - head * QBLOCK) % 128, 1) if head else part)
            heads.append(jnp.concatenate(parts, axis=1))
        o_val = (sigmoid(gate) * jnp.concatenate(heads, axis=0)).astype(bf16)
        proj = mm(wo_t[layer], o_val)
        yield
        resid = res[grp] + both(tab[layer, 2]) * proj
        r_scr[...] = resid
        yield
        h_t = (norm(resid, 0) * both(tab[layer, 3]) + both(tab[layer, 4])).astype(bf16)
        yield
        n_chunk = 4
        rows = 2 * width // n_chunk
        ups = {}
        for pos in range(n_chunk + 1):
            if pos < n_chunk:
                ups[pos] = [mm(wu_t[layer, pl.ds(base + pos * rows, rows), :], h_t) for base in (0, 2 * width)]
                yield
            if pos:
                left, right = ups[pos - 1]
                gated = 0.5 * left
                m_scr[(pos - 1) * rows:pos * rows, :] = ((gated * jnp.tanh(gated) + gated) * right).astype(bf16)
                yield

    def finish(idx, last):
        layer, grp = split(idx)
        resid = r_scr[...]
        down = mm(wd_t[layer], m_scr[...])
        yield
        resid = resid + both(tab[layer, 5]) * down
        yield
        if last:
            for smp in range(GROUP):
                out_stage[grp * GROUP + smp] = resid[:, smp * own:(smp + 1) * own].astype(bf16).T
                yield
        else:
            res[grp] = resid
            yield
            emit_h(layer + 1, grp, resid)
            yield

    def out_push(grp, slot):
        return (out_stage.at[pl.ds(grp * GROUP, GROUP), pl.ds(slot * seq, seq)],
                out_hbm.at[pl.ds(row * half_smp + grp * GROUP, GROUP)],
                osend_sem.at[slot, grp], orecv_sem.at[row, grp], 4 * plane + 2 * core + slot)

    def sent(idx, last):
        layer, grp = split(idx)
        if last:
            for slot in range(2):
                push(*out_push(grp, slot))
        else:
            halo_start(layer + 1, grp)

    def interleave(*stages):
        stages = list(stages)
        while stages:
            for stage in list(stages):
                if next(stage, stages) is stages:
                    stages.remove(stage)

    n_steps = n_layers * n_groups
    split_at = n_steps - n_groups
    halo_wait(0, 0)
    interleave(project(0))
    halo_wait(0, 1)
    interleave(attend(0), project(1))
    halo_wait(0, 2)
    interleave(mix(0), attend(1), project(2))

    @pl.loop(2, split_at + 2)
    def _(idx):
        halo_wait(*split(idx + 1))
        interleave(finish(idx - 2, False), mix(idx - 1), attend(idx), project(idx + 1))
        sent(idx - 2, False)

    @pl.loop(split_at + 2, n_steps - 1)
    def _(idx):
        halo_wait(*split(idx + 1))
        interleave(finish(idx - 2, True), mix(idx - 1), attend(idx), project(idx + 1))
        sent(idx - 2, True)

    interleave(finish(n_steps - 3, True), mix(n_steps - 2), attend(n_steps - 1))
    sent(n_steps - 3, True)
    interleave(finish(n_steps - 2, True), mix(n_steps - 1))
    sent(n_steps - 2, True)
    interleave(finish(n_steps - 1, True))
    sent(n_steps - 1, True)

    for half in range(2):
        push_done(*cond_push(half))
        push_done(*mask_push(half))

        @pl.when(side_ok)
        def _():
            push_done(*mask_side(half))

        @pl.loop(0, n_layers)
        def _(layer):
            push_done(*bias_push(half, layer))

        @pl.loop(0, n_groups)
        def _(grp):
            push_done(*act_push(half, grp))
            push_done(*out_push(grp, half))

    @pl.loop(0, n_layers)
    def _(layer):
        @pl.loop(0, n_groups)
        def _(grp):
            @pl.when(has_prev)
            def _():
                halo_copy(layer, grp, 0).wait_send()

            @pl.when(has_next)
            def _():
                halo_copy(layer, grp, 1).wait_send()

    for half in range(2):
        @pl.loop(0, n_groups)
        def _(grp):
            arrived(out_hbm.at[pl.ds(half * half_smp + grp * GROUP, GROUP)], orecv_sem.at[half, grp])


def solution(mesh):
    n_dev = mesh.shape['sp']

    def device_fn(atom_act, cond, pair, atom_mask, w_cond, b_cond, w_qkvg, b_query, w_pair, w_out, w_up, w_down):
        samples, seq, width = atom_act.shape
        n_layers = w_qkvg.shape[0]
        n_heads = width // QBLOCK
        half_smp = samples // 2
        n_groups = half_smp // GROUP
        own = 2 * seq
        ext = own + 2 * EDGE
        n_blocks = own // QBLOCK
        blocks, _, window, c_pair = pair.shape
        f32, bf16 = jnp.float32, jnp.bfloat16
        pair_t = pair.transpose(0, 1, 3, 2).reshape(blocks * QBLOCK * c_pair, window)
        vmem = pl.BlockSpec(memory_space=pltpu.VMEM)
        hbm = pl.BlockSpec(memory_space=pl.ANY)
        cols = GROUP * own
        dma = pltpu.SemaphoreType.DMA
        return pl.pallas_call(
            functools.partial(body, n_dev),
            out_shape=jax.ShapeDtypeStruct(atom_act.shape, bf16),
            in_specs=[hbm, hbm, hbm, vmem, hbm, vmem, hbm, vmem, vmem, hbm, hbm, hbm],
            out_specs=hbm,
            scratch_shapes=[
                pltpu.VMEM(pair_t.shape, bf16),
                pltpu.VMEM(w_cond.shape, bf16),
                pltpu.VMEM(w_qkvg.shape, bf16),
                pltpu.VMEM(w_out.shape, bf16),
                pltpu.VMEM(w_up.shape, bf16),
                pltpu.VMEM(w_down.shape, bf16),
                pltpu.VMEM((half_smp, own, width), bf16),
                pltpu.VMEM((own, width), bf16),
                pltpu.VMEM((8, 128), jnp.int32),
                pltpu.VMEM((4, 8, 128), jnp.int32),
                pltpu.VMEM((n_layers, blocks, n_heads * QBLOCK, window), bf16),
                pltpu.VMEM((n_layers, 2, blocks, n_heads * QBLOCK, window), bf16),
                pltpu.VMEM((half_smp, own, width), bf16),
                pltpu.VMEM((n_groups, width, cols), f32),
                pltpu.VMEM((n_groups, width, cols), bf16),
                pltpu.VMEM((n_layers, half_smp, ext, width), bf16),
                pltpu.VMEM((n_layers, 6, width, own), f32),
                pltpu.VMEM((n_layers, n_blocks, KEY_WINDOW, 128), f32),
                pltpu.VMEM((n_layers, width, width), bf16),
                pltpu.VMEM((n_layers, width, width), bf16),
                pltpu.VMEM((n_layers, width, width), bf16),
                pltpu.VMEM((n_layers, 4 * width, width), bf16),
                pltpu.VMEM((n_layers, width, 2 * width), bf16),
                pltpu.VMEM((n_layers, width, width), f32),
                pltpu.VMEM((GROUP, ext, width), bf16),
                pltpu.VMEM((GROUP, width, n_blocks * 128), bf16),
                pltpu.VMEM((GROUP, ext, width), bf16),
                pltpu.VMEM((GROUP, width, ext), bf16),
                pltpu.VMEM((width, cols), f32),
                pltpu.VMEM((width, cols), f32),
                pltpu.VMEM((2 * width, cols), bf16),
                dma((6,)),
                dma((n_layers, n_groups, 2)),
                dma((n_layers, n_groups, 2)),
                dma((2,)),
                dma((2,)),
                dma((4,)),
                dma((4,)),
                dma((2, n_groups)),
                dma((2, n_groups)),
                dma((2, n_layers)),
                dma((2, n_layers)),
                dma((2, n_groups)),
                dma((2, n_groups)),
            ],
            compiler_params=pltpu.CompilerParams(
                collective_id=0, has_side_effects=True, vmem_limit_bytes=60 * 1024 * 1024),
        )(atom_act, cond, pair_t, atom_mask.reshape(1, seq), w_cond, b_cond, w_qkvg, b_query,
          w_pair, w_out, w_up, w_down)

    act_spec = P('dp', 'sp', None)
    in_specs = (act_spec, P('sp', None), P('sp', None, None, None), P('sp'), P(), P(), P(), P(), P(), P(), P(), P())
    return jax.shard_map(device_fn, mesh=mesh, in_specs=in_specs, out_specs=act_spec, check_vma=False)
```

```python
import functools
import math

import jax
import jax.numpy as jnp
from jax import lax
from jax.experimental import pallas as pl
from jax.experimental.pallas import tpu as pltpu
from jax.sharding import PartitionSpec as P

QBLOCK = 32
KEY_WINDOW = 128
EDGE = 48
LN_EPS = 1e-5
GROUP = 2
LOG2E = math.log2(math.e)
MESH = pl.DeviceIdType.MESH


def mm(lhs, rhs):
    return jnp.dot(lhs, rhs, preferred_element_type=jnp.float32)


def sigmoid(vals):
    return 0.5 * jnp.tanh(0.5 * vals) + 0.5


def norm(vals, axis):
    mean = jnp.mean(vals, axis=axis, keepdims=True)
    cent = vals - mean
    var = jnp.mean(cent * cent, axis=axis, keepdims=True)
    return cent * lax.rsqrt(var + LN_EPS)


def body(n_dev, act_hbm, cond_hbm, pair_hbm, mask_ref, wcond_hbm, bcond_ref, wqkvg_hbm, bquery_ref, wpair_ref,
         wout_hbm, wup_hbm, wdown_hbm, out_hbm,
         pair, wcond, wqkvg, wout, wup, wdown,
         act_in, cond_in, mask_own, mask_in, bias_own, bias_in, out_stage,
         res, h_cm, h_ext, tab, bias, wq_t, wg_t, wo_t, wu_t, wd_t, bq_t,
         k_scr, q_scr, v_nat, v_scr, o_scr, s_scr, m_scr,
         in_sem, send_sem, recv_sem, csend_sem, crecv_sem, msend_sem, mrecv_sem, asend_sem, arecv_sem,
         bsend_sem, brecv_sem, osend_sem, orecv_sem):
    n_layers, width = bquery_ref.shape
    n_heads = width // QBLOCK
    head_dim = width // n_heads
    samples, seq, _ = act_hbm.shape
    half_smp = samples // 2
    n_groups = half_smp // GROUP
    own = 2 * seq
    ext = own + 2 * EDGE
    n_blocks = own // QBLOCK
    f32, bf16 = jnp.float32, jnp.bfloat16

    me = lax.axis_index('sp')
    plane, row, core = me // 4, (me // 2) % 2, me % 2
    n_planes = n_dev // 4
    chunk = 2 * plane + core
    has_prev, has_next = chunk > 0, chunk < 2 * n_planes - 1

    def owner(chunk_idx, row_idx):
        return (chunk_idx // 2) * 4 + 2 * row_idx + chunk_idx % 2

    def remote(src, dst, ssem, rsem, peer):
        return pltpu.make_async_remote_copy(
            src_ref=src, dst_ref=dst, send_sem=ssem, recv_sem=rsem, device_id={'sp': peer}, device_id_type=MESH)

    def push(src, dst, ssem, rsem, peer):
        @pl.when(peer != me)
        def _():
            remote(src, dst, ssem, rsem, peer).start()

        @pl.when(peer == me)
        def _():
            pltpu.make_async_copy(src, dst, rsem).start()

    def push_done(src, dst, ssem, rsem, peer):
        @pl.when(peer != me)
        def _():
            remote(src, dst, ssem, rsem, peer).wait_send()

    def arrived(dst, rsem):
        pltpu.make_async_copy(dst, dst, rsem).wait()

    loads = [pltpu.make_async_copy(src, dst, in_sem.at[pos]) for pos, (src, dst) in enumerate(
        [(pair_hbm, pair), (wcond_hbm, wcond), (wqkvg_hbm, wqkvg), (wout_hbm, wout), (wup_hbm, wup), (wdown_hbm, wdown)])]
    for load in loads:
        load.start()

    zero_rows = jnp.zeros((GROUP, EDGE, width), bf16)

    @pl.loop(0, n_layers)
    def _(layer):
        @pl.loop(0, n_groups)
        def _(grp):
            h_ext[layer, pl.ds(grp * GROUP, GROUP), 0:EDGE, :] = zero_rows
            h_ext[layer, pl.ds(grp * GROUP, GROUP), EDGE + own:ext, :] = zero_rows

    mask_own[...] = jnp.zeros_like(mask_own)
    mask_own[0:1, 0:seq] = mask_ref[...]
    mask_in[0] = jnp.zeros_like(mask_own)
    mask_in[3] = jnp.zeros_like(mask_own)

    barrier = pltpu.get_barrier_semaphore()

    for other in range(4):
        peer = 4 * plane + other

        @pl.when(peer != me)
        def _():
            pl.semaphore_signal(barrier, inc=1, device_id={'sp': peer}, device_id_type=MESH)

    beyond = chunk + 2 * core - 1
    has_beyond = jnp.logical_and(beyond >= 0, beyond < 2 * n_planes)

    @pl.when(has_beyond)
    def _():
        pl.semaphore_signal(barrier, inc=1, device_id={'sp': owner(beyond, row)}, device_id_type=MESH)

    home = 2 * plane + row

    def cond_push(half):
        return (cond_hbm, cond_in.at[pl.ds(core * seq, seq)], csend_sem.at[half], crecv_sem.at[core], owner(home, half))

    def mask_push(half):
        return (mask_own, mask_in.at[1 + core], msend_sem.at[half], mrecv_sem.at[1 + core], owner(home, half))

    def mask_side(direction):
        return remote(mask_in.at[1 + direction], mask_in.at[3 - 3 * direction], msend_sem.at[2 + direction],
                      mrecv_sem.at[3 - 3 * direction], owner(chunk + 2 * direction - 1, row))

    def act_push(half, grp):
        return (act_hbm.at[pl.ds(half * half_smp + grp * GROUP, GROUP)],
                act_in.at[pl.ds(grp * GROUP, GROUP), pl.ds(core * seq, seq)],
                asend_sem.at[half, grp], arecv_sem.at[core, grp], owner(home, half))

    def bias_push(half, layer):
        return (bias_own.at[layer], bias_in.at[layer, core], bsend_sem.at[half, layer], brecv_sem.at[core, layer],
                owner(home, half))

    c_pair = wpair_ref.shape[0]
    n_col = wpair_ref.shape[1]
    tall, deep = n_col * 16, 16 * c_pair
    pick_col = (lax.broadcasted_iota(jnp.int32, (tall, n_col), 0) // 16
                == lax.broadcasted_iota(jnp.int32, (tall, n_col), 1)).astype(bf16)
    pick_chan = (lax.broadcasted_iota(jnp.int32, (c_pair, deep), 1) % c_pair
                 == lax.broadcasted_iota(jnp.int32, (c_pair, deep), 0)).astype(bf16)
    spread = lax.dot_general(
        wpair_ref[...], pick_chan, (((0,), (0,)), ((), ())), preferred_element_type=f32).astype(bf16)
    spread = mm(pick_col, spread)
    same = (lax.broadcasted_iota(jnp.int32, (tall, deep), 0) % 16 == lax.broadcasted_iota(jnp.int32, (tall, deep), 1) // c_pair)
    w_block = jnp.where(same, spread, 0.0).astype(bf16)
    loads[0].wait()
    for part in range(seq // 16):
        vals = pair[part * deep:(part + 1) * deep].astype(f32).reshape(16, c_pair, KEY_WINDOW)
        vals = norm(vals, 1).astype(bf16).reshape(deep, KEY_WINDOW)
        res_bias = mm(w_block, vals).astype(bf16)
        blk, sub = part // 2, part % 2
        for layer in range(n_layers):
            for head in range(n_heads):
                col = layer * n_heads + head
                bias_own[layer, blk, head * QBLOCK + sub * 16:head * QBLOCK + (sub + 1) * 16, :] = res_bias[col * 16:(col + 1) * 16]
    def weights(layer):
        wq_t[layer] = wqkvg[layer, :, :width].T
        bq_t[layer] = jnp.broadcast_to(bquery_ref[pl.ds(layer, 1), :], (width, width)).T
        wg_t[layer] = wqkvg[layer, :, 3 * width:].T
        wo_t[layer] = wout[layer].T
        for idx in range(4):
            wu_t[layer, idx * width:(idx + 1) * width, :] = wup[layer, :, idx * width:(idx + 1) * width].T
        for idx in range(2):
            wd_t[layer, :, idx * width:(idx + 1) * width] = wdown[layer, idx * width:(idx + 1) * width, :].T

    for load in loads[2:]:
        load.wait()

    @pl.loop(0, n_layers)
    def _(layer):
        weights(layer)

    n_beyond = jnp.where(has_beyond, 1, 0)
    pl.semaphore_wait(barrier, 3 + n_beyond)

    for half in range(2):
        push(*cond_push(half))
    for grp in range(3):
        for half in range(2):
            push(*act_push(half, grp))
        if grp == 0:
            for half in range(2):
                push(*mask_push(half))
    for half in range(2):
        push(*bias_push(half, 0))
    for grp in range(3, n_groups):
        for half in range(2):
            push(*act_push(half, grp))
    for layer in range(1, n_layers):
        for half in range(2):
            push(*bias_push(half, layer))

    for slot in range(2):
        arrived(cond_in.at[pl.ds(slot * seq, seq)], crecv_sem.at[slot])
    cond_norm = norm(cond_in[...].astype(f32), -1).astype(bf16)
    loads[1].wait()

    def tables(layer):
        proj = mm(cond_norm, wcond[layer])
        gates = bcond_ref[pl.ds(layer, 1), :]
        for idx, bias_idx in enumerate((0, None, 1, 2, None, 3)):
            piece = proj[:, idx * width:(idx + 1) * width]
            if bias_idx is not None:
                piece = sigmoid(piece + gates[:, bias_idx * width:(bias_idx + 1) * width])
            tab[layer, idx] = piece.T

    def both(vals):
        return jnp.concatenate([vals] * GROUP, axis=1)

    def halo_copy(layer, grp, direction):
        smp = pl.ds(grp * GROUP, GROUP)
        src = pl.ds(own if direction else EDGE, EDGE)
        dst = pl.ds(0 if direction else own + EDGE, EDGE)
        return remote(h_ext.at[layer, smp, src, :], h_ext.at[layer, smp, dst, :],
                      send_sem.at[layer, grp, direction], recv_sem.at[layer, grp, direction],
                      owner(chunk + 1 if direction else chunk - 1, row))

    def halo_start(layer, grp):
        @pl.when(has_prev)
        def _():
            halo_copy(layer, grp, 0).start()

        @pl.when(has_next)
        def _():
            halo_copy(layer, grp, 1).start()

    def halo_wait(layer, grp):
        @pl.when(has_next)
        def _():
            halo_copy(layer, grp, 0).wait_recv()

        @pl.when(has_prev)
        def _():
            halo_copy(layer, grp, 1).wait_recv()

    def emit_h(layer, grp, resid):
        h_t = (norm(resid, 0) * both(tab[layer, 0]) + both(tab[layer, 1])).astype(bf16)
        h_cm[grp] = h_t
        for smp in range(GROUP):
            h_ext[layer, grp * GROUP + smp, EDGE:EDGE + own, :] = h_t[:, smp * own:(smp + 1) * own].T

    def act_wait(grp):
        for slot in range(2):
            arrived(act_in.at[pl.ds(grp * GROUP, GROUP), pl.ds(slot * seq, seq)], arecv_sem.at[slot, grp])

    def enter(grp):
        cols = [act_in[grp * GROUP + smp].T.astype(f32) for smp in range(GROUP)]
        yield
        resid = jnp.concatenate(cols, axis=1)
        res[grp] = resid
        yield
        emit_h(0, grp, resid)
        yield

    def enter_now(grp):
        act_wait(grp)
        for _ in enter(grp):
            pass
        halo_start(0, grp)

    def bias_wait(layer):
        for slot in range(2):
            arrived(bias_in.at[layer, slot], brecv_sem.at[slot, layer])

    def bias_table(layer, mask_bias):
        for blk in range(n_blocks):
            nat = bias_in[layer, blk // 2, blk % 2].astype(f32)
            order = [(slot - blk) % n_heads for slot in range(n_heads)]
            nat = jnp.concatenate([nat[head * QBLOCK:(head + 1) * QBLOCK] for head in order], axis=0)
            bias[layer, blk] = ((nat + mask_bias[:, blk * QBLOCK:blk * QBLOCK + KEY_WINDOW]) * LOG2E).T
            yield

    tables(0)
    enter_now(0)
    tables(1)
    enter_now(1)
    tables(2)
    for slot in range(1, 3):
        arrived(mask_in.at[slot], mrecv_sem.at[slot])

    @pl.when(has_prev)
    def _():
        mask_side(0).start()

    @pl.when(has_next)
    def _():
        mask_side(1).start()

    enter_now(2)
    @pl.when(has_prev)
    def _():
        arrived(mask_in.at[0], mrecv_sem.at[0])

    @pl.when(has_next)
    def _():
        arrived(mask_in.at[3], mrecv_sem.at[3])

    mask_row = jnp.concatenate([mask_in[0, 0:1, seq - EDGE:seq], mask_in[1, 0:1, :seq], mask_in[2, 0:1, :seq],
                                mask_in[3, 0:1, :EDGE], jnp.zeros((1, 256 - ext), jnp.int32)], axis=1)
    mask_bias = (mask_row.astype(f32) - 1.0) * 1e9
    bias_wait(0)
    for _ in bias_table(0, mask_bias):
        pass
    enter_now(3)

    lane = lax.broadcasted_iota(jnp.int32, (1, width), 1)
    scale = head_dim ** -0.5 * LOG2E
    keep = [jnp.where(lane // QBLOCK == slot, 1.0, 0.0).astype(bf16) for slot in range(n_heads)]

    def split(idx):
        return idx // n_groups, idx % n_groups

    def project(idx):
        layer, grp = split(idx)
        w_kv = wqkvg[layer, :, width:3 * width]
        k_v = {0: mm(h_ext[layer, grp * GROUP], w_kv)}
        yield
        q_t = mm(wq_t[layer], h_cm[grp])
        yield
        k_v[1] = mm(h_ext[layer, grp * GROUP + 1], w_kv)
        yield
        yield from idle(2)
        for smp in range(GROUP):
            k_scr[smp] = k_v[smp][:, :width].astype(bf16)
            v_nat[smp] = k_v[smp][:, width:].astype(bf16)
            yield
            for head in range(n_heads):
                rows = slice(head * head_dim, (head + 1) * head_dim)
                part = q_t[rows, smp * own:(smp + 1) * own] + bq_t[layer, rows]
                part = (pltpu.roll(part, head * QBLOCK, 1) if head else part).astype(bf16)
                for blk in range(n_blocks):
                    q_scr[smp, rows, blk * 128:(blk + 1) * 128] = part * keep[(head + blk) % n_heads]
                if head % 2:
                    yield
            v_scr[smp] = v_nat[smp].T
            yield
            if smp == 0:
                yield from idle(2)

    def score(unit):
        smp, duo = unit // 2, unit % 2
        return mm(k_scr[smp, duo * 64:duo * 64 + 160], q_scr[smp, :, duo * 256:(duo + 1) * 256])

    def score_early():
        for unit in range(2):
            logit = score(unit)
            yield
            for sub in range(2):
                s_scr[unit, sub] = logit[sub * QBLOCK:sub * QBLOCK + KEY_WINDOW, sub * 128:(sub + 1) * 128]
            yield

    def attend(idx):
        layer, grp = split(idx)
        logits = {}
        out = {}

        def prob(unit, sub):
            blk = 2 * (unit % 2) + sub
            if unit < 2:
                x = s_scr[unit, sub]
            else:
                x = logits[unit][sub * QBLOCK:sub * QBLOCK + KEY_WINDOW, sub * 128:(sub + 1) * 128]
            x = x * scale + bias[layer, blk]
            e = jnp.exp2(x - jnp.max(x, axis=0, keepdims=True))
            p = (e * (1.0 / jnp.sum(e, axis=0, keepdims=True))).astype(bf16)
            parts = [p]
            if blk:
                parts = [jnp.zeros((blk * QBLOCK, 128), bf16)] + parts
            if blk < n_blocks - 1:
                parts = parts + [jnp.zeros(((n_blocks - 1 - blk) * QBLOCK, 128), bf16)]
            return jnp.concatenate(parts, axis=0)

        def place(unit):
            smp, duo = unit // 2, unit % 2
            cols = slice(smp * own, (smp + 1) * own)
            for head in range(n_heads):
                rows = slice(head * head_dim, (head + 1) * head_dim)
                pair_out = [out[unit][rows, sub * 128:(sub + 1) * 128] for sub in range(2)]
                pick = lane // QBLOCK == (head + 2 * duo + 1) % n_heads
                merged = jnp.where(pick, pair_out[1], pair_out[0])
                if duo:
                    first = lane // QBLOCK == (head + 2) % n_heads
                    merged = jnp.where(jnp.logical_or(pick, first), merged, o_scr[rows, cols])
                o_scr[rows, cols] = merged

        for unit in range(2 * GROUP):
            if unit >= 2:
                logits[unit] = score(unit) if unit not in logits else logits[unit]
            probs = []
            for sub in range(2):
                probs.append(prob(unit, sub))
                yield
            out[unit] = mm(v_scr[unit // 2], jnp.concatenate(probs, axis=1))
            if unit + 2 < 2 * GROUP and unit + 2 >= 2:
                logits[unit + 2] = score(unit + 2)
            if unit:
                place(unit - 1)
            yield
        place(2 * GROUP - 1)
        yield

    def mix(idx):
        layer, grp = split(idx)
        gate = mm(wg_t[layer], h_cm[grp])
        yield
        heads = []
        for head in range(n_heads):
            rows = slice(head * head_dim, (head + 1) * head_dim)
            parts = []
            for smp in range(GROUP):
                part = o_scr[rows, smp * own:(smp + 1) * own]
                parts.append(pltpu.roll(part, (128 - head * QBLOCK) % 128, 1) if head else part)
            heads.append(jnp.concatenate(parts, axis=1))
        o_val = (sigmoid(gate) * jnp.concatenate(heads, axis=0)).astype(bf16)
        proj = mm(wo_t[layer], o_val)
        yield
        yield from idle(2)
        resid = res[grp] + both(tab[layer, 2]) * proj
        res[grp] = resid
        yield
        h_t = (norm(resid, 0) * both(tab[layer, 3]) + both(tab[layer, 4])).astype(bf16)
        yield
        n_chunk = 4
        rows = 2 * width // n_chunk
        ups = {}
        for pos in range(n_chunk + 1):
            if pos < n_chunk:
                ups[pos] = [mm(wu_t[layer, pl.ds(base + pos * rows, rows), :], h_t) for base in (0, 2 * width)]
                yield
                if pos == 0:
                    yield from idle(0)
            if pos:
                left, right = ups[pos - 1]
                gated = 0.5 * left
                m_scr[(pos - 1) * rows:pos * rows, :] = ((gated * jnp.tanh(gated) + gated) * right).astype(bf16)
                yield

    def finish(idx, last):
        layer, grp = split(idx)
        down = mm(wd_t[layer], m_scr[...])
        yield
        yield from idle(2)
        resid = res[grp] + both(tab[layer, 5]) * down
        yield
        if last:
            for smp in range(GROUP):
                out_stage[grp * GROUP + smp] = resid[:, smp * own:(smp + 1) * own].astype(bf16).T
                yield
        else:
            res[grp] = resid
            yield
            emit_h(layer + 1, grp, resid)
            yield

    def out_push(grp, slot):
        return (out_stage.at[pl.ds(grp * GROUP, GROUP), pl.ds(slot * seq, seq)],
                out_hbm.at[pl.ds(row * half_smp + grp * GROUP, GROUP)],
                osend_sem.at[slot, grp], orecv_sem.at[row, grp], 4 * plane + 2 * core + slot)

    def sent(idx, last):
        layer, grp = split(idx)
        if last:
            for slot in range(2):
                push(*out_push(grp, slot))
        else:
            halo_start(layer + 1, grp)

    def idle(rounds):
        for _ in range(rounds):
            yield

    def chain(*parts):
        for part in parts:
            yield from part

    def interleave(*stages):
        stages = list(stages)
        while stages:
            for stage in list(stages):
                if next(stage, stages) is stages:
                    stages.remove(stage)

    def loop_body(idx, last, *extra):
        halo_wait(*split(idx + 1))
        interleave(
            attend(idx),
            chain(idle(7), finish(idx - 2, last)),
            chain(idle(1), mix(idx - 1)),
            chain(project(idx + 1), idle(1), score_early()), *extra)
        sent(idx - 2, last)

    n_steps = n_layers * n_groups
    split_at = n_steps - n_groups
    act_wait(4)
    halo_wait(0, 0)
    interleave(enter(4), chain(project(0), score_early()))
    halo_start(0, 4)
    act_wait(5)
    halo_wait(0, 1)
    interleave(attend(0), chain(project(1), idle(1), score_early()), enter(5))
    halo_start(0, 5)
    act_wait(6)
    halo_wait(0, 2)
    interleave(mix(0), attend(1), chain(project(2), idle(1), score_early()), enter(6))
    halo_start(0, 6)
    act_wait(7)
    loop_body(2, False, enter(7))
    halo_start(0, 7)

    @pl.loop(3, 6)
    def _(idx):
        loop_body(idx, False)

    @pl.loop(6, 8)
    def _(idx):
        bias_wait(idx - 5)
        loop_body(idx, False, bias_table(idx - 5, mask_bias))

    @pl.loop(8, split_at + 2)
    def _(idx):
        loop_body(idx, False)

    @pl.loop(split_at + 2, n_steps - 1)
    def _(idx):
        loop_body(idx, True)

    interleave(finish(n_steps - 3, True), mix(n_steps - 2), attend(n_steps - 1))
    sent(n_steps - 3, True)
    interleave(finish(n_steps - 2, True), mix(n_steps - 1))
    sent(n_steps - 2, True)
    interleave(finish(n_steps - 1, True))
    sent(n_steps - 1, True)

    for half in range(2):
        push_done(*cond_push(half))
        push_done(*mask_push(half))

        @pl.loop(0, n_layers)
        def _(layer):
            push_done(*bias_push(half, layer))

        @pl.loop(0, n_groups)
        def _(grp):
            push_done(*act_push(half, grp))
            push_done(*out_push(grp, half))

    @pl.when(has_prev)
    def _():
        mask_side(0).wait_send()

    @pl.when(has_next)
    def _():
        mask_side(1).wait_send()

    @pl.loop(0, n_layers)
    def _(layer):
        @pl.loop(0, n_groups)
        def _(grp):
            @pl.when(has_prev)
            def _():
                halo_copy(layer, grp, 0).wait_send()

            @pl.when(has_next)
            def _():
                halo_copy(layer, grp, 1).wait_send()

    for half in range(2):
        @pl.loop(0, n_groups)
        def _(grp):
            arrived(out_hbm.at[pl.ds(half * half_smp + grp * GROUP, GROUP)], orecv_sem.at[half, grp])


def solution(mesh):
    n_dev = mesh.shape['sp']

    def device_fn(atom_act, cond, pair, atom_mask, w_cond, b_cond, w_qkvg, b_query, w_pair, w_out, w_up, w_down):
        samples, seq, width = atom_act.shape
        n_layers = w_qkvg.shape[0]
        n_heads = width // QBLOCK
        half_smp = samples // 2
        n_groups = half_smp // GROUP
        own = 2 * seq
        ext = own + 2 * EDGE
        n_blocks = own // QBLOCK
        blocks, _, window, c_pair = pair.shape
        f32, bf16 = jnp.float32, jnp.bfloat16
        pair_t = pair.transpose(0, 1, 3, 2).reshape(blocks * QBLOCK * c_pair, window)
        vmem = pl.BlockSpec(memory_space=pltpu.VMEM)
        hbm = pl.BlockSpec(memory_space=pl.ANY)
        cols = GROUP * own
        dma = pltpu.SemaphoreType.DMA
        return pl.pallas_call(
            functools.partial(body, n_dev),
            out_shape=jax.ShapeDtypeStruct(atom_act.shape, bf16),
            in_specs=[hbm, hbm, hbm, vmem, hbm, vmem, hbm, vmem, vmem, hbm, hbm, hbm],
            out_specs=hbm,
            scratch_shapes=[
                pltpu.VMEM(pair_t.shape, bf16),
                pltpu.VMEM(w_cond.shape, bf16),
                pltpu.VMEM(w_qkvg.shape, bf16),
                pltpu.VMEM(w_out.shape, bf16),
                pltpu.VMEM(w_up.shape, bf16),
                pltpu.VMEM(w_down.shape, bf16),
                pltpu.VMEM((half_smp, own, width), bf16),
                pltpu.VMEM((own, width), bf16),
                pltpu.VMEM((8, 128), jnp.int32),
                pltpu.VMEM((4, 8, 128), jnp.int32),
                pltpu.VMEM((n_layers, blocks, n_heads * QBLOCK, window), bf16),
                pltpu.VMEM((n_layers, 2, blocks, n_heads * QBLOCK, window), bf16),
                pltpu.VMEM((half_smp, own, width), bf16),
                pltpu.VMEM((n_groups, width, cols), f32),
                pltpu.VMEM((n_groups, width, cols), bf16),
                pltpu.VMEM((n_layers, half_smp, ext, width), bf16),
                pltpu.VMEM((n_layers, 6, width, own), f32),
                pltpu.VMEM((n_layers, n_blocks, KEY_WINDOW, 128), f32),
                pltpu.VMEM((n_layers, width, width), bf16),
                pltpu.VMEM((n_layers, width, width), bf16),
                pltpu.VMEM((n_layers, width, width), bf16),
                pltpu.VMEM((n_layers, 4 * width, width), bf16),
                pltpu.VMEM((n_layers, width, 2 * width), bf16),
                pltpu.VMEM((n_layers, width, width), f32),
                pltpu.VMEM((GROUP, ext, width), bf16),
                pltpu.VMEM((GROUP, width, n_blocks * 128), bf16),
                pltpu.VMEM((GROUP, ext, width), bf16),
                pltpu.VMEM((GROUP, width, ext), bf16),
                pltpu.VMEM((width, cols), f32),
                pltpu.VMEM((2, 2, KEY_WINDOW, 128), f32),
                pltpu.VMEM((2 * width, cols), bf16),
                dma((6,)),
                dma((n_layers, n_groups, 2)),
                dma((n_layers, n_groups, 2)),
                dma((2,)),
                dma((2,)),
                dma((4,)),
                dma((4,)),
                dma((2, n_groups)),
                dma((2, n_groups)),
                dma((2, n_layers)),
                dma((2, n_layers)),
                dma((2, n_groups)),
                dma((2, n_groups)),
            ],
            compiler_params=pltpu.CompilerParams(
                collective_id=0, has_side_effects=True, vmem_limit_bytes=60 * 1024 * 1024),
        )(atom_act, cond, pair_t, atom_mask.reshape(1, seq), w_cond, b_cond, w_qkvg, b_query,
          w_pair, w_out, w_up, w_down)

    act_spec = P('dp', 'sp', None)
    in_specs = (act_spec, P('sp', None), P('sp', None, None, None), P('sp'), P(), P(), P(), P(), P(), P(), P(), P())
    return jax.shard_map(device_fn, mesh=mesh, in_specs=in_specs, out_specs=act_spec, check_vma=False)
```

```python
import functools
import math

import jax
import jax.numpy as jnp
from jax import lax
from jax.experimental import pallas as pl
from jax.experimental.pallas import tpu as pltpu
from jax.sharding import PartitionSpec as P

QBLOCK = 32
KEY_WINDOW = 128
EDGE = 48
LN_EPS = 1e-5
GROUP = 2
LOG2E = math.log2(math.e)
MESH = pl.DeviceIdType.MESH


def mm(lhs, rhs):
    return jnp.dot(lhs, rhs, preferred_element_type=jnp.float32)


def mm_nt(lhs, rhs):
    return lax.dot_general(lhs, rhs, (((1,), (1,)), ((), ())), preferred_element_type=jnp.float32)


def sigmoid(vals):
    return 0.5 * jnp.tanh(0.5 * vals) + 0.5


def norm(vals, axis):
    mean = jnp.mean(vals, axis=axis, keepdims=True)
    cent = vals - mean
    var = jnp.mean(cent * cent, axis=axis, keepdims=True)
    return cent * lax.rsqrt(var + LN_EPS)


def body(n_dev, act_hbm, cond_hbm, pair_hbm, mask_ref, wcond_hbm, bcond_ref, wqkvg_hbm, bquery_ref, wpair_ref,
         wout_hbm, wup_hbm, wdown_hbm, out_hbm,
         pair, wcond, wqkvg, wout, wup, wdown, cond_own, act,
         act_in, cond_in, mask_own, mask_in, bias_own, bias_in, out_stage,
         res, h_cm, h_ext, tab, bias, wv_t, wg_t, wo_t, wu_t, wd_t,
         k_scr, q_scr, v_scr, o_scr, s_scr, m_scr, h_mid,
         in_sem, send_sem, recv_sem, csend_sem, crecv_sem, msend_sem, mrecv_sem, asend_sem, arecv_sem,
         bsend_sem, brecv_sem, osend_sem, orecv_sem):
    n_layers, width = bquery_ref.shape
    n_heads = width // QBLOCK
    head_dim = width // n_heads
    samples, seq, _ = act_hbm.shape
    half_smp = samples // 2
    n_groups = half_smp // GROUP
    own = 2 * seq
    ext = own + 2 * EDGE
    n_blocks = own // QBLOCK
    f32, bf16 = jnp.float32, jnp.bfloat16

    me = lax.axis_index('sp')
    plane, row, core = me // 4, (me // 2) % 2, me % 2
    n_planes = n_dev // 4
    chunk = 2 * plane + core
    has_prev, has_next = chunk > 0, chunk < 2 * n_planes - 1

    def owner(chunk_idx, row_idx):
        return (chunk_idx // 2) * 4 + 2 * row_idx + chunk_idx % 2

    def remote(src, dst, ssem, rsem, peer):
        return pltpu.make_async_remote_copy(
            src_ref=src, dst_ref=dst, send_sem=ssem, recv_sem=rsem, device_id={'sp': peer}, device_id_type=MESH)

    def push(src, dst, ssem, rsem, peer):
        @pl.when(peer != me)
        def _():
            remote(src, dst, ssem, rsem, peer).start()

        @pl.when(peer == me)
        def _():
            pltpu.make_async_copy(src, dst, rsem).start()

    def push_done(src, dst, ssem, rsem, peer):
        @pl.when(peer != me)
        def _():
            remote(src, dst, ssem, rsem, peer).wait_send()

    def arrived(dst, rsem):
        pltpu.make_async_copy(dst, dst, rsem).wait()

    loads = [pltpu.make_async_copy(src, dst, in_sem.at[pos]) for pos, (src, dst) in enumerate(
        [(pair_hbm, pair), (wcond_hbm, wcond), (wqkvg_hbm, wqkvg), (wout_hbm, wout), (wup_hbm, wup), (wdown_hbm, wdown),
         (cond_hbm, cond_own), (act_hbm, act)])]
    for load in loads:
        load.start()

    zero_rows = jnp.zeros((GROUP, EDGE, width), bf16)

    @pl.loop(0, n_layers)
    def _(layer):
        @pl.loop(0, n_groups)
        def _(grp):
            h_ext[layer, pl.ds(grp * GROUP, GROUP), 0:EDGE, :] = zero_rows
            h_ext[layer, pl.ds(grp * GROUP, GROUP), EDGE + own:ext, :] = zero_rows

    mask_own[...] = jnp.zeros_like(mask_own)
    mask_own[0:1, 0:seq] = mask_ref[...]
    mask_in[0] = jnp.zeros_like(mask_own)
    mask_in[3] = jnp.zeros_like(mask_own)

    barrier = pltpu.get_barrier_semaphore()

    for other in range(4):
        peer = 4 * plane + other

        @pl.when(peer != me)
        def _():
            pl.semaphore_signal(barrier, inc=1, device_id={'sp': peer}, device_id_type=MESH)

    beyond = chunk + 2 * core - 1
    has_beyond = jnp.logical_and(beyond >= 0, beyond < 2 * n_planes)

    @pl.when(has_beyond)
    def _():
        pl.semaphore_signal(barrier, inc=1, device_id={'sp': owner(beyond, row)}, device_id_type=MESH)

    home = 2 * plane + row

    def cond_push(dest):
        return (cond_own, cond_in.at[pl.ds(core * seq, seq)], csend_sem.at[dest], crecv_sem.at[core], owner(home, dest))

    def mask_push(dest):
        return (mask_own, mask_in.at[1 + core], msend_sem.at[dest], mrecv_sem.at[1 + core], owner(home, dest))

    def mask_side(direction):
        return remote(mask_in.at[1 + direction], mask_in.at[3 - 3 * direction], msend_sem.at[2 + direction],
                      mrecv_sem.at[3 - 3 * direction], owner(chunk + 2 * direction - 1, row))

    def act_push(dest, grp):
        return (act.at[pl.ds(dest * half_smp + grp * GROUP, GROUP)],
                act_in.at[pl.ds(grp * GROUP, GROUP), pl.ds(core * seq, seq)],
                asend_sem.at[dest], arecv_sem.at[core, grp], owner(home, dest))

    def bias_push(dest, layer):
        return (bias_own.at[layer], bias_in.at[layer, core], bsend_sem.at[dest], brecv_sem.at[core, layer],
                owner(home, dest))

    c_pair = wpair_ref.shape[0]
    n_col = wpair_ref.shape[1]
    tall, deep = n_col * 16, 16 * c_pair
    pick_col = (lax.broadcasted_iota(jnp.int32, (tall, n_col), 0) // 16
                == lax.broadcasted_iota(jnp.int32, (tall, n_col), 1)).astype(bf16)
    pick_chan = (lax.broadcasted_iota(jnp.int32, (c_pair, deep), 1) % c_pair
                 == lax.broadcasted_iota(jnp.int32, (c_pair, deep), 0)).astype(bf16)
    spread = lax.dot_general(
        wpair_ref[...], pick_chan, (((0,), (0,)), ((), ())), preferred_element_type=f32).astype(bf16)
    spread = mm(pick_col, spread)
    same = (lax.broadcasted_iota(jnp.int32, (tall, deep), 0) % 16 == lax.broadcasted_iota(jnp.int32, (tall, deep), 1) // c_pair)
    w_block = jnp.where(same, spread, 0.0).astype(bf16)
    loads[0].wait()
    for part in range(seq // 16):
        vals = pair[part * deep:(part + 1) * deep].astype(f32).reshape(16, c_pair, KEY_WINDOW)
        vals = norm(vals, 1).astype(bf16).reshape(deep, KEY_WINDOW)
        res_bias = mm(w_block, vals).astype(bf16)
        blk, sub = part // 2, part % 2
        for layer in range(n_layers):
            for head in range(n_heads):
                col = layer * n_heads + head
                bias_own[layer, blk, head * QBLOCK + sub * 16:head * QBLOCK + (sub + 1) * 16, :] = res_bias[col * 16:(col + 1) * 16]
    half = jnp.array(0.5, bf16)

    def weights(layer):
        wv_t[layer] = wqkvg[layer, :, 2 * width:3 * width].T
        wg_t[layer] = wqkvg[layer, :, 3 * width:].T * half
        wo_t[layer] = wout[layer].T
        for idx in range(4):
            piece = wup[layer, :, idx * width:(idx + 1) * width].T
            wu_t[layer, idx * width:(idx + 1) * width, :] = piece * half if idx < 2 else piece
        for idx in range(2):
            wd_t[layer, :, idx * width:(idx + 1) * width] = wdown[layer, idx * width:(idx + 1) * width, :].T

    for load in loads[2:]:
        load.wait()

    @pl.loop(0, n_layers)
    def _(layer):
        weights(layer)

    n_beyond = jnp.where(has_beyond, 1, 0)
    pl.semaphore_wait(barrier, 3 + n_beyond)

    for dest in range(2):
        push(*cond_push(dest))
    for grp in range(3):
        for dest in range(2):
            push(*act_push(dest, grp))
        if grp == 0:
            for dest in range(2):
                push(*mask_push(dest))
    for dest in range(2):
        push(*bias_push(dest, 0))
    for grp in range(3, n_groups):
        for dest in range(2):
            push(*act_push(dest, grp))
    for layer in range(1, n_layers):
        for dest in range(2):
            push(*bias_push(dest, layer))

    for slot in range(2):
        arrived(cond_in.at[pl.ds(slot * seq, seq)], crecv_sem.at[slot])
    cond_norm = norm(cond_in[...].astype(f32), -1).astype(bf16)
    loads[1].wait()

    def tables(layer, first=0, last=6):
        proj = mm(cond_norm, wcond[layer, :, first * width:last * width])
        gates = bcond_ref[pl.ds(layer, 1), :]
        for idx, bias_idx in list(enumerate((0, None, 1, 2, None, 3)))[first:last]:
            piece = proj[:, (idx - first) * width:(idx - first + 1) * width]
            if bias_idx is not None:
                piece = sigmoid(piece + gates[:, bias_idx * width:(bias_idx + 1) * width])
            tab[layer, idx] = piece.T

    def both(vals):
        return jnp.concatenate([vals] * GROUP, axis=1)

    def halo_copy(layer, grp, direction):
        smp = pl.ds(grp * GROUP, GROUP)
        src = pl.ds(own if direction else EDGE, EDGE)
        dst = pl.ds(0 if direction else own + EDGE, EDGE)
        return remote(h_ext.at[layer, smp, src, :], h_ext.at[layer, smp, dst, :],
                      send_sem.at[direction], recv_sem.at[layer, grp, direction],
                      owner(chunk + 1 if direction else chunk - 1, row))

    def halo_start(layer, grp):
        @pl.when(has_prev)
        def _():
            halo_copy(layer, grp, 0).start()

        @pl.when(has_next)
        def _():
            halo_copy(layer, grp, 1).start()

    def halo_wait(layer, grp):
        @pl.when(has_next)
        def _():
            halo_copy(layer, grp, 0).wait_recv()

        @pl.when(has_prev)
        def _():
            halo_copy(layer, grp, 1).wait_recv()

    def emit_h(layer, grp, resid):
        h_t = (norm(resid, 0) * both(tab[layer, 0]) + both(tab[layer, 1])).astype(bf16)
        h_cm[grp] = h_t
        for smp in range(GROUP):
            h_ext[layer, grp * GROUP + smp, EDGE:EDGE + own, :] = h_t[:, smp * own:(smp + 1) * own].T

    def act_wait(grp):
        for slot in range(2):
            arrived(act_in.at[pl.ds(grp * GROUP, GROUP), pl.ds(slot * seq, seq)], arecv_sem.at[slot, grp])

    def enter(grp):
        cols = [act_in[grp * GROUP + smp].T.astype(f32) for smp in range(GROUP)]
        yield
        resid = jnp.concatenate(cols, axis=1)
        res[grp] = resid
        yield
        emit_h(0, grp, resid)
        yield

    def enter_now(grp):
        act_wait(grp)
        for _ in enter(grp):
            pass
        halo_start(0, grp)

    def bias_wait(layer):
        for slot in range(2):
            arrived(bias_in.at[layer, slot], brecv_sem.at[slot, layer])

    def bias_table(layer, mask_bias):
        for blk in range(n_blocks):
            nat = bias_in[layer, blk // 2, blk % 2].astype(f32)
            order = [(slot - blk) % n_heads for slot in range(n_heads)]
            nat = jnp.concatenate([nat[head * QBLOCK:(head + 1) * QBLOCK] for head in order], axis=0)
            bias[layer, blk] = ((nat + mask_bias[:, blk * QBLOCK:blk * QBLOCK + KEY_WINDOW]) * LOG2E).T
            yield

    tables(0, 0, 2)
    enter_now(0)
    tables(0, 2, 6)
    tables(1)
    enter_now(1)
    tables(2)
    for slot in range(1, 3):
        arrived(mask_in.at[slot], mrecv_sem.at[slot])

    @pl.when(has_prev)
    def _():
        mask_side(0).start()

    @pl.when(has_next)
    def _():
        mask_side(1).start()

    enter_now(2)
    @pl.when(has_prev)
    def _():
        arrived(mask_in.at[0], mrecv_sem.at[0])

    @pl.when(has_next)
    def _():
        arrived(mask_in.at[3], mrecv_sem.at[3])

    mask_row = jnp.concatenate([mask_in[0, 0:1, seq - EDGE:seq], mask_in[1, 0:1, :seq], mask_in[2, 0:1, :seq],
                                mask_in[3, 0:1, :EDGE], jnp.zeros((1, 256 - ext), jnp.int32)], axis=1)
    mask_bias = (mask_row.astype(f32) - 1.0) * 1e9
    bias_wait(0)
    for _ in bias_table(0, mask_bias):
        pass
    enter_now(3)

    lane = lax.broadcasted_iota(jnp.int32, (1, width), 1)
    scale = head_dim ** -0.5 * LOG2E
    keep = [jnp.where(lane // QBLOCK == slot, 1.0, 0.0).astype(bf16) for slot in range(n_heads)]

    def split(idx):
        return idx // n_groups, idx % n_groups

    def project(idx):
        layer, grp = split(idx)
        w_qk = wqkvg[layer, :, :2 * width]
        b_q = bquery_ref[pl.ds(layer, 1), :]
        q_k = {}
        v_t = {}

        def k_q(smp):
            q_k[smp] = mm(h_ext[layer, grp * GROUP + smp], w_qk)

        def vals(smp):
            v_t[smp] = mm_nt(wv_t[layer], h_ext[layer, grp * GROUP + smp])

        def keys(smp):
            k_scr[smp] = q_k[smp][:, width:].astype(bf16)

        def queries(smp):
            q_val = (q_k[smp][EDGE:EDGE + own, :width] + b_q).astype(bf16)
            for blk in range(n_blocks):
                part = q_val[blk * QBLOCK:(blk + 1) * QBLOCK]
                for slot in range(n_heads):
                    first = blk * 128 + slot * QBLOCK
                    q_scr[smp, first:first + QBLOCK, :] = part * keep[(slot - blk) % n_heads]
                if blk % 2:
                    yield

        k_q(0)
        yield
        yield from idle(0)
        vals(0)
        yield
        yield from idle(0)
        keys(0)
        yield
        yield from queries(0)
        k_q(1)
        yield from idle(0)
        v_scr[0] = v_t[0].astype(bf16)
        yield
        vals(1)
        yield
        yield from idle(0)
        keys(1)
        yield
        yield from queries(1)
        yield from idle(2)
        v_scr[1] = v_t[1].astype(bf16)
        yield

    def score(unit):
        smp, duo = unit // 2, unit % 2
        return mm_nt(k_scr[smp, duo * 64:duo * 64 + 160], q_scr[smp, duo * 256:(duo + 1) * 256, :])

    def score_early():
        for unit in range(2):
            logit = score(unit)
            yield
            for sub in range(2):
                s_scr[unit, sub] = logit[sub * QBLOCK:sub * QBLOCK + KEY_WINDOW, sub * 128:(sub + 1) * 128]
            yield

    def attend(idx):
        layer, grp = split(idx)
        logits = {}
        out = {}

        def prob(unit, sub):
            blk = 2 * (unit % 2) + sub
            if unit < 2:
                x = s_scr[unit, sub]
            else:
                x = logits[unit][sub * QBLOCK:sub * QBLOCK + KEY_WINDOW, sub * 128:(sub + 1) * 128]
            x = x * scale + bias[layer, blk]
            e = jnp.exp2(x - jnp.max(x, axis=0, keepdims=True))
            p = (e * (0.5 / jnp.sum(e, axis=0, keepdims=True))).astype(bf16)
            parts = [p]
            if blk:
                parts = [jnp.zeros((blk * QBLOCK, 128), bf16)] + parts
            if blk < n_blocks - 1:
                parts = parts + [jnp.zeros(((n_blocks - 1 - blk) * QBLOCK, 128), bf16)]
            return jnp.concatenate(parts, axis=0)

        def place(unit):
            smp, duo = unit // 2, unit % 2
            cols = slice(smp * own, (smp + 1) * own)
            for head in range(n_heads):
                rows = slice(head * head_dim, (head + 1) * head_dim)
                pair_out = [out[unit][rows, sub * 128:(sub + 1) * 128] for sub in range(2)]
                pick = lane // QBLOCK == (head + 2 * duo + 1) % n_heads
                merged = jnp.where(pick, pair_out[1], pair_out[0])
                if duo:
                    first = lane // QBLOCK == (head + 2) % n_heads
                    merged = jnp.where(jnp.logical_or(pick, first), merged, o_scr[rows, cols])
                o_scr[rows, cols] = merged

        for unit in range(2 * GROUP):
            if unit >= 2:
                logits[unit] = score(unit) if unit not in logits else logits[unit]
            probs = []
            for sub in range(2):
                probs.append(prob(unit, sub))
                yield
            out[unit] = mm(v_scr[unit // 2], jnp.concatenate(probs, axis=1))
            if unit + 2 < 2 * GROUP and unit + 2 >= 2:
                logits[unit + 2] = score(unit + 2)
            if unit:
                place(unit - 1)
            yield
        place(2 * GROUP - 1)
        yield

    def mix(idx):
        layer, grp = split(idx)
        gate = mm(wg_t[layer], h_cm[grp])
        yield
        yield from idle(2)
        heads = []
        for head in range(n_heads):
            rows = slice(head * head_dim, (head + 1) * head_dim)
            parts = []
            for smp in range(GROUP):
                part = o_scr[rows, smp * own:(smp + 1) * own]
                parts.append(pltpu.roll(part, (128 - head * QBLOCK) % 128, 1) if head else part)
            heads.append(jnp.concatenate(parts, axis=1))
        o_val = ((jnp.tanh(gate) + 1.0) * jnp.concatenate(heads, axis=0)).astype(bf16)
        proj = mm(wo_t[layer], o_val)
        yield
        yield from idle(2)
        resid = res[grp] + both(tab[layer, 2]) * proj
        res[grp] = resid
        yield
        yield from idle(4)
        h_mid[...] = (norm(resid, 0) * both(tab[layer, 3]) + both(tab[layer, 4])).astype(bf16)
        yield

    def finish(idx, last):
        layer, grp = split(idx)
        h_t = h_mid[...]
        n_chunk = 2
        rows = 2 * width // n_chunk
        ups = {}
        for pos in range(n_chunk + 1):
            if pos < n_chunk:
                ups[pos] = [mm(wu_t[layer, pl.ds(base + pos * rows, rows), :], h_t) for base in (0, 2 * width)]
                yield
                if pos == 0:
                    yield from idle(1)
            if pos:
                left, right = ups[pos - 1]
                m_scr[(pos - 1) * rows:pos * rows, :] = ((left * jnp.tanh(left) + left) * right).astype(bf16)
                yield
        down = mm(wd_t[layer], m_scr[...])
        yield
        yield from idle(0)
        resid = res[grp] + both(tab[layer, 5]) * down
        yield
        if last:
            for smp in range(GROUP):
                out_stage[grp * GROUP + smp] = resid[:, smp * own:(smp + 1) * own].astype(bf16).T
                yield
        else:
            res[grp] = resid
            yield
            emit_h(layer + 1, grp, resid)
            yield

    def out_push(grp, slot):
        return (out_stage.at[pl.ds(grp * GROUP, GROUP), pl.ds(slot * seq, seq)],
                out_hbm.at[pl.ds(row * half_smp + grp * GROUP, GROUP)],
                osend_sem.at[slot], orecv_sem.at[row], 4 * plane + 2 * core + slot)

    def sent(idx, last):
        layer, grp = split(idx)
        if last:
            for slot in range(2):
                push(*out_push(grp, slot))
        else:
            halo_start(layer + 1, grp)

    def idle(rounds):
        for _ in range(rounds):
            yield

    def chain(*parts):
        for part in parts:
            yield from part

    def interleave(*stages):
        stages = list(stages)
        while stages:
            for stage in list(stages):
                if next(stage, stages) is stages:
                    stages.remove(stage)

    def loop_body(idx, last, *extra):
        halo_wait(*split(idx + 1))
        interleave(chain(idle(1), finish(idx - 2, last)), chain(idle(0), mix(idx - 1)), attend(idx), chain(idle(2), project(idx + 1)), chain(idle(10), score_early()), *extra)
        sent(idx - 2, last)

    n_steps = n_layers * n_groups
    split_at = n_steps - n_groups
    act_wait(4)
    halo_wait(0, 0)
    interleave(enter(4), chain(project(0), score_early()))
    halo_start(0, 4)
    act_wait(5)
    halo_wait(0, 1)
    interleave(attend(0), chain(project(1), score_early()), enter(5))
    halo_start(0, 5)
    act_wait(6)
    halo_wait(0, 2)
    interleave(mix(0), attend(1), chain(project(2), score_early()), enter(6))
    halo_start(0, 6)
    act_wait(7)
    loop_body(2, False, enter(7))
    halo_start(0, 7)

    @pl.loop(3, 6)
    def _(idx):
        loop_body(idx, False)

    @pl.loop(6, 8)
    def _(idx):
        bias_wait(idx - 5)
        loop_body(idx, False, bias_table(idx - 5, mask_bias))

    @pl.loop(8, split_at + 2)
    def _(idx):
        loop_body(idx, False)

    @pl.loop(split_at + 2, n_steps - 1)
    def _(idx):
        loop_body(idx, True)

    interleave(finish(n_steps - 3, True), mix(n_steps - 2), attend(n_steps - 1))
    sent(n_steps - 3, True)
    interleave(finish(n_steps - 2, True), mix(n_steps - 1))
    sent(n_steps - 2, True)
    interleave(finish(n_steps - 1, True))
    sent(n_steps - 1, True)

    def drained(src, ssem):
        pltpu.make_async_copy(src, src, ssem).wait()

    for dest in range(2):
        push_done(*cond_push(dest))
        push_done(*mask_push(dest))

        @pl.when(owner(home, dest) != me)
        def _():
            drained(bias_own, bsend_sem.at[dest])
            drained(act.at[pl.ds(0, half_smp)], asend_sem.at[dest])

        @pl.when(4 * plane + 2 * core + dest != me)
        def _():
            drained(out_stage.at[:, pl.ds(0, seq)], osend_sem.at[dest])

    @pl.when(has_prev)
    def _():
        mask_side(0).wait_send()
        drained(h_ext.at[:, :, pl.ds(0, EDGE)], send_sem.at[0])

    @pl.when(has_next)
    def _():
        mask_side(1).wait_send()
        drained(h_ext.at[:, :, pl.ds(0, EDGE)], send_sem.at[1])

    for dest in range(2):
        arrived(out_hbm.at[pl.ds(dest * half_smp, half_smp)], orecv_sem.at[dest])


def solution(mesh):
    n_dev = mesh.shape['sp']

    def device_fn(atom_act, cond, pair, atom_mask, w_cond, b_cond, w_qkvg, b_query, w_pair, w_out, w_up, w_down):
        samples, seq, width = atom_act.shape
        n_layers = w_qkvg.shape[0]
        n_heads = width // QBLOCK
        half_smp = samples // 2
        n_groups = half_smp // GROUP
        own = 2 * seq
        ext = own + 2 * EDGE
        n_blocks = own // QBLOCK
        blocks, _, window, c_pair = pair.shape
        f32, bf16 = jnp.float32, jnp.bfloat16
        pair_t = pair.transpose(0, 1, 3, 2).reshape(blocks * QBLOCK * c_pair, window)
        vmem = pl.BlockSpec(memory_space=pltpu.VMEM)
        hbm = pl.BlockSpec(memory_space=pl.ANY)
        cols = GROUP * own
        dma = pltpu.SemaphoreType.DMA
        return pl.pallas_call(
            functools.partial(body, n_dev),
            out_shape=jax.ShapeDtypeStruct(atom_act.shape, bf16),
            in_specs=[hbm, hbm, hbm, vmem, hbm, vmem, hbm, vmem, vmem, hbm, hbm, hbm],
            out_specs=hbm,
            scratch_shapes=[
                pltpu.VMEM(pair_t.shape, bf16),
                pltpu.VMEM(w_cond.shape, bf16),
                pltpu.VMEM(w_qkvg.shape, bf16),
                pltpu.VMEM(w_out.shape, bf16),
                pltpu.VMEM(w_up.shape, bf16),
                pltpu.VMEM(w_down.shape, bf16),
                pltpu.VMEM(cond.shape, bf16),
                pltpu.VMEM(atom_act.shape, bf16),
                pltpu.VMEM((half_smp, own, width), bf16),
                pltpu.VMEM((own, width), bf16),
                pltpu.VMEM((8, 128), jnp.int32),
                pltpu.VMEM((4, 8, 128), jnp.int32),
                pltpu.VMEM((n_layers, blocks, n_heads * QBLOCK, window), bf16),
                pltpu.VMEM((n_layers, 2, blocks, n_heads * QBLOCK, window), bf16),
                pltpu.VMEM((half_smp, own, width), bf16),
                pltpu.VMEM((n_groups, width, cols), f32),
                pltpu.VMEM((n_groups, width, cols), bf16),
                pltpu.VMEM((n_layers, half_smp, ext, width), bf16),
                pltpu.VMEM((n_layers, 6, width, own), f32),
                pltpu.VMEM((n_layers, n_blocks, KEY_WINDOW, 128), f32),
                pltpu.VMEM((n_layers, width, width), bf16),
                pltpu.VMEM((n_layers, width, width), bf16),
                pltpu.VMEM((n_layers, width, width), bf16),
                pltpu.VMEM((n_layers, 4 * width, width), bf16),
                pltpu.VMEM((n_layers, width, 2 * width), bf16),
                pltpu.VMEM((GROUP, ext, width), bf16),
                pltpu.VMEM((GROUP, n_blocks * 128, width), bf16),
                pltpu.VMEM((GROUP, width, ext), bf16),
                pltpu.VMEM((width, cols), f32),
                pltpu.VMEM((2, 2, KEY_WINDOW, 128), f32),
                pltpu.VMEM((2 * width, cols), bf16),
                pltpu.VMEM((width, cols), bf16),
                dma((12,)),
                dma((2,)),
                dma((n_layers, n_groups, 2)),
                dma((2,)),
                dma((2,)),
                dma((4,)),
                dma((4,)),
                dma((2,)),
                dma((2, n_groups)),
                dma((2,)),
                dma((2, n_layers)),
                dma((2,)),
                dma((2,)),
            ],
            compiler_params=pltpu.CompilerParams(
                collective_id=0, has_side_effects=True, vmem_limit_bytes=60 * 1024 * 1024),
        )(atom_act, cond, pair_t, atom_mask.reshape(1, seq), w_cond, b_cond, w_qkvg, b_query,
          w_pair, w_out, w_up, w_down)

    act_spec = P('dp', 'sp', None)
    in_specs = (act_spec, P('sp', None), P('sp', None, None, None), P('sp'), P(), P(), P(), P(), P(), P(), P(), P())
    return jax.shard_map(device_fn, mesh=mesh, in_specs=in_specs, out_specs=act_spec, check_vma=False)
```

```python
import functools
import math

import jax
import jax.numpy as jnp
from jax import lax
from jax.experimental import pallas as pl
from jax.experimental.pallas import tpu as pltpu
from jax.sharding import PartitionSpec as P

QBLOCK = 32
KEY_WINDOW = 128
EDGE = 48
LN_EPS = 1e-5
GROUP = 2
LOG2E = math.log2(math.e)
MESH = pl.DeviceIdType.MESH


def mm(lhs, rhs):
    return jnp.dot(lhs, rhs, preferred_element_type=jnp.float32)


def mm_nt(lhs, rhs):
    return lax.dot_general(lhs, rhs, (((1,), (1,)), ((), ())), preferred_element_type=jnp.float32)


def sigmoid(vals):
    return 0.5 * jnp.tanh(0.5 * vals) + 0.5


def norm(vals, axis):
    mean = jnp.mean(vals, axis=axis, keepdims=True)
    cent = vals - mean
    var = jnp.mean(cent * cent, axis=axis, keepdims=True)
    return cent * lax.rsqrt(var + LN_EPS)


def body(n_dev, act_hbm, cond_hbm, pair_hbm, mask_ref, wcond_hbm, bcond_ref, wqkvg_hbm, bquery_ref, wpair_ref,
         wout_hbm, wup_hbm, wdown_hbm, out_hbm,
         pair, wcond, wqkvg, wout, wup, wdown, cond_own, act,
         act_in, cond_in, mask_own, mask_in, bias_own, bias_in, out_stage,
         res, h_cm, h_ext, tab, bias, wv_t, wg_t, wo_t, wu_t, wd_t, wc_t, bc_t,
         k_scr, q_scr, v_scr, o_scr, s_scr, m_scr, h_mid,
         in_sem, send_sem, recv_sem, csend_sem, crecv_sem, msend_sem, mrecv_sem, asend_sem, arecv_sem,
         bsend_sem, brecv_sem, osend_sem, orecv_sem):
    n_layers, width = bquery_ref.shape
    n_heads = width // QBLOCK
    head_dim = width // n_heads
    samples, seq, _ = act_hbm.shape
    half_smp = samples // 2
    n_groups = half_smp // GROUP
    own = 2 * seq
    ext = own + 2 * EDGE
    n_blocks = own // QBLOCK
    f32, bf16 = jnp.float32, jnp.bfloat16

    me = lax.axis_index('sp')
    plane, row, core = me // 4, (me // 2) % 2, me % 2
    n_planes = n_dev // 4
    chunk = 2 * plane + core
    has_prev, has_next = chunk > 0, chunk < 2 * n_planes - 1

    def owner(chunk_idx, row_idx):
        return (chunk_idx // 2) * 4 + 2 * row_idx + chunk_idx % 2

    def remote(src, dst, ssem, rsem, peer):
        return pltpu.make_async_remote_copy(
            src_ref=src, dst_ref=dst, send_sem=ssem, recv_sem=rsem, device_id={'sp': peer}, device_id_type=MESH)

    def push(src, dst, ssem, rsem, peer):
        @pl.when(peer != me)
        def _():
            remote(src, dst, ssem, rsem, peer).start()

        @pl.when(peer == me)
        def _():
            pltpu.make_async_copy(src, dst, rsem).start()

    def push_done(src, dst, ssem, rsem, peer):
        @pl.when(peer != me)
        def _():
            remote(src, dst, ssem, rsem, peer).wait_send()

    def arrived(dst, rsem):
        pltpu.make_async_copy(dst, dst, rsem).wait()

    loads = [pltpu.make_async_copy(src, dst, in_sem.at[pos]) for pos, (src, dst) in enumerate(
        [(pair_hbm, pair), (wcond_hbm, wcond), (wqkvg_hbm, wqkvg), (wout_hbm, wout), (wup_hbm, wup), (wdown_hbm, wdown),
         (cond_hbm, cond_own), (act_hbm, act)])]
    for load in loads:
        load.start()

    zero_rows = jnp.zeros((GROUP, EDGE, width), bf16)

    @pl.loop(0, n_layers)
    def _(layer):
        @pl.loop(0, n_groups)
        def _(grp):
            h_ext[layer, pl.ds(grp * GROUP, GROUP), 0:EDGE, :] = zero_rows
            h_ext[layer, pl.ds(grp * GROUP, GROUP), EDGE + own:ext, :] = zero_rows

    mask_own[...] = jnp.zeros_like(mask_own)
    mask_own[0:1, 0:seq] = mask_ref[...]
    mask_in[0] = jnp.zeros_like(mask_own)
    mask_in[3] = jnp.zeros_like(mask_own)

    barrier = pltpu.get_barrier_semaphore()

    for other in range(4):
        peer = 4 * plane + other

        @pl.when(peer != me)
        def _():
            pl.semaphore_signal(barrier, inc=1, device_id={'sp': peer}, device_id_type=MESH)

    beyond = chunk + 2 * core - 1
    has_beyond = jnp.logical_and(beyond >= 0, beyond < 2 * n_planes)

    @pl.when(has_beyond)
    def _():
        pl.semaphore_signal(barrier, inc=1, device_id={'sp': owner(beyond, row)}, device_id_type=MESH)

    home = 2 * plane + row

    def cond_push(dest):
        return (cond_own, cond_in.at[pl.ds(core * seq, seq)], csend_sem.at[dest], crecv_sem.at[core], owner(home, dest))

    def mask_push(dest):
        return (mask_own, mask_in.at[1 + core], msend_sem.at[dest], mrecv_sem.at[1 + core], owner(home, dest))

    def mask_side(direction):
        return remote(mask_in.at[1 + direction], mask_in.at[3 - 3 * direction], msend_sem.at[2 + direction],
                      mrecv_sem.at[3 - 3 * direction], owner(chunk + 2 * direction - 1, row))

    def act_push(dest, grp):
        return (act.at[pl.ds(dest * half_smp + grp * GROUP, GROUP)],
                act_in.at[pl.ds(grp * GROUP, GROUP), pl.ds(core * seq, seq)],
                asend_sem.at[dest], arecv_sem.at[core, grp], owner(home, dest))

    def bias_push(dest, layer):
        return (bias_own.at[layer], bias_in.at[layer, core], bsend_sem.at[dest], brecv_sem.at[core, layer],
                owner(home, dest))

    c_pair = wpair_ref.shape[0]
    n_col = wpair_ref.shape[1]
    tall, deep = n_col * 16, 16 * c_pair
    pick_col = (lax.broadcasted_iota(jnp.int32, (tall, n_col), 0) // 16
                == lax.broadcasted_iota(jnp.int32, (tall, n_col), 1)).astype(bf16)
    pick_chan = (lax.broadcasted_iota(jnp.int32, (c_pair, deep), 1) % c_pair
                 == lax.broadcasted_iota(jnp.int32, (c_pair, deep), 0)).astype(bf16)
    spread = lax.dot_general(
        wpair_ref[...], pick_chan, (((0,), (0,)), ((), ())), preferred_element_type=f32).astype(bf16)
    spread = mm(pick_col, spread)
    same = (lax.broadcasted_iota(jnp.int32, (tall, deep), 0) % 16 == lax.broadcasted_iota(jnp.int32, (tall, deep), 1) // c_pair)
    w_block = jnp.where(same, spread, 0.0).astype(bf16)
    loads[0].wait()
    for part in range(seq // 16):
        vals = pair[part * deep:(part + 1) * deep].astype(f32).reshape(16, c_pair, KEY_WINDOW)
        vals = norm(vals, 1).astype(bf16).reshape(deep, KEY_WINDOW)
        res_bias = mm(w_block, vals).astype(bf16)
        blk, sub = part // 2, part % 2
        for layer in range(n_layers):
            for head in range(n_heads):
                col = layer * n_heads + head
                bias_own[layer, blk, head * QBLOCK + sub * 16:head * QBLOCK + (sub + 1) * 16, :] = res_bias[col * 16:(col + 1) * 16]
    half = jnp.array(0.5, bf16)

    def weights(layer):
        for idx, bias_idx in enumerate((0, None, 1, 2, None, 3)):
            piece = wcond[layer, :, idx * width:(idx + 1) * width].T
            wc_t[layer, idx * width:(idx + 1) * width, :] = piece if bias_idx is None else piece * half
            if bias_idx is not None:
                cell = bcond_ref[pl.ds(layer, 1), :][:, bias_idx * width:(bias_idx + 1) * width] * 0.5
                bc_t[layer, bias_idx] = jnp.broadcast_to(cell, (own, width)).T
        wv_t[layer] = wqkvg[layer, :, 2 * width:3 * width].T
        wg_t[layer] = wqkvg[layer, :, 3 * width:].T * half
        wo_t[layer] = wout[layer].T
        for idx in range(4):
            piece = wup[layer, :, idx * width:(idx + 1) * width].T
            wu_t[layer, idx * width:(idx + 1) * width, :] = piece * half if idx < 2 else piece
        for idx in range(2):
            wd_t[layer, :, idx * width:(idx + 1) * width] = wdown[layer, idx * width:(idx + 1) * width, :].T

    for load in loads[1:]:
        load.wait()

    weights(0)

    n_beyond = jnp.where(has_beyond, 1, 0)
    pl.semaphore_wait(barrier, 3 + n_beyond)

    for dest in range(2):
        push(*cond_push(dest))
    for grp in range(3):
        for dest in range(2):
            push(*act_push(dest, grp))
        if grp == 0:
            for dest in range(2):
                push(*mask_push(dest))
    for dest in range(2):
        push(*bias_push(dest, 0))
    for grp in range(3, n_groups):
        for dest in range(2):
            push(*act_push(dest, grp))
    for layer in range(1, n_layers):
        for dest in range(2):
            push(*bias_push(dest, layer))

    @pl.loop(1, n_layers)
    def _(layer):
        weights(layer)

    for slot in range(2):
        arrived(cond_in.at[pl.ds(slot * seq, seq)], crecv_sem.at[slot])
    cond_norm = norm(cond_in[...].astype(f32), -1).astype(bf16)

    def tables(layer, first=0, last=6):
        proj = mm_nt(wc_t[layer, first * width:last * width], cond_norm)
        yield
        for idx, bias_idx in list(enumerate((0, None, 1, 2, None, 3)))[first:last]:
            piece = proj[(idx - first) * width:(idx - first + 1) * width]
            if bias_idx is not None:
                piece = 0.5 * jnp.tanh(piece + bc_t[layer, bias_idx]) + 0.5
            tab[layer, idx] = piece
            yield

    def idle(rounds):
        for _ in range(rounds):
            yield

    def chain(*parts):
        for part in parts:
            yield from part

    def interleave(*stages):
        stages = list(stages)
        while stages:
            for stage in list(stages):
                if next(stage, stages) is stages:
                    stages.remove(stage)

    def both(vals):
        return jnp.concatenate([vals] * GROUP, axis=1)

    def halo_copy(layer, grp, direction):
        smp = pl.ds(grp * GROUP, GROUP)
        src = pl.ds(own if direction else EDGE, EDGE)
        dst = pl.ds(0 if direction else own + EDGE, EDGE)
        return remote(h_ext.at[layer, smp, src, :], h_ext.at[layer, smp, dst, :],
                      send_sem.at[direction], recv_sem.at[layer, grp, direction],
                      owner(chunk + 1 if direction else chunk - 1, row))

    def halo_start(layer, grp):
        @pl.when(has_prev)
        def _():
            halo_copy(layer, grp, 0).start()

        @pl.when(has_next)
        def _():
            halo_copy(layer, grp, 1).start()

    def halo_wait(layer, grp):
        @pl.when(has_next)
        def _():
            halo_copy(layer, grp, 0).wait_recv()

        @pl.when(has_prev)
        def _():
            halo_copy(layer, grp, 1).wait_recv()

    def emit_h(layer, grp, resid):
        h_t = (norm(resid, 0) * both(tab[layer, 0]) + both(tab[layer, 1])).astype(bf16)
        h_cm[grp] = h_t
        for smp in range(GROUP):
            h_ext[layer, grp * GROUP + smp, EDGE:EDGE + own, :] = h_t[:, smp * own:(smp + 1) * own].T

    def act_wait(grp):
        for slot in range(2):
            arrived(act_in.at[pl.ds(grp * GROUP, GROUP), pl.ds(slot * seq, seq)], arecv_sem.at[slot, grp])

    def enter(grp):
        cols = [act_in[grp * GROUP + smp].T.astype(f32) for smp in range(GROUP)]
        yield
        resid = jnp.concatenate(cols, axis=1)
        res[grp] = resid
        yield
        emit_h(0, grp, resid)
        yield

    def bias_wait(layer):
        for slot in range(2):
            arrived(bias_in.at[layer, slot], brecv_sem.at[slot, layer])

    def bias_table(layer, mask_bias):
        for blk in range(n_blocks):
            nat = bias_in[layer, blk // 2, blk % 2].astype(f32)
            order = [(slot - blk) % n_heads for slot in range(n_heads)]
            nat = jnp.concatenate([nat[head * QBLOCK:(head + 1) * QBLOCK] for head in order], axis=0)
            bias[layer, blk] = ((nat + mask_bias[:, blk * QBLOCK:blk * QBLOCK + KEY_WINDOW]) * LOG2E).T
            yield

    interleave(tables(0, 0, 2))
    act_wait(0)
    interleave(enter(0))
    halo_start(0, 0)
    act_wait(1)
    interleave(enter(1), chain(tables(0, 2, 6), tables(1)))
    halo_start(0, 1)
    for slot in range(1, 3):
        arrived(mask_in.at[slot], mrecv_sem.at[slot])

    @pl.when(has_prev)
    def _():
        mask_side(0).start()

    @pl.when(has_next)
    def _():
        mask_side(1).start()

    act_wait(2)
    interleave(enter(2), tables(2))
    halo_start(0, 2)
    @pl.when(has_prev)
    def _():
        arrived(mask_in.at[0], mrecv_sem.at[0])

    @pl.when(has_next)
    def _():
        arrived(mask_in.at[3], mrecv_sem.at[3])

    mask_row = jnp.concatenate([mask_in[0, 0:1, seq - EDGE:seq], mask_in[1, 0:1, :seq], mask_in[2, 0:1, :seq],
                                mask_in[3, 0:1, :EDGE], jnp.zeros((1, 256 - ext), jnp.int32)], axis=1)
    mask_bias = (mask_row.astype(f32) - 1.0) * 1e9
    bias_wait(0)
    act_wait(3)
    interleave(enter(3), bias_table(0, mask_bias))
    halo_start(0, 3)

    lane = lax.broadcasted_iota(jnp.int32, (1, width), 1)
    scale = head_dim ** -0.5 * LOG2E
    keep = [jnp.where(lane // QBLOCK == slot, 1.0, 0.0).astype(bf16) for slot in range(n_heads)]

    def split(idx):
        return idx // n_groups, idx % n_groups

    def project(idx):
        layer, grp = split(idx)
        w_qk = wqkvg[layer, :, :2 * width]
        b_q = bquery_ref[pl.ds(layer, 1), :]
        q_k = {}
        v_t = {}

        def k_q(smp):
            q_k[smp] = mm(h_ext[layer, grp * GROUP + smp], w_qk)

        def vals(smp):
            v_t[smp] = mm_nt(wv_t[layer], h_ext[layer, grp * GROUP + smp])

        def keys(smp):
            k_scr[smp] = q_k[smp][:, width:].astype(bf16)

        def queries(smp):
            q_val = (q_k[smp][EDGE:EDGE + own, :width] + b_q).astype(bf16)
            for blk in range(n_blocks):
                part = q_val[blk * QBLOCK:(blk + 1) * QBLOCK]
                for slot in range(n_heads):
                    first = blk * 128 + slot * QBLOCK
                    q_scr[smp, first:first + QBLOCK, :] = part * keep[(slot - blk) % n_heads]
                if blk % 2:
                    yield

        k_q(0)
        yield
        yield from idle(0)
        vals(0)
        yield
        yield from idle(0)
        keys(0)
        yield
        yield from queries(0)
        k_q(1)
        yield from idle(0)
        v_scr[0] = v_t[0].astype(bf16)
        yield
        vals(1)
        yield
        yield from idle(0)
        keys(1)
        yield
        yield from queries(1)
        yield from idle(2)
        v_scr[1] = v_t[1].astype(bf16)
        yield

    def score(unit):
        smp, duo = unit // 2, unit % 2
        return mm_nt(k_scr[smp, duo * 64:duo * 64 + 160], q_scr[smp, duo * 256:(duo + 1) * 256, :])

    def score_early():
        for unit in range(2):
            logit = score(unit)
            yield
            for sub in range(2):
                s_scr[unit, sub] = logit[sub * QBLOCK:sub * QBLOCK + KEY_WINDOW, sub * 128:(sub + 1) * 128]
            yield

    def attend(idx):
        layer, grp = split(idx)
        logits = {}
        out = {}

        def prob(unit, sub):
            blk = 2 * (unit % 2) + sub
            if unit < 2:
                x = s_scr[unit, sub]
            else:
                x = logits[unit][sub * QBLOCK:sub * QBLOCK + KEY_WINDOW, sub * 128:(sub + 1) * 128]
            x = x * scale + bias[layer, blk]
            e = jnp.exp2(x - jnp.max(x, axis=0, keepdims=True))
            p = (e * (0.5 / jnp.sum(e, axis=0, keepdims=True))).astype(bf16)
            parts = [p]
            if blk:
                parts = [jnp.zeros((blk * QBLOCK, 128), bf16)] + parts
            if blk < n_blocks - 1:
                parts = parts + [jnp.zeros(((n_blocks - 1 - blk) * QBLOCK, 128), bf16)]
            return jnp.concatenate(parts, axis=0)

        def place(unit):
            smp, duo = unit // 2, unit % 2
            cols = slice(smp * own, (smp + 1) * own)
            for head in range(n_heads):
                rows = slice(head * head_dim, (head + 1) * head_dim)
                pair_out = [out[unit][rows, sub * 128:(sub + 1) * 128] for sub in range(2)]
                pick = lane // QBLOCK == (head + 2 * duo + 1) % n_heads
                merged = jnp.where(pick, pair_out[1], pair_out[0])
                if duo:
                    first = lane // QBLOCK == (head + 2) % n_heads
                    merged = jnp.where(jnp.logical_or(pick, first), merged, o_scr[rows, cols])
                o_scr[rows, cols] = merged

        for unit in range(2 * GROUP):
            if unit >= 2:
                logits[unit] = score(unit) if unit not in logits else logits[unit]
            probs = []
            for sub in range(2):
                probs.append(prob(unit, sub))
                yield
            out[unit] = mm(v_scr[unit // 2], jnp.concatenate(probs, axis=1))
            if unit + 2 < 2 * GROUP and unit + 2 >= 2:
                logits[unit + 2] = score(unit + 2)
            if unit:
                place(unit - 1)
            yield
        place(2 * GROUP - 1)
        yield

    def mix(idx):
        layer, grp = split(idx)
        gate = mm(wg_t[layer], h_cm[grp])
        yield
        yield from idle(2)
        heads = []
        for head in range(n_heads):
            rows = slice(head * head_dim, (head + 1) * head_dim)
            parts = []
            for smp in range(GROUP):
                part = o_scr[rows, smp * own:(smp + 1) * own]
                parts.append(pltpu.roll(part, (128 - head * QBLOCK) % 128, 1) if head else part)
            heads.append(jnp.concatenate(parts, axis=1))
        o_val = ((jnp.tanh(gate) + 1.0) * jnp.concatenate(heads, axis=0)).astype(bf16)
        proj = mm(wo_t[layer], o_val)
        yield
        yield from idle(2)
        resid = res[grp] + both(tab[layer, 2]) * proj
        res[grp] = resid
        yield
        yield from idle(4)
        h_mid[...] = (norm(resid, 0) * both(tab[layer, 3]) + both(tab[layer, 4])).astype(bf16)
        yield

    def finish(idx, last):
        layer, grp = split(idx)
        h_t = h_mid[...]
        n_chunk = 2
        rows = 2 * width // n_chunk
        ups = {}
        for pos in range(n_chunk + 1):
            if pos < n_chunk:
                ups[pos] = [mm(wu_t[layer, pl.ds(base + pos * rows, rows), :], h_t) for base in (0, 2 * width)]
                yield
                if pos == 0:
                    yield from idle(1)
            if pos:
                left, right = ups[pos - 1]
                m_scr[(pos - 1) * rows:pos * rows, :] = ((left * jnp.tanh(left) + left) * right).astype(bf16)
                yield
        down = mm(wd_t[layer], m_scr[...])
        yield
        yield from idle(0)
        resid = res[grp] + both(tab[layer, 5]) * down
        yield
        if last:
            for smp in range(GROUP):
                out_stage[grp * GROUP + smp] = resid[:, smp * own:(smp + 1) * own].astype(bf16).T
                yield
        else:
            res[grp] = resid
            yield
            emit_h(layer + 1, grp, resid)
            yield

    def out_push(grp, slot):
        return (out_stage.at[pl.ds(grp * GROUP, GROUP), pl.ds(slot * seq, seq)],
                out_hbm.at[pl.ds(row * half_smp + grp * GROUP, GROUP)],
                osend_sem.at[slot], orecv_sem.at[row], 4 * plane + 2 * core + slot)

    def sent(idx, last):
        layer, grp = split(idx)
        if last:
            for slot in range(2):
                push(*out_push(grp, slot))
        else:
            halo_start(layer + 1, grp)

    def loop_body(idx, last, *extra):
        halo_wait(*split(idx + 1))
        interleave(chain(idle(1), finish(idx - 2, last)), chain(idle(0), mix(idx - 1)), attend(idx), chain(idle(2), project(idx + 1)), chain(idle(10), score_early()), *extra)
        sent(idx - 2, last)

    n_steps = n_layers * n_groups
    split_at = n_steps - n_groups
    act_wait(4)
    halo_wait(0, 0)
    interleave(enter(4), chain(project(0), score_early()))
    halo_start(0, 4)
    act_wait(5)
    halo_wait(0, 1)
    interleave(attend(0), chain(project(1), score_early()), enter(5))
    halo_start(0, 5)
    act_wait(6)
    halo_wait(0, 2)
    interleave(mix(0), attend(1), chain(project(2), score_early()), enter(6))
    halo_start(0, 6)
    act_wait(7)
    loop_body(2, False, enter(7))
    halo_start(0, 7)

    @pl.loop(3, 7)
    def _(idx):
        loop_body(idx, False)

    bias_wait(1)
    loop_body(7, False, bias_table(1, mask_bias))

    @pl.loop(8, 12)
    def _(idx):
        loop_body(idx, False)

    bias_wait(2)
    loop_body(12, False, bias_table(2, mask_bias))

    @pl.loop(13, split_at + 2)
    def _(idx):
        loop_body(idx, False)

    @pl.loop(split_at + 2, n_steps - 1)
    def _(idx):
        loop_body(idx, True)

    interleave(finish(n_steps - 3, True), mix(n_steps - 2), attend(n_steps - 1))
    sent(n_steps - 3, True)
    interleave(finish(n_steps - 2, True), mix(n_steps - 1))
    sent(n_steps - 2, True)
    interleave(finish(n_steps - 1, True))
    sent(n_steps - 1, True)

    def drained(src, ssem):
        pltpu.make_async_copy(src, src, ssem).wait()

    for dest in range(2):
        push_done(*cond_push(dest))
        push_done(*mask_push(dest))

        @pl.when(owner(home, dest) != me)
        def _():
            drained(bias_own, bsend_sem.at[dest])
            drained(act.at[pl.ds(0, half_smp)], asend_sem.at[dest])

        @pl.when(4 * plane + 2 * core + dest != me)
        def _():
            drained(out_stage.at[:, pl.ds(0, seq)], osend_sem.at[dest])

    @pl.when(has_prev)
    def _():
        mask_side(0).wait_send()
        drained(h_ext.at[:, :, pl.ds(0, EDGE)], send_sem.at[0])

    @pl.when(has_next)
    def _():
        mask_side(1).wait_send()
        drained(h_ext.at[:, :, pl.ds(0, EDGE)], send_sem.at[1])

    for dest in range(2):
        arrived(out_hbm.at[pl.ds(dest * half_smp, half_smp)], orecv_sem.at[dest])


def solution(mesh):
    n_dev = mesh.shape['sp']

    def device_fn(atom_act, cond, pair, atom_mask, w_cond, b_cond, w_qkvg, b_query, w_pair, w_out, w_up, w_down):
        samples, seq, width = atom_act.shape
        n_layers = w_qkvg.shape[0]
        n_heads = width // QBLOCK
        half_smp = samples // 2
        n_groups = half_smp // GROUP
        own = 2 * seq
        ext = own + 2 * EDGE
        n_blocks = own // QBLOCK
        blocks, _, window, c_pair = pair.shape
        f32, bf16 = jnp.float32, jnp.bfloat16
        pair_t = pair.transpose(0, 1, 3, 2).reshape(blocks * QBLOCK * c_pair, window)
        vmem = pl.BlockSpec(memory_space=pltpu.VMEM)
        hbm = pl.BlockSpec(memory_space=pl.ANY)
        cols = GROUP * own
        dma = pltpu.SemaphoreType.DMA
        return pl.pallas_call(
            functools.partial(body, n_dev),
            out_shape=jax.ShapeDtypeStruct(atom_act.shape, bf16),
            in_specs=[hbm, hbm, hbm, vmem, hbm, vmem, hbm, vmem, vmem, hbm, hbm, hbm],
            out_specs=hbm,
            scratch_shapes=[
                pltpu.VMEM(pair_t.shape, bf16),
                pltpu.VMEM(w_cond.shape, bf16),
                pltpu.VMEM(w_qkvg.shape, bf16),
                pltpu.VMEM(w_out.shape, bf16),
                pltpu.VMEM(w_up.shape, bf16),
                pltpu.VMEM(w_down.shape, bf16),
                pltpu.VMEM(cond.shape, bf16),
                pltpu.VMEM(atom_act.shape, bf16),
                pltpu.VMEM((half_smp, own, width), bf16),
                pltpu.VMEM((own, width), bf16),
                pltpu.VMEM((8, 128), jnp.int32),
                pltpu.VMEM((4, 8, 128), jnp.int32),
                pltpu.VMEM((n_layers, blocks, n_heads * QBLOCK, window), bf16),
                pltpu.VMEM((n_layers, 2, blocks, n_heads * QBLOCK, window), bf16),
                pltpu.VMEM((half_smp, own, width), bf16),
                pltpu.VMEM((n_groups, width, cols), f32),
                pltpu.VMEM((n_groups, width, cols), bf16),
                pltpu.VMEM((n_layers, half_smp, ext, width), bf16),
                pltpu.VMEM((n_layers, 6, width, own), f32),
                pltpu.VMEM((n_layers, n_blocks, KEY_WINDOW, 128), f32),
                pltpu.VMEM((n_layers, width, width), bf16),
                pltpu.VMEM((n_layers, width, width), bf16),
                pltpu.VMEM((n_layers, width, width), bf16),
                pltpu.VMEM((n_layers, 4 * width, width), bf16),
                pltpu.VMEM((n_layers, width, 2 * width), bf16),
                pltpu.VMEM((n_layers, 6 * width, width), bf16),
                pltpu.VMEM((n_layers, 4, width, own), f32),
                pltpu.VMEM((GROUP, ext, width), bf16),
                pltpu.VMEM((GROUP, n_blocks * 128, width), bf16),
                pltpu.VMEM((GROUP, width, ext), bf16),
                pltpu.VMEM((width, cols), f32),
                pltpu.VMEM((2, 2, KEY_WINDOW, 128), f32),
                pltpu.VMEM((2 * width, cols), bf16),
                pltpu.VMEM((width, cols), bf16),
                dma((12,)),
                dma((2,)),
                dma((n_layers, n_groups, 2)),
                dma((2,)),
                dma((2,)),
                dma((4,)),
                dma((4,)),
                dma((2,)),
                dma((2, n_groups)),
                dma((2,)),
                dma((2, n_layers)),
                dma((2,)),
                dma((2,)),
            ],
            compiler_params=pltpu.CompilerParams(
                collective_id=0, has_side_effects=True, vmem_limit_bytes=60 * 1024 * 1024),
        )(atom_act, cond, pair_t, atom_mask.reshape(1, seq), w_cond, b_cond, w_qkvg, b_query,
          w_pair, w_out, w_up, w_down)

    act_spec = P('dp', 'sp', None)
    in_specs = (act_spec, P('sp', None), P('sp', None, None, None), P('sp'), P(), P(), P(), P(), P(), P(), P(), P())
    return jax.shard_map(device_fn, mesh=mesh, in_specs=in_specs, out_specs=act_spec, check_vma=False)
```

```python
import functools
import math

import jax
import jax.numpy as jnp
from jax import lax
from jax.experimental import pallas as pl
from jax.experimental.pallas import tpu as pltpu
from jax.sharding import PartitionSpec as P

QBLOCK = 32
KEY_WINDOW = 128
EDGE = 48
LN_EPS = 1e-5
GROUP = 2
LOG2E = math.log2(math.e)
MESH = pl.DeviceIdType.MESH


def mm(lhs, rhs):
    return jnp.dot(lhs, rhs, preferred_element_type=jnp.float32)


def mm_nt(lhs, rhs):
    return lax.dot_general(lhs, rhs, (((1,), (1,)), ((), ())), preferred_element_type=jnp.float32)


def sigmoid(vals):
    return 0.5 * jnp.tanh(0.5 * vals) + 0.5


def norm(vals, axis):
    mean = jnp.mean(vals, axis=axis, keepdims=True)
    cent = vals - mean
    var = jnp.mean(cent * cent, axis=axis, keepdims=True)
    return cent * lax.rsqrt(var + LN_EPS)


def body(n_dev, act_hbm, cond_hbm, pair_hbm, mask_ref, wcond_hbm, bcond_ref, wqkvg_hbm, bquery_ref, wpair_ref,
         wout_hbm, wup_hbm, wdown_hbm, out_hbm,
         pair, wcond, wqkvg, wout, wup, wdown, cond_own, act,
         act_in, cond_in, mask_own, mask_in, bias_own, bias_in, out_stage,
         res, h_cm, h_ext, tab, bias, wv_t, wg_t, wo_t, wu_t, wd_t, wc_t, bc_t,
         k_scr, q_scr, v_scr, o_scr, s_scr, m_scr, h_mid,
         in_sem, send_sem, recv_sem, csend_sem, crecv_sem, msend_sem, mrecv_sem, asend_sem, arecv_sem,
         bsend_sem, brecv_sem, osend_sem, orecv_sem):
    n_layers, width = bquery_ref.shape
    n_heads = width // QBLOCK
    head_dim = width // n_heads
    samples, seq, _ = act_hbm.shape
    half_smp = samples // 2
    n_groups = half_smp // GROUP
    own = 2 * seq
    ext = own + 2 * EDGE
    n_blocks = own // QBLOCK
    f32, bf16 = jnp.float32, jnp.bfloat16

    me = lax.axis_index('sp')
    plane, row, core = me // 4, (me // 2) % 2, me % 2
    n_planes = n_dev // 4
    chunk = 2 * plane + core
    has_prev, has_next = chunk > 0, chunk < 2 * n_planes - 1

    def owner(chunk_idx, row_idx):
        return (chunk_idx // 2) * 4 + 2 * row_idx + chunk_idx % 2

    def remote(src, dst, ssem, rsem, peer):
        return pltpu.make_async_remote_copy(
            src_ref=src, dst_ref=dst, send_sem=ssem, recv_sem=rsem, device_id={'sp': peer}, device_id_type=MESH)

    def push(src, dst, ssem, rsem, peer):
        @pl.when(peer != me)
        def _():
            remote(src, dst, ssem, rsem, peer).start()

        @pl.when(peer == me)
        def _():
            pltpu.make_async_copy(src, dst, rsem).start()

    def push_done(src, dst, ssem, rsem, peer):
        @pl.when(peer != me)
        def _():
            remote(src, dst, ssem, rsem, peer).wait_send()

    def arrived(dst, rsem):
        pltpu.make_async_copy(dst, dst, rsem).wait()

    barrier = pltpu.get_barrier_semaphore()

    for other in range(4):
        peer = 4 * plane + other

        @pl.when(peer != me)
        def _():
            pl.semaphore_signal(barrier, inc=1, device_id={'sp': peer}, device_id_type=MESH)

    beyond = chunk + 2 * core - 1
    has_beyond = jnp.logical_and(beyond >= 0, beyond < 2 * n_planes)

    @pl.when(has_beyond)
    def _():
        pl.semaphore_signal(barrier, inc=1, device_id={'sp': owner(beyond, row)}, device_id_type=MESH)

    loads = [pltpu.make_async_copy(src, dst, in_sem.at[pos]) for pos, (src, dst) in enumerate(
        [(pair_hbm, pair), (wcond_hbm, wcond), (wqkvg_hbm, wqkvg), (wout_hbm, wout), (wup_hbm, wup), (wdown_hbm, wdown),
         (cond_hbm, cond_own), (act_hbm, act)])]
    for load in loads:
        load.start()

    def clear(first, slot):
        @pl.loop(0, n_layers)
        def _(layer):
            @pl.loop(0, n_groups)
            def _(grp):
                h_ext[layer, pl.ds(grp * GROUP, GROUP), first:first + EDGE, :] = jnp.zeros((GROUP, EDGE, width), bf16)

        mask_in[slot] = jnp.zeros_like(mask_own)

    @pl.when(jnp.logical_not(has_prev))
    def _():
        clear(0, 0)

    @pl.when(jnp.logical_not(has_next))
    def _():
        clear(EDGE + own, 3)

    mask_own[...] = jnp.zeros_like(mask_own)
    mask_own[0:1, 0:seq] = mask_ref[...]

    home = 2 * plane + row

    def cond_push(dest):
        return (cond_own, cond_in.at[pl.ds(core * seq, seq)], csend_sem.at[dest], crecv_sem.at[core], owner(home, dest))

    def mask_push(dest):
        return (mask_own, mask_in.at[1 + core], msend_sem.at[dest], mrecv_sem.at[1 + core], owner(home, dest))

    def mask_side(direction):
        return remote(mask_in.at[1 + direction], mask_in.at[3 - 3 * direction], msend_sem.at[2 + direction],
                      mrecv_sem.at[3 - 3 * direction], owner(chunk + 2 * direction - 1, row))

    def act_push(dest, grp):
        return (act.at[pl.ds(dest * half_smp + grp * GROUP, GROUP)],
                act_in.at[pl.ds(grp * GROUP, GROUP), pl.ds(core * seq, seq)],
                asend_sem.at[dest], arecv_sem.at[core, grp], owner(home, dest))

    def bias_push(dest, layer):
        return (bias_own.at[layer], bias_in.at[layer, core], bsend_sem.at[dest], brecv_sem.at[core, layer],
                owner(home, dest))

    c_pair = wpair_ref.shape[0]
    n_col = wpair_ref.shape[1]
    tall, deep = n_col * 16, 16 * c_pair
    pick_col = (lax.broadcasted_iota(jnp.int32, (tall, n_col), 0) // 16
                == lax.broadcasted_iota(jnp.int32, (tall, n_col), 1)).astype(bf16)
    pick_chan = (lax.broadcasted_iota(jnp.int32, (c_pair, deep), 1) % c_pair
                 == lax.broadcasted_iota(jnp.int32, (c_pair, deep), 0)).astype(bf16)
    spread = lax.dot_general(
        wpair_ref[...], pick_chan, (((0,), (0,)), ((), ())), preferred_element_type=f32).astype(bf16)
    spread = mm(pick_col, spread)
    same = (lax.broadcasted_iota(jnp.int32, (tall, deep), 0) % 16 == lax.broadcasted_iota(jnp.int32, (tall, deep), 1) // c_pair)
    w_block = jnp.where(same, spread, 0.0).astype(bf16)
    loads[0].wait()
    for part in range(seq // 16):
        vals = pair[part * deep:(part + 1) * deep].astype(f32).reshape(16, c_pair, KEY_WINDOW)
        vals = norm(vals, 1).astype(bf16).reshape(deep, KEY_WINDOW)
        res_bias = mm(w_block, vals).astype(bf16)
        blk, sub = part // 2, part % 2
        for layer in range(n_layers):
            for head in range(n_heads):
                col = layer * n_heads + head
                bias_own[layer, blk, head * QBLOCK + sub * 16:head * QBLOCK + (sub + 1) * 16, :] = res_bias[col * 16:(col + 1) * 16]
    half = jnp.array(0.5, bf16)

    def weights(layer):
        for idx, bias_idx in enumerate((0, None, 1, 2, None, 3)):
            piece = wcond[layer, :, idx * width:(idx + 1) * width].T
            wc_t[layer, idx * width:(idx + 1) * width, :] = piece if bias_idx is None else piece * half
            if bias_idx is not None:
                cell = bcond_ref[pl.ds(layer, 1), :][:, bias_idx * width:(bias_idx + 1) * width] * 0.5
                bc_t[layer, bias_idx] = jnp.broadcast_to(cell, (own, width)).T
        wv_t[layer] = wqkvg[layer, :, 2 * width:3 * width].T
        wg_t[layer] = wqkvg[layer, :, 3 * width:].T * half
        wo_t[layer] = wout[layer].T
        for idx in range(4):
            piece = wup[layer, :, idx * width:(idx + 1) * width].T
            wu_t[layer, idx * width:(idx + 1) * width, :] = piece * half if idx < 2 else piece
        for idx in range(2):
            wd_t[layer, :, idx * width:(idx + 1) * width] = wdown[layer, idx * width:(idx + 1) * width, :].T

    for load in loads[1:]:
        load.wait()

    weights(0)

    n_beyond = jnp.where(has_beyond, 1, 0)
    pl.semaphore_wait(barrier, 3 + n_beyond)

    for dest in range(2):
        push(*cond_push(dest))
    for grp in range(3):
        for dest in range(2):
            push(*act_push(dest, grp))
        if grp == 0:
            for dest in range(2):
                push(*mask_push(dest))
    for dest in range(2):
        push(*bias_push(dest, 0))
    for grp in range(3, n_groups):
        for dest in range(2):
            push(*act_push(dest, grp))
    for layer in range(1, n_layers):
        for dest in range(2):
            push(*bias_push(dest, layer))

    @pl.loop(1, n_layers)
    def _(layer):
        weights(layer)

    for slot in range(2):
        arrived(cond_in.at[pl.ds(slot * seq, seq)], crecv_sem.at[slot])
    cond_norm = norm(cond_in[...].astype(f32), -1).astype(bf16)

    def tables(layer, first=0, last=6):
        proj = mm_nt(wc_t[layer, first * width:last * width], cond_norm)
        yield
        for idx, bias_idx in list(enumerate((0, None, 1, 2, None, 3)))[first:last]:
            piece = proj[(idx - first) * width:(idx - first + 1) * width]
            if bias_idx is not None:
                piece = 0.5 * jnp.tanh(piece + bc_t[layer, bias_idx]) + 0.5
            tab[layer, idx] = piece
            yield

    def idle(rounds):
        for _ in range(rounds):
            yield

    def chain(*parts):
        for part in parts:
            yield from part

    def interleave(*stages):
        stages = list(stages)
        while stages:
            for stage in list(stages):
                if next(stage, stages) is stages:
                    stages.remove(stage)

    def both(vals):
        return jnp.concatenate([vals] * GROUP, axis=1)

    def halo_copy(layer, grp, direction):
        smp = pl.ds(grp * GROUP, GROUP)
        src = pl.ds(own if direction else EDGE, EDGE)
        dst = pl.ds(0 if direction else own + EDGE, EDGE)
        return remote(h_ext.at[layer, smp, src, :], h_ext.at[layer, smp, dst, :],
                      send_sem.at[direction], recv_sem.at[layer, grp, direction],
                      owner(chunk + 1 if direction else chunk - 1, row))

    def halo_start(layer, grp):
        @pl.when(has_prev)
        def _():
            halo_copy(layer, grp, 0).start()

        @pl.when(has_next)
        def _():
            halo_copy(layer, grp, 1).start()

    def halo_wait(layer, grp):
        @pl.when(has_next)
        def _():
            halo_copy(layer, grp, 0).wait_recv()

        @pl.when(has_prev)
        def _():
            halo_copy(layer, grp, 1).wait_recv()

    def emit_h(layer, grp, resid):
        h_t = (norm(resid, 0) * both(tab[layer, 0]) + both(tab[layer, 1])).astype(bf16)
        h_cm[grp] = h_t
        for smp in range(GROUP):
            h_ext[layer, grp * GROUP + smp, EDGE:EDGE + own, :] = h_t[:, smp * own:(smp + 1) * own].T

    def act_wait(grp):
        for slot in range(2):
            arrived(act_in.at[pl.ds(grp * GROUP, GROUP), pl.ds(slot * seq, seq)], arecv_sem.at[slot, grp])

    def enter(grp):
        cols = [act_in[grp * GROUP + smp].T.astype(f32) for smp in range(GROUP)]
        yield
        resid = jnp.concatenate(cols, axis=1)
        res[grp] = resid
        yield
        emit_h(0, grp, resid)
        yield

    def bias_wait(layer):
        for slot in range(2):
            arrived(bias_in.at[layer, slot], brecv_sem.at[slot, layer])

    def bias_table(layer, mask_bias):
        for blk in range(n_blocks):
            nat = bias_in[layer, blk // 2, blk % 2].astype(f32)
            order = [(slot - blk) % n_heads for slot in range(n_heads)]
            nat = jnp.concatenate([nat[head * QBLOCK:(head + 1) * QBLOCK] for head in order], axis=0)
            bias[layer, blk] = ((nat + mask_bias[:, blk * QBLOCK:blk * QBLOCK + KEY_WINDOW]) * LOG2E).T
            yield

    interleave(tables(0, 0, 2))
    act_wait(0)
    interleave(enter(0))
    halo_start(0, 0)
    act_wait(1)
    interleave(enter(1), chain(tables(0, 2, 6), tables(1)))
    halo_start(0, 1)
    for slot in range(1, 3):
        arrived(mask_in.at[slot], mrecv_sem.at[slot])

    @pl.when(has_prev)
    def _():
        mask_side(0).start()

    @pl.when(has_next)
    def _():
        mask_side(1).start()

    act_wait(2)
    interleave(enter(2), tables(2))
    halo_start(0, 2)
    @pl.when(has_prev)
    def _():
        arrived(mask_in.at[0], mrecv_sem.at[0])

    @pl.when(has_next)
    def _():
        arrived(mask_in.at[3], mrecv_sem.at[3])

    mask_row = jnp.concatenate([mask_in[0, 0:1, seq - EDGE:seq], mask_in[1, 0:1, :seq], mask_in[2, 0:1, :seq],
                                mask_in[3, 0:1, :EDGE], jnp.zeros((1, 256 - ext), jnp.int32)], axis=1)
    mask_bias = (mask_row.astype(f32) - 1.0) * 1e9
    bias_wait(0)
    act_wait(3)
    interleave(enter(3), bias_table(0, mask_bias))
    halo_start(0, 3)

    lane = lax.broadcasted_iota(jnp.int32, (1, width), 1)
    scale = head_dim ** -0.5 * LOG2E
    keep = [jnp.where(lane // QBLOCK == slot, 1.0, 0.0).astype(bf16) for slot in range(n_heads)]

    def split(idx):
        return idx // n_groups, idx % n_groups

    def project(idx):
        layer, grp = split(idx)
        w_qk = wqkvg[layer, :, :2 * width]
        b_q = bquery_ref[pl.ds(layer, 1), :]
        q_k = {}
        v_t = {}

        def k_q(smp):
            q_k[smp] = mm(h_ext[layer, grp * GROUP + smp], w_qk)

        def vals(smp):
            v_t[smp] = mm_nt(wv_t[layer], h_ext[layer, grp * GROUP + smp])

        def keys(smp):
            k_scr[smp] = q_k[smp][:, width:].astype(bf16)

        def queries(smp):
            q_val = (q_k[smp][EDGE:EDGE + own, :width] + b_q).astype(bf16)
            for blk in range(n_blocks):
                part = q_val[blk * QBLOCK:(blk + 1) * QBLOCK]
                for slot in range(n_heads):
                    first = blk * 128 + slot * QBLOCK
                    q_scr[smp, first:first + QBLOCK, :] = part * keep[(slot - blk) % n_heads]
                if blk % 2:
                    yield

        k_q(0)
        yield
        yield from idle(0)
        vals(0)
        yield
        yield from idle(0)
        keys(0)
        yield
        yield from queries(0)
        k_q(1)
        yield from idle(0)
        v_scr[0] = v_t[0].astype(bf16)
        yield
        vals(1)
        yield
        yield from idle(0)
        keys(1)
        yield
        yield from queries(1)
        yield from idle(2)
        v_scr[1] = v_t[1].astype(bf16)
        yield

    def score(unit):
        smp, duo = unit // 2, unit % 2
        return mm_nt(k_scr[smp, duo * 64:duo * 64 + 160], q_scr[smp, duo * 256:(duo + 1) * 256, :])

    def score_early():
        for unit in range(2):
            logit = score(unit)
            yield
            for sub in range(2):
                s_scr[unit, sub] = logit[sub * QBLOCK:sub * QBLOCK + KEY_WINDOW, sub * 128:(sub + 1) * 128]
            yield

    def attend(idx):
        layer, grp = split(idx)
        logits = {}
        out = {}

        def prob(unit, sub):
            blk = 2 * (unit % 2) + sub
            if unit < 2:
                x = s_scr[unit, sub]
            else:
                x = logits[unit][sub * QBLOCK:sub * QBLOCK + KEY_WINDOW, sub * 128:(sub + 1) * 128]
            x = x * scale + bias[layer, blk]
            e = jnp.exp2(x - jnp.max(x, axis=0, keepdims=True))
            p = (e * (0.5 / jnp.sum(e, axis=0, keepdims=True))).astype(bf16)
            parts = [p]
            if blk:
                parts = [jnp.zeros((blk * QBLOCK, 128), bf16)] + parts
            if blk < n_blocks - 1:
                parts = parts + [jnp.zeros(((n_blocks - 1 - blk) * QBLOCK, 128), bf16)]
            return jnp.concatenate(parts, axis=0)

        def place(unit):
            smp, duo = unit // 2, unit % 2
            cols = slice(smp * own, (smp + 1) * own)
            for head in range(n_heads):
                rows = slice(head * head_dim, (head + 1) * head_dim)
                pair_out = [out[unit][rows, sub * 128:(sub + 1) * 128] for sub in range(2)]
                pick = lane // QBLOCK == (head + 2 * duo + 1) % n_heads
                merged = jnp.where(pick, pair_out[1], pair_out[0])
                if duo:
                    first = lane // QBLOCK == (head + 2) % n_heads
                    merged = jnp.where(jnp.logical_or(pick, first), merged, o_scr[rows, cols])
                o_scr[rows, cols] = merged

        for unit in range(2 * GROUP):
            if unit >= 2:
                logits[unit] = score(unit) if unit not in logits else logits[unit]
            probs = []
            for sub in range(2):
                probs.append(prob(unit, sub))
                yield
            out[unit] = mm(v_scr[unit // 2], jnp.concatenate(probs, axis=1))
            if unit + 2 < 2 * GROUP and unit + 2 >= 2:
                logits[unit + 2] = score(unit + 2)
            if unit:
                place(unit - 1)
            yield
        place(2 * GROUP - 1)
        yield

    def mix(idx):
        layer, grp = split(idx)
        gate = mm(wg_t[layer], h_cm[grp])
        yield
        yield from idle(2)
        heads = []
        for head in range(n_heads):
            rows = slice(head * head_dim, (head + 1) * head_dim)
            parts = []
            for smp in range(GROUP):
                part = o_scr[rows, smp * own:(smp + 1) * own]
                parts.append(pltpu.roll(part, (128 - head * QBLOCK) % 128, 1) if head else part)
            heads.append(jnp.concatenate(parts, axis=1))
        o_val = ((jnp.tanh(gate) + 1.0) * jnp.concatenate(heads, axis=0)).astype(bf16)
        proj = mm(wo_t[layer], o_val)
        yield
        yield from idle(2)
        resid = res[grp] + both(tab[layer, 2]) * proj
        res[grp] = resid
        yield
        yield from idle(4)
        h_mid[...] = (norm(resid, 0) * both(tab[layer, 3]) + both(tab[layer, 4])).astype(bf16)
        yield

    def finish(idx, last):
        layer, grp = split(idx)
        h_t = h_mid[...]
        n_chunk = 2
        rows = 2 * width // n_chunk
        ups = {}
        for pos in range(n_chunk + 1):
            if pos < n_chunk:
                ups[pos] = [mm(wu_t[layer, pl.ds(base + pos * rows, rows), :], h_t) for base in (0, 2 * width)]
                yield
                if pos == 0:
                    yield from idle(1)
            if pos:
                left, right = ups[pos - 1]
                m_scr[(pos - 1) * rows:pos * rows, :] = ((left * jnp.tanh(left) + left) * right).astype(bf16)
                yield
        down = mm(wd_t[layer], m_scr[...])
        yield
        yield from idle(0)
        resid = res[grp] + both(tab[layer, 5]) * down
        yield
        if last:
            for smp in range(GROUP):
                out_stage[grp * GROUP + smp] = resid[:, smp * own:(smp + 1) * own].astype(bf16).T
                yield
        else:
            res[grp] = resid
            yield
            emit_h(layer + 1, grp, resid)
            yield

    def out_push(grp, slot):
        return (out_stage.at[pl.ds(grp * GROUP, GROUP), pl.ds(slot * seq, seq)],
                out_hbm.at[pl.ds(row * half_smp + grp * GROUP, GROUP)],
                osend_sem.at[slot], orecv_sem.at[row], 4 * plane + 2 * core + slot)

    def sent(idx, last):
        layer, grp = split(idx)
        if last:
            for slot in range(2):
                push(*out_push(grp, slot))
        else:
            halo_start(layer + 1, grp)

    def loop_body(idx, last, *extra):
        halo_wait(*split(idx + 1))
        interleave(chain(idle(1), finish(idx - 2, last)), chain(idle(0), mix(idx - 1)), attend(idx), chain(idle(2), project(idx + 1)), chain(idle(10), score_early()), *extra)
        sent(idx - 2, last)

    n_steps = n_layers * n_groups
    split_at = n_steps - n_groups
    act_wait(4)
    halo_wait(0, 0)
    interleave(enter(4), chain(project(0), score_early()))
    halo_start(0, 4)
    act_wait(5)
    halo_wait(0, 1)
    interleave(attend(0), chain(project(1), score_early()), enter(5))
    halo_start(0, 5)
    act_wait(6)
    halo_wait(0, 2)
    interleave(mix(0), attend(1), chain(project(2), score_early()), enter(6))
    halo_start(0, 6)
    act_wait(7)
    loop_body(2, False, enter(7))
    halo_start(0, 7)

    @pl.loop(3, 7)
    def _(idx):
        loop_body(idx, False)

    bias_wait(1)
    loop_body(7, False, bias_table(1, mask_bias))

    @pl.loop(8, 12)
    def _(idx):
        loop_body(idx, False)

    bias_wait(2)
    loop_body(12, False, bias_table(2, mask_bias))

    @pl.loop(13, split_at + 2)
    def _(idx):
        loop_body(idx, False)

    @pl.loop(split_at + 2, n_steps - 1)
    def _(idx):
        loop_body(idx, True)

    interleave(finish(n_steps - 3, True), mix(n_steps - 2), attend(n_steps - 1))
    sent(n_steps - 3, True)
    interleave(finish(n_steps - 2, True), mix(n_steps - 1))
    sent(n_steps - 2, True)
    interleave(finish(n_steps - 1, True))
    sent(n_steps - 1, True)

    def drained(src, ssem):
        pltpu.make_async_copy(src, src, ssem).wait()

    for dest in range(2):
        push_done(*cond_push(dest))
        push_done(*mask_push(dest))

        @pl.when(owner(home, dest) != me)
        def _():
            drained(bias_own, bsend_sem.at[dest])
            drained(act.at[pl.ds(0, half_smp)], asend_sem.at[dest])

        @pl.when(4 * plane + 2 * core + dest != me)
        def _():
            drained(out_stage.at[:, pl.ds(0, seq)], osend_sem.at[dest])

    @pl.when(has_prev)
    def _():
        mask_side(0).wait_send()
        drained(h_ext.at[:, :, pl.ds(0, EDGE)], send_sem.at[0])

    @pl.when(has_next)
    def _():
        mask_side(1).wait_send()
        drained(h_ext.at[:, :, pl.ds(0, EDGE)], send_sem.at[1])

    for dest in range(2):
        arrived(out_hbm.at[pl.ds(dest * half_smp, half_smp)], orecv_sem.at[dest])


def solution(mesh):
    n_dev = mesh.shape['sp']

    def device_fn(atom_act, cond, pair, atom_mask, w_cond, b_cond, w_qkvg, b_query, w_pair, w_out, w_up, w_down):
        samples, seq, width = atom_act.shape
        n_layers = w_qkvg.shape[0]
        n_heads = width // QBLOCK
        half_smp = samples // 2
        n_groups = half_smp // GROUP
        own = 2 * seq
        ext = own + 2 * EDGE
        n_blocks = own // QBLOCK
        blocks, _, window, c_pair = pair.shape
        f32, bf16 = jnp.float32, jnp.bfloat16
        pair_t = pair.transpose(0, 1, 3, 2).reshape(blocks * QBLOCK * c_pair, window)
        vmem = pl.BlockSpec(memory_space=pltpu.VMEM)
        hbm = pl.BlockSpec(memory_space=pl.ANY)
        cols = GROUP * own
        dma = pltpu.SemaphoreType.DMA
        return pl.pallas_call(
            functools.partial(body, n_dev),
            out_shape=jax.ShapeDtypeStruct(atom_act.shape, bf16),
            in_specs=[hbm, hbm, hbm, vmem, hbm, vmem, hbm, vmem, vmem, hbm, hbm, hbm],
            out_specs=hbm,
            scratch_shapes=[
                pltpu.VMEM(pair_t.shape, bf16),
                pltpu.VMEM(w_cond.shape, bf16),
                pltpu.VMEM(w_qkvg.shape, bf16),
                pltpu.VMEM(w_out.shape, bf16),
                pltpu.VMEM(w_up.shape, bf16),
                pltpu.VMEM(w_down.shape, bf16),
                pltpu.VMEM(cond.shape, bf16),
                pltpu.VMEM(atom_act.shape, bf16),
                pltpu.VMEM((half_smp, own, width), bf16),
                pltpu.VMEM((own, width), bf16),
                pltpu.VMEM((8, 128), jnp.int32),
                pltpu.VMEM((4, 8, 128), jnp.int32),
                pltpu.VMEM((n_layers, blocks, n_heads * QBLOCK, window), bf16),
                pltpu.VMEM((n_layers, 2, blocks, n_heads * QBLOCK, window), bf16),
                pltpu.VMEM((half_smp, own, width), bf16),
                pltpu.VMEM((n_groups, width, cols), f32),
                pltpu.VMEM((n_groups, width, cols), bf16),
                pltpu.VMEM((n_layers, half_smp, ext, width), bf16),
                pltpu.VMEM((n_layers, 6, width, own), f32),
                pltpu.VMEM((n_layers, n_blocks, KEY_WINDOW, 128), f32),
                pltpu.VMEM((n_layers, width, width), bf16),
                pltpu.VMEM((n_layers, width, width), bf16),
                pltpu.VMEM((n_layers, width, width), bf16),
                pltpu.VMEM((n_layers, 4 * width, width), bf16),
                pltpu.VMEM((n_layers, width, 2 * width), bf16),
                pltpu.VMEM((n_layers, 6 * width, width), bf16),
                pltpu.VMEM((n_layers, 4, width, own), f32),
                pltpu.VMEM((GROUP, ext, width), bf16),
                pltpu.VMEM((GROUP, n_blocks * 128, width), bf16),
                pltpu.VMEM((GROUP, width, ext), bf16),
                pltpu.VMEM((width, cols), f32),
                pltpu.VMEM((2, 2, KEY_WINDOW, 128), f32),
                pltpu.VMEM((2 * width, cols), bf16),
                pltpu.VMEM((width, cols), bf16),
                dma((12,)),
                dma((2,)),
                dma((n_layers, n_groups, 2)),
                dma((2,)),
                dma((2,)),
                dma((4,)),
                dma((4,)),
                dma((2,)),
                dma((2, n_groups)),
                dma((2,)),
                dma((2, n_layers)),
                dma((2,)),
                dma((2,)),
            ],
            compiler_params=pltpu.CompilerParams(
                collective_id=0, has_side_effects=True, vmem_limit_bytes=60 * 1024 * 1024),
        )(atom_act, cond, pair_t, atom_mask.reshape(1, seq), w_cond, b_cond, w_qkvg, b_query,
          w_pair, w_out, w_up, w_down)

    act_spec = P('dp', 'sp', None)
    in_specs = (act_spec, P('sp', None), P('sp', None, None, None), P('sp'), P(), P(), P(), P(), P(), P(), P(), P())
    return jax.shard_map(device_fn, mesh=mesh, in_specs=in_specs, out_specs=act_spec, check_vma=False)
```

```python
import functools
import math

import jax
import jax.numpy as jnp
from jax import lax
from jax.experimental import pallas as pl
from jax.experimental.pallas import tpu as pltpu
from jax.sharding import PartitionSpec as P

QBLOCK = 32
KEY_WINDOW = 128
EDGE = 48
LN_EPS = 1e-5
GROUP = 2
LOG2E = math.log2(math.e)
MESH = pl.DeviceIdType.MESH


def mm(lhs, rhs):
    return jnp.dot(lhs, rhs, preferred_element_type=jnp.float32)


def mm_nt(lhs, rhs):
    return lax.dot_general(lhs, rhs, (((1,), (1,)), ((), ())), preferred_element_type=jnp.float32)


def sigmoid(vals):
    return 0.5 * jnp.tanh(0.5 * vals) + 0.5


def norm(vals, axis):
    mean = jnp.mean(vals, axis=axis, keepdims=True)
    cent = vals - mean
    var = jnp.mean(cent * cent, axis=axis, keepdims=True)
    return cent * lax.rsqrt(var + LN_EPS)


def body(n_dev, act_hbm, cond_hbm, pair_hbm, mask_ref, wcond_hbm, bcond_ref, wqkvg_hbm, bquery_ref, wpair_ref,
         wout_hbm, wup_hbm, wdown_hbm, out_hbm,
         pair, wcond, wqkvg, wout, wup, wdown, cond_own, act,
         act_in, cond_in, mask_own, mask_in, bias_own, bias_in, out_stage,
         res, h_cm, h_ext, tab, bias, wv_t, wg_t, wo_t, wu_t, wd_t, wc_t, bc_t,
         k_scr, q_scr, v_scr, o_scr, s_scr, m_scr, h_mid,
         in_sem, send_sem, recv_sem, csend_sem, crecv_sem, msend_sem, mrecv_sem, asend_sem, arecv_sem,
         bsend_sem, brecv_sem, osend_sem, orecv_sem):
    n_layers, width = bquery_ref.shape
    n_heads = width // QBLOCK
    head_dim = width // n_heads
    samples, seq, _ = act_hbm.shape
    half_smp = samples // 2
    n_groups = half_smp // GROUP
    own = 2 * seq
    ext = own + 2 * EDGE
    n_blocks = own // QBLOCK
    f32, bf16 = jnp.float32, jnp.bfloat16

    me = lax.axis_index('sp')
    plane, row, core = me // 4, (me // 2) % 2, me % 2
    n_planes = n_dev // 4
    chunk = 2 * plane + core
    has_prev, has_next = chunk > 0, chunk < 2 * n_planes - 1

    def owner(chunk_idx, row_idx):
        return (chunk_idx // 2) * 4 + 2 * row_idx + chunk_idx % 2

    def remote(src, dst, ssem, rsem, peer):
        return pltpu.make_async_remote_copy(
            src_ref=src, dst_ref=dst, send_sem=ssem, recv_sem=rsem, device_id={'sp': peer}, device_id_type=MESH)

    def push(src, dst, ssem, rsem, peer):
        @pl.when(peer != me)
        def _():
            remote(src, dst, ssem, rsem, peer).start()

        @pl.when(peer == me)
        def _():
            pltpu.make_async_copy(src, dst, rsem).start()

    def push_done(src, dst, ssem, rsem, peer):
        @pl.when(peer != me)
        def _():
            remote(src, dst, ssem, rsem, peer).wait_send()

    def arrived(dst, rsem):
        pltpu.make_async_copy(dst, dst, rsem).wait()

    barrier = pltpu.get_barrier_semaphore()

    for other in range(4):
        peer = 4 * plane + other

        @pl.when(peer != me)
        def _():
            pl.semaphore_signal(barrier, inc=1, device_id={'sp': peer}, device_id_type=MESH)

    beyond = chunk + 2 * core - 1
    has_beyond = jnp.logical_and(beyond >= 0, beyond < 2 * n_planes)

    @pl.when(has_beyond)
    def _():
        pl.semaphore_signal(barrier, inc=1, device_id={'sp': owner(beyond, row)}, device_id_type=MESH)

    loads = [pltpu.make_async_copy(src, dst, in_sem.at[pos]) for pos, (src, dst) in enumerate(
        [(pair_hbm, pair), (wcond_hbm, wcond), (wqkvg_hbm, wqkvg), (wout_hbm, wout), (wup_hbm, wup), (wdown_hbm, wdown),
         (cond_hbm, cond_own), (act_hbm, act)])]
    for load in loads:
        load.start()

    def clear(first, slot):
        @pl.loop(0, n_layers)
        def _(layer):
            @pl.loop(0, n_groups)
            def _(grp):
                h_ext[layer, pl.ds(grp * GROUP, GROUP), first:first + EDGE, :] = jnp.zeros((GROUP, EDGE, width), bf16)

        mask_in[slot] = jnp.zeros_like(mask_own)

    @pl.when(jnp.logical_not(has_prev))
    def _():
        clear(0, 0)

    @pl.when(jnp.logical_not(has_next))
    def _():
        clear(EDGE + own, 3)

    mask_own[...] = jnp.zeros_like(mask_own)
    mask_own[0:1, 0:seq] = mask_ref[...]

    home = 2 * plane + row

    def cond_push(dest):
        return (cond_own, cond_in.at[pl.ds(core * seq, seq)], csend_sem.at[dest], crecv_sem.at[core], owner(home, dest))

    def mask_push(dest):
        return (mask_own, mask_in.at[1 + core], msend_sem.at[dest], mrecv_sem.at[1 + core], owner(home, dest))

    def mask_side(direction):
        return remote(mask_in.at[1 + direction], mask_in.at[3 - 3 * direction], msend_sem.at[2 + direction],
                      mrecv_sem.at[3 - 3 * direction], owner(chunk + 2 * direction - 1, row))

    def act_push(dest, grp):
        return (act.at[pl.ds(dest * half_smp + grp * GROUP, GROUP)],
                act_in.at[pl.ds(grp * GROUP, GROUP), pl.ds(core * seq, seq)],
                asend_sem.at[dest], arecv_sem.at[core, grp], owner(home, dest))

    def bias_push(dest, layer):
        return (bias_own.at[layer], bias_in.at[layer, core], bsend_sem.at[dest], brecv_sem.at[core, layer],
                owner(home, dest))

    c_pair = wpair_ref.shape[0]
    n_col = wpair_ref.shape[1]
    tall, deep = n_col * 16, 16 * c_pair
    pick_col = (lax.broadcasted_iota(jnp.int32, (tall, n_col), 0) // 16
                == lax.broadcasted_iota(jnp.int32, (tall, n_col), 1)).astype(bf16)
    pick_chan = (lax.broadcasted_iota(jnp.int32, (c_pair, deep), 1) % c_pair
                 == lax.broadcasted_iota(jnp.int32, (c_pair, deep), 0)).astype(bf16)
    spread = lax.dot_general(
        wpair_ref[...], pick_chan, (((0,), (0,)), ((), ())), preferred_element_type=f32).astype(bf16)
    spread = mm(pick_col, spread)
    same = (lax.broadcasted_iota(jnp.int32, (tall, deep), 0) % 16 == lax.broadcasted_iota(jnp.int32, (tall, deep), 1) // c_pair)
    w_block = jnp.where(same, spread, 0.0).astype(bf16)
    loads[0].wait()
    for part in range(seq // 16):
        vals = pair[part * deep:(part + 1) * deep].astype(f32).reshape(16, c_pair, KEY_WINDOW)
        vals = norm(vals, 1).astype(bf16).reshape(deep, KEY_WINDOW)
        res_bias = mm(w_block, vals).astype(bf16)
        blk, sub = part // 2, part % 2
        for layer in range(n_layers):
            for head in range(n_heads):
                col = layer * n_heads + head
                bias_own[layer, blk, head * QBLOCK + sub * 16:head * QBLOCK + (sub + 1) * 16, :] = res_bias[col * 16:(col + 1) * 16]
    half = jnp.array(0.5, bf16)

    def weights(layer):
        for idx, bias_idx in enumerate((0, None, 1, 2, None, 3)):
            piece = wcond[layer, :, idx * width:(idx + 1) * width].T
            wc_t[layer, idx * width:(idx + 1) * width, :] = piece if bias_idx is None else piece * half
            if bias_idx is not None:
                cell = bcond_ref[pl.ds(layer, 1), :][:, bias_idx * width:(bias_idx + 1) * width] * 0.5
                bc_t[layer, bias_idx] = jnp.broadcast_to(cell, (own, width)).T
        wv_t[layer] = wqkvg[layer, :, 2 * width:3 * width].T
        wg_t[layer] = wqkvg[layer, :, 3 * width:].T * half
        wo_t[layer] = wout[layer].T
        for idx in range(4):
            piece = wup[layer, :, idx * width:(idx + 1) * width].T
            wu_t[layer, idx * width:(idx + 1) * width, :] = piece * half if idx < 2 else piece
        for idx in range(2):
            wd_t[layer, :, idx * width:(idx + 1) * width] = wdown[layer, idx * width:(idx + 1) * width, :].T

    for load in loads[1:]:
        load.wait()

    weights(0)

    n_beyond = jnp.where(has_beyond, 1, 0)
    pl.semaphore_wait(barrier, 3 + n_beyond)

    for dest in (1 - row, row):
        push(*cond_push(dest))
    for grp in range(3):
        for dest in (1 - row, row):
            push(*act_push(dest, grp))
        if grp == 0:
            for dest in (1 - row, row):
                push(*mask_push(dest))
    for dest in (1 - row, row):
        push(*bias_push(dest, 0))
    for grp in range(3, n_groups):
        for dest in (1 - row, row):
            push(*act_push(dest, grp))
    for layer in range(1, n_layers):
        for dest in (1 - row, row):
            push(*bias_push(dest, layer))

    @pl.loop(1, n_layers)
    def _(layer):
        weights(layer)

    for slot in range(2):
        arrived(cond_in.at[pl.ds(slot * seq, seq)], crecv_sem.at[slot])
    cond_norm = norm(cond_in[...].astype(f32), -1).astype(bf16)

    def tables(layer, first=0, last=6):
        proj = mm_nt(wc_t[layer, first * width:last * width], cond_norm)
        yield
        for idx, bias_idx in list(enumerate((0, None, 1, 2, None, 3)))[first:last]:
            piece = proj[(idx - first) * width:(idx - first + 1) * width]
            if bias_idx is not None:
                piece = 0.5 * jnp.tanh(piece + bc_t[layer, bias_idx]) + 0.5
            tab[layer, idx] = piece
            yield

    def idle(rounds):
        for _ in range(rounds):
            yield

    def chain(*parts):
        for part in parts:
            yield from part

    def interleave(*stages):
        stages = list(stages)
        while stages:
            for stage in list(stages):
                if next(stage, stages) is stages:
                    stages.remove(stage)

    def both(vals):
        return jnp.concatenate([vals] * GROUP, axis=1)

    def halo_copy(layer, grp, direction):
        smp = pl.ds(grp * GROUP, GROUP)
        src = pl.ds(own if direction else EDGE, EDGE)
        dst = pl.ds(0 if direction else own + EDGE, EDGE)
        return remote(h_ext.at[layer, smp, src, :], h_ext.at[layer, smp, dst, :],
                      send_sem.at[direction], recv_sem.at[layer, grp, direction],
                      owner(chunk + 1 if direction else chunk - 1, row))

    def halo_start(layer, grp):
        @pl.when(has_prev)
        def _():
            halo_copy(layer, grp, 0).start()

        @pl.when(has_next)
        def _():
            halo_copy(layer, grp, 1).start()

    def halo_wait(layer, grp):
        @pl.when(has_next)
        def _():
            halo_copy(layer, grp, 0).wait_recv()

        @pl.when(has_prev)
        def _():
            halo_copy(layer, grp, 1).wait_recv()

    def emit_h(layer, grp, resid):
        h_t = (norm(resid, 0) * both(tab[layer, 0]) + both(tab[layer, 1])).astype(bf16)
        h_cm[grp] = h_t
        for smp in range(GROUP):
            h_ext[layer, grp * GROUP + smp, EDGE:EDGE + own, :] = h_t[:, smp * own:(smp + 1) * own].T

    def act_wait(grp):
        for slot in range(2):
            arrived(act_in.at[pl.ds(grp * GROUP, GROUP), pl.ds(slot * seq, seq)], arecv_sem.at[slot, grp])

    def enter(grp):
        cols = [act_in[grp * GROUP + smp].T.astype(f32) for smp in range(GROUP)]
        yield
        resid = jnp.concatenate(cols, axis=1)
        res[grp] = resid
        yield
        emit_h(0, grp, resid)
        yield

    def bias_wait(layer):
        for slot in range(2):
            arrived(bias_in.at[layer, slot], brecv_sem.at[slot, layer])

    def bias_table(layer, mask_bias):
        for blk in range(n_blocks):
            nat = bias_in[layer, blk // 2, blk % 2].astype(f32)
            order = [(slot - blk) % n_heads for slot in range(n_heads)]
            nat = jnp.concatenate([nat[head * QBLOCK:(head + 1) * QBLOCK] for head in order], axis=0)
            bias[layer, blk] = ((nat + mask_bias[:, blk * QBLOCK:blk * QBLOCK + KEY_WINDOW]) * LOG2E).T
            yield

    interleave(tables(0, 0, 2))
    act_wait(0)
    interleave(enter(0))
    halo_start(0, 0)
    act_wait(1)
    interleave(enter(1), chain(tables(0, 2, 6), tables(1)))
    halo_start(0, 1)
    for slot in range(1, 3):
        arrived(mask_in.at[slot], mrecv_sem.at[slot])

    @pl.when(has_prev)
    def _():
        mask_side(0).start()

    @pl.when(has_next)
    def _():
        mask_side(1).start()

    act_wait(2)
    interleave(enter(2), tables(2))
    halo_start(0, 2)
    @pl.when(has_prev)
    def _():
        arrived(mask_in.at[0], mrecv_sem.at[0])

    @pl.when(has_next)
    def _():
        arrived(mask_in.at[3], mrecv_sem.at[3])

    mask_row = jnp.concatenate([mask_in[0, 0:1, seq - EDGE:seq], mask_in[1, 0:1, :seq], mask_in[2, 0:1, :seq],
                                mask_in[3, 0:1, :EDGE], jnp.zeros((1, 256 - ext), jnp.int32)], axis=1)
    mask_bias = (mask_row.astype(f32) - 1.0) * 1e9
    bias_wait(0)
    act_wait(3)
    interleave(enter(3), bias_table(0, mask_bias))
    halo_start(0, 3)

    lane = lax.broadcasted_iota(jnp.int32, (1, width), 1)
    scale = head_dim ** -0.5 * LOG2E
    keep = [jnp.where(lane // QBLOCK == slot, 1.0, 0.0).astype(bf16) for slot in range(n_heads)]

    def split(idx):
        return idx // n_groups, idx % n_groups

    def project(idx):
        layer, grp = split(idx)
        w_qk = wqkvg[layer, :, :2 * width]
        b_q = bquery_ref[pl.ds(layer, 1), :]
        q_k = {}
        v_t = {}

        def k_q(smp):
            q_k[smp] = mm(h_ext[layer, grp * GROUP + smp], w_qk)

        def vals(smp):
            v_t[smp] = mm_nt(wv_t[layer], h_ext[layer, grp * GROUP + smp])

        def keys(smp):
            k_scr[smp] = q_k[smp][:, width:].astype(bf16)

        def queries(smp):
            q_val = (q_k[smp][EDGE:EDGE + own, :width] + b_q).astype(bf16)
            for blk in range(n_blocks):
                part = q_val[blk * QBLOCK:(blk + 1) * QBLOCK]
                for slot in range(n_heads):
                    first = blk * 128 + slot * QBLOCK
                    q_scr[smp, first:first + QBLOCK, :] = part * keep[(slot - blk) % n_heads]
                if blk % 2:
                    yield

        k_q(0)
        yield
        yield from idle(0)
        vals(0)
        yield
        yield from idle(0)
        keys(0)
        yield
        yield from queries(0)
        k_q(1)
        yield from idle(0)
        v_scr[0] = v_t[0].astype(bf16)
        yield
        vals(1)
        yield
        yield from idle(0)
        keys(1)
        yield
        yield from queries(1)
        yield from idle(2)
        v_scr[1] = v_t[1].astype(bf16)
        yield

    def score(unit):
        smp, duo = unit // 2, unit % 2
        return mm_nt(k_scr[smp, duo * 64:duo * 64 + 160], q_scr[smp, duo * 256:(duo + 1) * 256, :])

    def score_early():
        for unit in range(2):
            logit = score(unit)
            yield
            for sub in range(2):
                s_scr[unit, sub] = logit[sub * QBLOCK:sub * QBLOCK + KEY_WINDOW, sub * 128:(sub + 1) * 128]
            yield

    def attend(idx):
        layer, grp = split(idx)
        logits = {}
        out = {}

        def prob(unit, sub):
            blk = 2 * (unit % 2) + sub
            if unit < 2:
                x = s_scr[unit, sub]
            else:
                x = logits[unit][sub * QBLOCK:sub * QBLOCK + KEY_WINDOW, sub * 128:(sub + 1) * 128]
            x = x * scale + bias[layer, blk]
            e = jnp.exp2(x - jnp.max(x, axis=0, keepdims=True))
            p = (e * (0.5 / jnp.sum(e, axis=0, keepdims=True))).astype(bf16)
            parts = [p]
            if blk:
                parts = [jnp.zeros((blk * QBLOCK, 128), bf16)] + parts
            if blk < n_blocks - 1:
                parts = parts + [jnp.zeros(((n_blocks - 1 - blk) * QBLOCK, 128), bf16)]
            return jnp.concatenate(parts, axis=0)

        def place(unit):
            smp, duo = unit // 2, unit % 2
            cols = slice(smp * own, (smp + 1) * own)
            for head in range(n_heads):
                rows = slice(head * head_dim, (head + 1) * head_dim)
                pair_out = [out[unit][rows, sub * 128:(sub + 1) * 128] for sub in range(2)]
                pick = lane // QBLOCK == (head + 2 * duo + 1) % n_heads
                merged = jnp.where(pick, pair_out[1], pair_out[0])
                if duo:
                    first = lane // QBLOCK == (head + 2) % n_heads
                    merged = jnp.where(jnp.logical_or(pick, first), merged, o_scr[rows, cols])
                o_scr[rows, cols] = merged

        for unit in range(2 * GROUP):
            if unit >= 2:
                logits[unit] = score(unit) if unit not in logits else logits[unit]
            probs = []
            for sub in range(2):
                probs.append(prob(unit, sub))
                yield
            out[unit] = mm(v_scr[unit // 2], jnp.concatenate(probs, axis=1))
            if unit + 2 < 2 * GROUP and unit + 2 >= 2:
                logits[unit + 2] = score(unit + 2)
            if unit:
                place(unit - 1)
            yield
        place(2 * GROUP - 1)
        yield

    def mix(idx):
        layer, grp = split(idx)
        gate = mm(wg_t[layer], h_cm[grp])
        yield
        yield from idle(2)
        heads = []
        for head in range(n_heads):
            rows = slice(head * head_dim, (head + 1) * head_dim)
            parts = []
            for smp in range(GROUP):
                part = o_scr[rows, smp * own:(smp + 1) * own]
                parts.append(pltpu.roll(part, (128 - head * QBLOCK) % 128, 1) if head else part)
            heads.append(jnp.concatenate(parts, axis=1))
        o_val = ((jnp.tanh(gate) + 1.0) * jnp.concatenate(heads, axis=0)).astype(bf16)
        proj = mm(wo_t[layer], o_val)
        yield
        yield from idle(2)
        resid = res[grp] + both(tab[layer, 2]) * proj
        res[grp] = resid
        yield
        yield from idle(4)
        h_mid[...] = (norm(resid, 0) * both(tab[layer, 3]) + both(tab[layer, 4])).astype(bf16)
        yield

    def finish(idx, last):
        layer, grp = split(idx)
        h_t = h_mid[...]
        n_chunk = 2
        rows = 2 * width // n_chunk
        ups = {}
        for pos in range(n_chunk + 1):
            if pos < n_chunk:
                ups[pos] = [mm(wu_t[layer, pl.ds(base + pos * rows, rows), :], h_t) for base in (0, 2 * width)]
                yield
                if pos == 0:
                    yield from idle(1)
            if pos:
                left, right = ups[pos - 1]
                m_scr[(pos - 1) * rows:pos * rows, :] = ((left * jnp.tanh(left) + left) * right).astype(bf16)
                yield
        down = mm(wd_t[layer], m_scr[...])
        yield
        yield from idle(0)
        resid = res[grp] + both(tab[layer, 5]) * down
        yield
        if last:
            for smp in range(GROUP):
                out_stage[grp * GROUP + smp] = resid[:, smp * own:(smp + 1) * own].astype(bf16).T
                yield
        else:
            res[grp] = resid
            yield
            emit_h(layer + 1, grp, resid)
            yield

    def out_push(grp, slot):
        return (out_stage.at[pl.ds(grp * GROUP, GROUP), pl.ds(slot * seq, seq)],
                out_hbm.at[pl.ds(row * half_smp + grp * GROUP, GROUP)],
                osend_sem.at[slot], orecv_sem.at[row], 4 * plane + 2 * core + slot)

    def sent(idx, last):
        layer, grp = split(idx)
        if last:
            for slot in range(2):
                push(*out_push(grp, slot))
        else:
            halo_start(layer + 1, grp)

    def loop_body(idx, last, *extra):
        halo_wait(*split(idx + 1))
        interleave(chain(idle(1), finish(idx - 2, last)), chain(idle(0), mix(idx - 1)), attend(idx), chain(idle(2), project(idx + 1)), chain(idle(10), score_early()), *extra)
        sent(idx - 2, last)

    n_steps = n_layers * n_groups
    split_at = n_steps - n_groups
    act_wait(4)
    halo_wait(0, 0)
    interleave(enter(4), chain(project(0), score_early()))
    halo_start(0, 4)
    act_wait(5)
    halo_wait(0, 1)
    interleave(attend(0), chain(project(1), score_early()), enter(5))
    halo_start(0, 5)
    act_wait(6)
    halo_wait(0, 2)
    interleave(mix(0), attend(1), chain(project(2), score_early()), enter(6))
    halo_start(0, 6)
    act_wait(7)
    loop_body(2, False, enter(7))
    halo_start(0, 7)

    @pl.loop(3, 7)
    def _(idx):
        loop_body(idx, False)

    bias_wait(1)
    loop_body(7, False, bias_table(1, mask_bias))

    @pl.loop(8, 12)
    def _(idx):
        loop_body(idx, False)

    bias_wait(2)
    loop_body(12, False, bias_table(2, mask_bias))

    @pl.loop(13, split_at + 2)
    def _(idx):
        loop_body(idx, False)

    @pl.loop(split_at + 2, n_steps - 1)
    def _(idx):
        loop_body(idx, True)

    interleave(finish(n_steps - 3, True), mix(n_steps - 2), attend(n_steps - 1))
    sent(n_steps - 3, True)
    interleave(finish(n_steps - 2, True), mix(n_steps - 1))
    sent(n_steps - 2, True)
    interleave(finish(n_steps - 1, True))
    sent(n_steps - 1, True)

    def drained(src, ssem):
        pltpu.make_async_copy(src, src, ssem).wait()

    for dest in range(2):
        push_done(*cond_push(dest))
        push_done(*mask_push(dest))

        @pl.when(owner(home, dest) != me)
        def _():
            drained(bias_own, bsend_sem.at[dest])
            drained(act.at[pl.ds(0, half_smp)], asend_sem.at[dest])

        @pl.when(4 * plane + 2 * core + dest != me)
        def _():
            drained(out_stage.at[:, pl.ds(0, seq)], osend_sem.at[dest])

    @pl.when(has_prev)
    def _():
        mask_side(0).wait_send()
        drained(h_ext.at[:, :, pl.ds(0, EDGE)], send_sem.at[0])

    @pl.when(has_next)
    def _():
        mask_side(1).wait_send()
        drained(h_ext.at[:, :, pl.ds(0, EDGE)], send_sem.at[1])

    for dest in range(2):
        arrived(out_hbm.at[pl.ds(dest * half_smp, half_smp)], orecv_sem.at[dest])


def solution(mesh):
    n_dev = mesh.shape['sp']

    def device_fn(atom_act, cond, pair, atom_mask, w_cond, b_cond, w_qkvg, b_query, w_pair, w_out, w_up, w_down):
        samples, seq, width = atom_act.shape
        n_layers = w_qkvg.shape[0]
        n_heads = width // QBLOCK
        half_smp = samples // 2
        n_groups = half_smp // GROUP
        own = 2 * seq
        ext = own + 2 * EDGE
        n_blocks = own // QBLOCK
        blocks, _, window, c_pair = pair.shape
        f32, bf16 = jnp.float32, jnp.bfloat16
        pair_t = pair.transpose(0, 1, 3, 2).reshape(blocks * QBLOCK * c_pair, window)
        vmem = pl.BlockSpec(memory_space=pltpu.VMEM)
        hbm = pl.BlockSpec(memory_space=pl.ANY)
        cols = GROUP * own
        dma = pltpu.SemaphoreType.DMA
        return pl.pallas_call(
            functools.partial(body, n_dev),
            out_shape=jax.ShapeDtypeStruct(atom_act.shape, bf16),
            in_specs=[hbm, hbm, hbm, vmem, hbm, vmem, hbm, vmem, vmem, hbm, hbm, hbm],
            out_specs=hbm,
            scratch_shapes=[
                pltpu.VMEM(pair_t.shape, bf16),
                pltpu.VMEM(w_cond.shape, bf16),
                pltpu.VMEM(w_qkvg.shape, bf16),
                pltpu.VMEM(w_out.shape, bf16),
                pltpu.VMEM(w_up.shape, bf16),
                pltpu.VMEM(w_down.shape, bf16),
                pltpu.VMEM(cond.shape, bf16),
                pltpu.VMEM(atom_act.shape, bf16),
                pltpu.VMEM((half_smp, own, width), bf16),
                pltpu.VMEM((own, width), bf16),
                pltpu.VMEM((8, 128), jnp.int32),
                pltpu.VMEM((4, 8, 128), jnp.int32),
                pltpu.VMEM((n_layers, blocks, n_heads * QBLOCK, window), bf16),
                pltpu.VMEM((n_layers, 2, blocks, n_heads * QBLOCK, window), bf16),
                pltpu.VMEM((half_smp, own, width), bf16),
                pltpu.VMEM((n_groups, width, cols), f32),
                pltpu.VMEM((n_groups, width, cols), bf16),
                pltpu.VMEM((n_layers, half_smp, ext, width), bf16),
                pltpu.VMEM((n_layers, 6, width, own), f32),
                pltpu.VMEM((n_layers, n_blocks, KEY_WINDOW, 128), f32),
                pltpu.VMEM((n_layers, width, width), bf16),
                pltpu.VMEM((n_layers, width, width), bf16),
                pltpu.VMEM((n_layers, width, width), bf16),
                pltpu.VMEM((n_layers, 4 * width, width), bf16),
                pltpu.VMEM((n_layers, width, 2 * width), bf16),
                pltpu.VMEM((n_layers, 6 * width, width), bf16),
                pltpu.VMEM((n_layers, 4, width, own), f32),
                pltpu.VMEM((GROUP, ext, width), bf16),
                pltpu.VMEM((GROUP, n_blocks * 128, width), bf16),
                pltpu.VMEM((GROUP, width, ext), bf16),
                pltpu.VMEM((width, cols), f32),
                pltpu.VMEM((2, 2, KEY_WINDOW, 128), f32),
                pltpu.VMEM((2 * width, cols), bf16),
                pltpu.VMEM((width, cols), bf16),
                dma((12,)),
                dma((2,)),
                dma((n_layers, n_groups, 2)),
                dma((2,)),
                dma((2,)),
                dma((4,)),
                dma((4,)),
                dma((2,)),
                dma((2, n_groups)),
                dma((2,)),
                dma((2, n_layers)),
                dma((2,)),
                dma((2,)),
            ],
            compiler_params=pltpu.CompilerParams(
                collective_id=0, has_side_effects=True, vmem_limit_bytes=60 * 1024 * 1024),
        )(atom_act, cond, pair_t, atom_mask.reshape(1, seq), w_cond, b_cond, w_qkvg, b_query,
          w_pair, w_out, w_up, w_down)

    act_spec = P('dp', 'sp', None)
    in_specs = (act_spec, P('sp', None), P('sp', None, None, None), P('sp'), P(), P(), P(), P(), P(), P(), P(), P())
    return jax.shard_map(device_fn, mesh=mesh, in_specs=in_specs, out_specs=act_spec, check_vma=False)
```

```python
import functools
import math

import jax
import jax.numpy as jnp
from jax import lax
from jax.experimental import pallas as pl
from jax.experimental.pallas import tpu as pltpu
from jax.sharding import PartitionSpec as P

QBLOCK = 32
KEY_WINDOW = 128
EDGE = 48
LN_EPS = 1e-5
GROUP = 2
LOG2E = math.log2(math.e)
MESH = pl.DeviceIdType.MESH


def mm(lhs, rhs):
    return jnp.dot(lhs, rhs, preferred_element_type=jnp.float32)


def mm_nt(lhs, rhs):
    return lax.dot_general(lhs, rhs, (((1,), (1,)), ((), ())), preferred_element_type=jnp.float32)


def sigmoid(vals):
    return 0.5 * jnp.tanh(0.5 * vals) + 0.5


def norm(vals, axis):
    mean = jnp.mean(vals, axis=axis, keepdims=True)
    cent = vals - mean
    var = jnp.mean(cent * cent, axis=axis, keepdims=True)
    return cent * lax.rsqrt(var + LN_EPS)


def body(n_dev, act_hbm, cond_hbm, pair_hbm, mask_ref, wcond_hbm, bcond_ref, wqkvg_hbm, bquery_ref, wpair_ref,
         wout_hbm, wup_hbm, wdown_hbm, out_hbm,
         pair, wcond, wqkvg, wout, wup, wdown, cond_own, act,
         act_in, cond_in, mask_own, mask_in, bias_own, bias_in, out_stage,
         res, h_cm, h_ext, tab, bias, wv_t, wg_t, wo_t, wu_t, wd_t, wc_t, bc_t,
         k_scr, q_scr, v_scr, o_scr, s_scr, m_scr, h_mid,
         in_sem, send_sem, recv_sem, csend_sem, crecv_sem, msend_sem, mrecv_sem, asend_sem, arecv_sem,
         bsend_sem, brecv_sem, osend_sem, orecv_sem):
    n_layers, width = bquery_ref.shape
    n_heads = width // QBLOCK
    head_dim = width // n_heads
    samples, seq, _ = act_hbm.shape
    half_smp = samples // 2
    n_groups = half_smp // GROUP
    own = 2 * seq
    ext = own + 2 * EDGE
    n_blocks = own // QBLOCK
    f32, bf16 = jnp.float32, jnp.bfloat16

    me = lax.axis_index('sp')
    plane, row, core = me // 4, (me // 2) % 2, me % 2
    n_planes = n_dev // 4
    chunk = 2 * plane + core
    has_prev, has_next = chunk > 0, chunk < 2 * n_planes - 1

    def owner(chunk_idx, row_idx):
        return (chunk_idx // 2) * 4 + 2 * row_idx + chunk_idx % 2

    def remote(src, dst, ssem, rsem, peer):
        return pltpu.make_async_remote_copy(
            src_ref=src, dst_ref=dst, send_sem=ssem, recv_sem=rsem, device_id={'sp': peer}, device_id_type=MESH)

    def push(src, dst, ssem, rsem, peer):
        @pl.when(peer != me)
        def _():
            remote(src, dst, ssem, rsem, peer).start()

        @pl.when(peer == me)
        def _():
            pltpu.make_async_copy(src, dst, rsem).start()

    def push_done(src, dst, ssem, rsem, peer):
        @pl.when(peer != me)
        def _():
            remote(src, dst, ssem, rsem, peer).wait_send()

    def arrived(dst, rsem):
        pltpu.make_async_copy(dst, dst, rsem).wait()

    barrier = pltpu.get_barrier_semaphore()

    for other in range(4):
        peer = 4 * plane + other

        @pl.when(peer != me)
        def _():
            pl.semaphore_signal(barrier, inc=1, device_id={'sp': peer}, device_id_type=MESH)

    beyond = chunk + 2 * core - 1
    has_beyond = jnp.logical_and(beyond >= 0, beyond < 2 * n_planes)

    @pl.when(has_beyond)
    def _():
        pl.semaphore_signal(barrier, inc=1, device_id={'sp': owner(beyond, row)}, device_id_type=MESH)

    loads = [pltpu.make_async_copy(src, dst, in_sem.at[pos]) for pos, (src, dst) in enumerate(
        [(pair_hbm, pair), (wcond_hbm, wcond), (wqkvg_hbm, wqkvg), (wout_hbm, wout), (wup_hbm, wup), (wdown_hbm, wdown),
         (cond_hbm, cond_own), (act_hbm, act)])]
    for load in loads:
        load.start()

    def clear(first, slot):
        @pl.loop(0, n_layers)
        def _(layer):
            @pl.loop(0, n_groups)
            def _(grp):
                h_ext[layer, pl.ds(grp * GROUP, GROUP), first:first + EDGE, :] = jnp.zeros((GROUP, EDGE, width), bf16)

        mask_in[slot] = jnp.zeros_like(mask_own)

    @pl.when(jnp.logical_not(has_prev))
    def _():
        clear(0, 0)

    @pl.when(jnp.logical_not(has_next))
    def _():
        clear(EDGE + own, 3)

    mask_own[...] = jnp.zeros_like(mask_own)
    mask_own[0:1, 0:seq] = mask_ref[...]

    home = 2 * plane + row

    def cond_push(dest):
        return (cond_own, cond_in.at[pl.ds(core * seq, seq)], csend_sem.at[dest], crecv_sem.at[core], owner(home, dest))

    def mask_push(dest):
        return (mask_own, mask_in.at[1 + core], msend_sem.at[dest], mrecv_sem.at[1 + core], owner(home, dest))

    def mask_side(direction):
        return remote(mask_in.at[1 + direction], mask_in.at[3 - 3 * direction], msend_sem.at[2 + direction],
                      mrecv_sem.at[3 - 3 * direction], owner(chunk + 2 * direction - 1, row))

    def act_push(dest, grp):
        return (act.at[pl.ds(dest * half_smp + grp * GROUP, GROUP)],
                act_in.at[pl.ds(grp * GROUP, GROUP), pl.ds(core * seq, seq)],
                asend_sem.at[dest], arecv_sem.at[core, grp], owner(home, dest))

    def bias_push(dest, layer):
        return (bias_own.at[layer], bias_in.at[layer, core], bsend_sem.at[dest], brecv_sem.at[core, layer],
                owner(home, dest))

    c_pair = wpair_ref.shape[0]
    n_col = wpair_ref.shape[1]
    tall, deep = n_col * 16, 16 * c_pair
    pick_col = (lax.broadcasted_iota(jnp.int32, (tall, n_col), 0) // 16
                == lax.broadcasted_iota(jnp.int32, (tall, n_col), 1)).astype(bf16)
    pick_chan = (lax.broadcasted_iota(jnp.int32, (c_pair, deep), 1) % c_pair
                 == lax.broadcasted_iota(jnp.int32, (c_pair, deep), 0)).astype(bf16)
    spread = lax.dot_general(
        wpair_ref[...], pick_chan, (((0,), (0,)), ((), ())), preferred_element_type=f32).astype(bf16)
    spread = mm(pick_col, spread)
    same = (lax.broadcasted_iota(jnp.int32, (tall, deep), 0) % 16 == lax.broadcasted_iota(jnp.int32, (tall, deep), 1) // c_pair)
    w_block = jnp.where(same, spread, 0.0).astype(bf16)
    loads[0].wait()
    for part in range(seq // 16):
        vals = pair[part * deep:(part + 1) * deep].astype(f32).reshape(16, c_pair, KEY_WINDOW)
        vals = norm(vals, 1).astype(bf16).reshape(deep, KEY_WINDOW)
        res_bias = mm(w_block, vals).astype(bf16)
        blk, sub = part // 2, part % 2
        for layer in range(n_layers):
            for head in range(n_heads):
                col = layer * n_heads + head
                bias_own[layer, blk, head * QBLOCK + sub * 16:head * QBLOCK + (sub + 1) * 16, :] = res_bias[col * 16:(col + 1) * 16]
    half = jnp.array(0.5, bf16)

    def weights(layer):
        for idx, bias_idx in enumerate((0, None, 1, 2, None, 3)):
            piece = wcond[layer, :, idx * width:(idx + 1) * width].T
            wc_t[layer, idx * width:(idx + 1) * width, :] = piece if bias_idx is None else piece * half
            if bias_idx is not None:
                cell = bcond_ref[pl.ds(layer, 1), :][:, bias_idx * width:(bias_idx + 1) * width] * 0.5
                bc_t[layer, bias_idx] = jnp.broadcast_to(cell, (own, width)).T
        wv_t[layer] = wqkvg[layer, :, 2 * width:3 * width].T
        wg_t[layer] = wqkvg[layer, :, 3 * width:].T * half
        wo_t[layer] = wout[layer].T
        for idx in range(4):
            piece = wup[layer, :, idx * width:(idx + 1) * width].T
            wu_t[layer, idx * width:(idx + 1) * width, :] = piece * half if idx < 2 else piece
        for idx in range(2):
            wd_t[layer, :, idx * width:(idx + 1) * width] = wdown[layer, idx * width:(idx + 1) * width, :].T

    for load in loads[1:]:
        load.wait()

    weights(0)

    n_beyond = jnp.where(has_beyond, 1, 0)
    pl.semaphore_wait(barrier, 3 + n_beyond)

    for dest in (1 - row, row):
        push(*cond_push(dest))
    for grp in range(3):
        for dest in (1 - row, row):
            push(*act_push(dest, grp))
        if grp == 0:
            for dest in (1 - row, row):
                push(*mask_push(dest))
    for dest in (1 - row, row):
        push(*bias_push(dest, 0))
    for grp in range(3, n_groups):
        for dest in (1 - row, row):
            push(*act_push(dest, grp))
    for layer in range(1, n_layers):
        for dest in (1 - row, row):
            push(*bias_push(dest, layer))

    @pl.loop(1, n_layers)
    def _(layer):
        weights(layer)

    for slot in range(2):
        arrived(cond_in.at[pl.ds(slot * seq, seq)], crecv_sem.at[slot])
    cond_norm = norm(cond_in[...].astype(f32), -1).astype(bf16)

    def tables(layer, first=0, last=6):
        proj = mm_nt(wc_t[layer, first * width:last * width], cond_norm)
        yield
        for idx, bias_idx in list(enumerate((0, None, 1, 2, None, 3)))[first:last]:
            piece = proj[(idx - first) * width:(idx - first + 1) * width]
            if bias_idx is not None:
                piece = 0.5 * jnp.tanh(piece + bc_t[layer, bias_idx]) + 0.5
            tab[layer, idx] = piece
            yield

    def idle(rounds):
        for _ in range(rounds):
            yield

    def chain(*parts):
        for part in parts:
            yield from part

    def interleave(*stages):
        stages = list(stages)
        while stages:
            for stage in list(stages):
                if next(stage, stages) is stages:
                    stages.remove(stage)

    def both(vals):
        return jnp.concatenate([vals] * GROUP, axis=1)

    def halo_copy(layer, grp, direction):
        smp = pl.ds(grp * GROUP, GROUP)
        src = pl.ds(own if direction else EDGE, EDGE)
        dst = pl.ds(0 if direction else own + EDGE, EDGE)
        return remote(h_ext.at[layer, smp, src, :], h_ext.at[layer, smp, dst, :],
                      send_sem.at[direction], recv_sem.at[layer, grp, direction],
                      owner(chunk + 1 if direction else chunk - 1, row))

    def halo_start(layer, grp):
        @pl.when(has_prev)
        def _():
            halo_copy(layer, grp, 0).start()

        @pl.when(has_next)
        def _():
            halo_copy(layer, grp, 1).start()

    def halo_wait(layer, grp):
        @pl.when(has_next)
        def _():
            halo_copy(layer, grp, 0).wait_recv()

        @pl.when(has_prev)
        def _():
            halo_copy(layer, grp, 1).wait_recv()

    def emit_h(layer, grp, resid):
        h_t = (norm(resid, 0) * both(tab[layer, 0]) + both(tab[layer, 1])).astype(bf16)
        h_cm[grp] = h_t
        for smp in range(GROUP):
            h_ext[layer, grp * GROUP + smp, EDGE:EDGE + own, :] = h_t[:, smp * own:(smp + 1) * own].T

    def act_wait(grp):
        for slot in range(2):
            arrived(act_in.at[pl.ds(grp * GROUP, GROUP), pl.ds(slot * seq, seq)], arecv_sem.at[slot, grp])

    def enter(grp):
        cols = [act_in[grp * GROUP + smp].T.astype(f32) for smp in range(GROUP)]
        yield
        resid = jnp.concatenate(cols, axis=1)
        res[grp] = resid
        yield
        emit_h(0, grp, resid)
        yield

    def bias_wait(layer):
        for slot in range(2):
            arrived(bias_in.at[layer, slot], brecv_sem.at[slot, layer])

    def bias_table(layer, mask_bias):
        for blk in range(n_blocks):
            nat = bias_in[layer, blk // 2, blk % 2].astype(f32)
            order = [(slot - blk) % n_heads for slot in range(n_heads)]
            nat = jnp.concatenate([nat[head * QBLOCK:(head + 1) * QBLOCK] for head in order], axis=0)
            bias[layer, blk] = ((nat + mask_bias[:, blk * QBLOCK:blk * QBLOCK + KEY_WINDOW]) * LOG2E).T
            yield

    interleave(tables(0, 0, 2))
    act_wait(0)
    interleave(enter(0))
    halo_start(0, 0)
    act_wait(1)
    interleave(enter(1), chain(tables(0, 2, 6), tables(1)))
    halo_start(0, 1)
    for slot in range(1, 3):
        arrived(mask_in.at[slot], mrecv_sem.at[slot])

    @pl.when(has_prev)
    def _():
        mask_side(0).start()

    @pl.when(has_next)
    def _():
        mask_side(1).start()

    act_wait(2)
    interleave(enter(2), tables(2))
    halo_start(0, 2)
    @pl.when(has_prev)
    def _():
        arrived(mask_in.at[0], mrecv_sem.at[0])

    @pl.when(has_next)
    def _():
        arrived(mask_in.at[3], mrecv_sem.at[3])

    mask_row = jnp.concatenate([mask_in[0, 0:1, seq - EDGE:seq], mask_in[1, 0:1, :seq], mask_in[2, 0:1, :seq],
                                mask_in[3, 0:1, :EDGE], jnp.zeros((1, 256 - ext), jnp.int32)], axis=1)
    mask_bias = (mask_row.astype(f32) - 1.0) * 1e9
    bias_wait(0)
    act_wait(3)
    interleave(enter(3), bias_table(0, mask_bias))
    halo_start(0, 3)

    lane = lax.broadcasted_iota(jnp.int32, (1, width), 1)
    scale = head_dim ** -0.5 * LOG2E
    keep = [jnp.where(lane // QBLOCK == slot, 1.0, 0.0).astype(bf16) for slot in range(n_heads)]

    def split(idx):
        return idx // n_groups, idx % n_groups

    def project(idx):
        layer, grp = split(idx)
        w_qk = wqkvg[layer, :, :2 * width]
        b_q = bquery_ref[pl.ds(layer, 1), :]
        q_k = {}
        v_t = {}

        def k_q(smp):
            q_k[smp] = mm(h_ext[layer, grp * GROUP + smp], w_qk)

        def vals(smp):
            v_t[smp] = mm_nt(wv_t[layer], h_ext[layer, grp * GROUP + smp])

        def keys(smp):
            k_scr[smp] = q_k[smp][:, width:].astype(bf16)

        def queries(smp):
            q_val = (q_k[smp][EDGE:EDGE + own, :width] + b_q).astype(bf16)
            for blk in range(n_blocks):
                part = q_val[blk * QBLOCK:(blk + 1) * QBLOCK]
                for slot in range(n_heads):
                    first = blk * 128 + slot * QBLOCK
                    q_scr[smp, first:first + QBLOCK, :] = part * keep[(slot - blk) % n_heads]
                if blk % 2:
                    yield

        k_q(0)
        yield
        yield from idle(0)
        vals(0)
        yield
        yield from idle(0)
        keys(0)
        yield
        yield from queries(0)
        k_q(1)
        yield from idle(0)
        v_scr[0] = v_t[0].astype(bf16)
        yield
        vals(1)
        yield
        yield from idle(0)
        keys(1)
        yield
        yield from queries(1)
        yield from idle(2)
        v_scr[1] = v_t[1].astype(bf16)
        yield

    def score(unit):
        smp, duo = unit // 2, unit % 2
        return mm_nt(k_scr[smp, duo * 64:duo * 64 + 160], q_scr[smp, duo * 256:(duo + 1) * 256, :])

    def score_early():
        for unit in range(2):
            logit = score(unit)
            yield
            for sub in range(2):
                s_scr[unit, sub] = logit[sub * QBLOCK:sub * QBLOCK + KEY_WINDOW, sub * 128:(sub + 1) * 128]
            yield

    def attend(idx):
        layer, grp = split(idx)
        logits = {}
        out = {}

        def prob(unit, sub):
            blk = 2 * (unit % 2) + sub
            if unit < 2:
                x = s_scr[unit, sub]
            else:
                x = logits[unit][sub * QBLOCK:sub * QBLOCK + KEY_WINDOW, sub * 128:(sub + 1) * 128]
            x = x * scale + bias[layer, blk]
            e = jnp.exp2(x - jnp.max(x, axis=0, keepdims=True))
            p = (e * (0.5 / jnp.sum(e, axis=0, keepdims=True))).astype(bf16)
            parts = [p]
            if blk:
                parts = [jnp.zeros((blk * QBLOCK, 128), bf16)] + parts
            if blk < n_blocks - 1:
                parts = parts + [jnp.zeros(((n_blocks - 1 - blk) * QBLOCK, 128), bf16)]
            return jnp.concatenate(parts, axis=0)

        def place(unit):
            smp, duo = unit // 2, unit % 2
            cols = slice(smp * own, (smp + 1) * own)
            for head in range(n_heads):
                rows = slice(head * head_dim, (head + 1) * head_dim)
                pair_out = [out[unit][rows, sub * 128:(sub + 1) * 128] for sub in range(2)]
                pick = lane // QBLOCK == (head + 2 * duo + 1) % n_heads
                merged = jnp.where(pick, pair_out[1], pair_out[0])
                if duo:
                    first = lane // QBLOCK == (head + 2) % n_heads
                    merged = jnp.where(jnp.logical_or(pick, first), merged, o_scr[rows, cols])
                o_scr[rows, cols] = merged

        for unit in range(2 * GROUP):
            if unit >= 2:
                logits[unit] = score(unit) if unit not in logits else logits[unit]
            probs = []
            for sub in range(2):
                probs.append(prob(unit, sub))
                yield
            out[unit] = mm(v_scr[unit // 2], jnp.concatenate(probs, axis=1))
            if unit + 2 < 2 * GROUP and unit + 2 >= 2:
                logits[unit + 2] = score(unit + 2)
            if unit:
                place(unit - 1)
            yield
        place(2 * GROUP - 1)
        yield

    def mix(idx):
        layer, grp = split(idx)
        gate = mm(wg_t[layer], h_cm[grp])
        yield
        yield from idle(3)
        heads = []
        for head in range(n_heads):
            rows = slice(head * head_dim, (head + 1) * head_dim)
            parts = []
            for smp in range(GROUP):
                part = o_scr[rows, smp * own:(smp + 1) * own]
                parts.append(pltpu.roll(part, (128 - head * QBLOCK) % 128, 1) if head else part)
            heads.append(jnp.concatenate(parts, axis=1))
        o_val = ((jnp.tanh(gate) + 1.0) * jnp.concatenate(heads, axis=0)).astype(bf16)
        proj = mm(wo_t[layer], o_val)
        yield
        yield from idle(2)
        resid = res[grp] + both(tab[layer, 2]) * proj
        res[grp] = resid
        yield
        yield from idle(4)
        h_mid[...] = (norm(resid, 0) * both(tab[layer, 3]) + both(tab[layer, 4])).astype(bf16)
        yield

    def finish(idx, last):
        layer, grp = split(idx)
        h_t = h_mid[...]
        n_chunk = 2
        rows = 2 * width // n_chunk
        ups = {}
        for pos in range(n_chunk + 1):
            if pos < n_chunk:
                ups[pos] = [mm(wu_t[layer, pl.ds(base + pos * rows, rows), :], h_t) for base in (0, 2 * width)]
                yield
                if pos == 0:
                    yield from idle(1)
            if pos:
                left, right = ups[pos - 1]
                m_scr[(pos - 1) * rows:pos * rows, :] = ((left * jnp.tanh(left) + left) * right).astype(bf16)
                yield
        down = mm(wd_t[layer], m_scr[...])
        yield
        yield from idle(0)
        resid = res[grp] + both(tab[layer, 5]) * down
        yield
        if last:
            for smp in range(GROUP):
                out_stage[grp * GROUP + smp] = resid[:, smp * own:(smp + 1) * own].astype(bf16).T
                yield
        else:
            res[grp] = resid
            yield
            emit_h(layer + 1, grp, resid)
            yield

    def out_push(grp, slot):
        return (out_stage.at[pl.ds(grp * GROUP, GROUP), pl.ds(slot * seq, seq)],
                out_hbm.at[pl.ds(row * half_smp + grp * GROUP, GROUP)],
                osend_sem.at[slot], orecv_sem.at[row], 4 * plane + 2 * core + slot)

    def sent(idx, last):
        layer, grp = split(idx)
        if last:
            for slot in range(2):
                push(*out_push(grp, slot))
        else:
            halo_start(layer + 1, grp)

    def loop_body(idx, last, *extra):
        halo_wait(*split(idx + 1))
        interleave(chain(idle(1), finish(idx - 2, last)), chain(idle(0), mix(idx - 1)), attend(idx), chain(idle(2), project(idx + 1)), chain(idle(10), score_early()), *extra)
        sent(idx - 2, last)

    n_steps = n_layers * n_groups
    split_at = n_steps - n_groups
    act_wait(4)
    halo_wait(0, 0)
    interleave(enter(4), chain(project(0), score_early()))
    halo_start(0, 4)
    act_wait(5)
    halo_wait(0, 1)
    interleave(attend(0), chain(project(1), score_early()), enter(5))
    halo_start(0, 5)
    act_wait(6)
    halo_wait(0, 2)
    interleave(mix(0), attend(1), chain(project(2), score_early()), enter(6))
    halo_start(0, 6)
    act_wait(7)
    loop_body(2, False, enter(7))
    halo_start(0, 7)

    @pl.loop(3, 7)
    def _(idx):
        loop_body(idx, False)

    bias_wait(1)
    loop_body(7, False, bias_table(1, mask_bias))

    @pl.loop(8, 12)
    def _(idx):
        loop_body(idx, False)

    bias_wait(2)
    loop_body(12, False, bias_table(2, mask_bias))

    @pl.loop(13, split_at + 2)
    def _(idx):
        loop_body(idx, False)

    @pl.loop(split_at + 2, n_steps - 1)
    def _(idx):
        loop_body(idx, True)

    interleave(finish(n_steps - 3, True), mix(n_steps - 2), attend(n_steps - 1))
    sent(n_steps - 3, True)
    interleave(finish(n_steps - 2, True), mix(n_steps - 1))
    sent(n_steps - 2, True)
    interleave(finish(n_steps - 1, True))
    sent(n_steps - 1, True)

    def drained(src, ssem):
        pltpu.make_async_copy(src, src, ssem).wait()

    for dest in range(2):
        push_done(*cond_push(dest))
        push_done(*mask_push(dest))

        @pl.when(owner(home, dest) != me)
        def _():
            drained(bias_own, bsend_sem.at[dest])
            drained(act.at[pl.ds(0, half_smp)], asend_sem.at[dest])

        @pl.when(4 * plane + 2 * core + dest != me)
        def _():
            drained(out_stage.at[:, pl.ds(0, seq)], osend_sem.at[dest])

    @pl.when(has_prev)
    def _():
        mask_side(0).wait_send()
        drained(h_ext.at[:, :, pl.ds(0, EDGE)], send_sem.at[0])

    @pl.when(has_next)
    def _():
        mask_side(1).wait_send()
        drained(h_ext.at[:, :, pl.ds(0, EDGE)], send_sem.at[1])

    for dest in range(2):
        arrived(out_hbm.at[pl.ds(dest * half_smp, half_smp)], orecv_sem.at[dest])


def solution(mesh):
    n_dev = mesh.shape['sp']

    def device_fn(atom_act, cond, pair, atom_mask, w_cond, b_cond, w_qkvg, b_query, w_pair, w_out, w_up, w_down):
        samples, seq, width = atom_act.shape
        n_layers = w_qkvg.shape[0]
        n_heads = width // QBLOCK
        half_smp = samples // 2
        n_groups = half_smp // GROUP
        own = 2 * seq
        ext = own + 2 * EDGE
        n_blocks = own // QBLOCK
        blocks, _, window, c_pair = pair.shape
        f32, bf16 = jnp.float32, jnp.bfloat16
        pair_t = pair.transpose(0, 1, 3, 2).reshape(blocks * QBLOCK * c_pair, window)
        vmem = pl.BlockSpec(memory_space=pltpu.VMEM)
        hbm = pl.BlockSpec(memory_space=pl.ANY)
        cols = GROUP * own
        dma = pltpu.SemaphoreType.DMA
        return pl.pallas_call(
            functools.partial(body, n_dev),
            out_shape=jax.ShapeDtypeStruct(atom_act.shape, bf16),
            in_specs=[hbm, hbm, hbm, vmem, hbm, vmem, hbm, vmem, vmem, hbm, hbm, hbm],
            out_specs=hbm,
            scratch_shapes=[
                pltpu.VMEM(pair_t.shape, bf16),
                pltpu.VMEM(w_cond.shape, bf16),
                pltpu.VMEM(w_qkvg.shape, bf16),
                pltpu.VMEM(w_out.shape, bf16),
                pltpu.VMEM(w_up.shape, bf16),
                pltpu.VMEM(w_down.shape, bf16),
                pltpu.VMEM(cond.shape, bf16),
                pltpu.VMEM(atom_act.shape, bf16),
                pltpu.VMEM((half_smp, own, width), bf16),
                pltpu.VMEM((own, width), bf16),
                pltpu.VMEM((8, 128), jnp.int32),
                pltpu.VMEM((4, 8, 128), jnp.int32),
                pltpu.VMEM((n_layers, blocks, n_heads * QBLOCK, window), bf16),
                pltpu.VMEM((n_layers, 2, blocks, n_heads * QBLOCK, window), bf16),
                pltpu.VMEM((half_smp, own, width), bf16),
                pltpu.VMEM((n_groups, width, cols), f32),
                pltpu.VMEM((n_groups, width, cols), bf16),
                pltpu.VMEM((n_layers, half_smp, ext, width), bf16),
                pltpu.VMEM((n_layers, 6, width, own), f32),
                pltpu.VMEM((n_layers, n_blocks, KEY_WINDOW, 128), f32),
                pltpu.VMEM((n_layers, width, width), bf16),
                pltpu.VMEM((n_layers, width, width), bf16),
                pltpu.VMEM((n_layers, width, width), bf16),
                pltpu.VMEM((n_layers, 4 * width, width), bf16),
                pltpu.VMEM((n_layers, width, 2 * width), bf16),
                pltpu.VMEM((n_layers, 6 * width, width), bf16),
                pltpu.VMEM((n_layers, 4, width, own), f32),
                pltpu.VMEM((GROUP, ext, width), bf16),
                pltpu.VMEM((GROUP, n_blocks * 128, width), bf16),
                pltpu.VMEM((GROUP, width, ext), bf16),
                pltpu.VMEM((width, cols), f32),
                pltpu.VMEM((2, 2, KEY_WINDOW, 128), f32),
                pltpu.VMEM((2 * width, cols), bf16),
                pltpu.VMEM((width, cols), bf16),
                dma((12,)),
                dma((2,)),
                dma((n_layers, n_groups, 2)),
                dma((2,)),
                dma((2,)),
                dma((4,)),
                dma((4,)),
                dma((2,)),
                dma((2, n_groups)),
                dma((2,)),
                dma((2, n_layers)),
                dma((2,)),
                dma((2,)),
            ],
            compiler_params=pltpu.CompilerParams(
                collective_id=0, has_side_effects=True, vmem_limit_bytes=60 * 1024 * 1024),
        )(atom_act, cond, pair_t, atom_mask.reshape(1, seq), w_cond, b_cond, w_qkvg, b_query,
          w_pair, w_out, w_up, w_down)

    act_spec = P('dp', 'sp', None)
    in_specs = (act_spec, P('sp', None), P('sp', None, None, None), P('sp'), P(), P(), P(), P(), P(), P(), P(), P())
    return jax.shard_map(device_fn, mesh=mesh, in_specs=in_specs, out_specs=act_spec, check_vma=False)
```
